32 devices in a mesh: tm: 2 (over x), py: 4 (over y, core), pz: 4 (over z).
Axes of the slice: x: 2, y: 2, z: 4, core: 2. Of those that a mesh axis runs over, the one named last changes fastest.
Arguments:
- start_states: float32 [2, 3, 128, 8, 16, 128], P('tm', None, None, None, ('py', 'pz')), may hold values from -6 to 6
Outputs:
- new_states: float32 [2, 3, 128, 8, 16, 128], P('tm', None, None, None, ('py', 'pz'))
The draws below stay inside these ranges and needn't reach their ends.
All inputs are finite; a program needn't handle non-finite values.
Results may differ from the reference program's by a relative error of at most 0.0001.
Values sent between devices are 32-bit elements; how exact they have to be, the bound alone decides.
A program may use at most 128 MiB of HBM per device.

```python
import jax
import jax.numpy as jnp
from jax import lax

N = 128
M = 64
PEN = 16
SLICES = 2


def shard_levels(rng, shape, shards, least, high):
    level = 1.0
    for dim, shards_of in shards:
        draws = jax.random.uniform(jax.random.fold_in(jax.random.fold_in(rng, 6), dim), (shards_of,), jnp.float32, least / len(shards), high / len(shards))
        level = level * jnp.repeat(jnp.exp(draws), shape[dim] // shards_of).reshape((-1,) + (1,) * (len(shape) - 1 - dim))
    return level


def bell_draw(rng, shape, width, most, cuts=(), kind=jnp.bfloat16):
    entries = width * jax.random.normal(rng, shape, jnp.float32)
    if cuts:
        entries = entries * shard_levels(rng, shape, cuts, -0.22, 0.18)
    return jnp.clip(entries, -most, most).astype(kind)


def setup_inputs(seed: int = 0) -> dict:
    arg_keys = jax.random.split(jax.random.key(seed), 2)
    return {
        "start_states": bell_draw(arg_keys[0], (SLICES, 3, N, N // PEN, PEN, N), 1.0, 6.0, ((0, 2), (4, 16)), jnp.float32),
    }


viscosity = 0.03
time_step = 0.004


def signed_wave(length):
    places = jnp.arange(length, dtype=jnp.int32)
    return jnp.where(places < length // 2, places, places - length).astype(jnp.float32)


def wavenumbers(retained):
    wave_x = signed_wave(retained)[:, None, None]
    wave_y = signed_wave(retained)[None, :, None]
    wave_z = jnp.arange(retained // 2, dtype=jnp.int32).astype(jnp.float32)[None, None, :]
    return wave_x, wave_y, wave_z


def vorticity(coeffs, wavegrid):
    wave_x, wave_y, wave_z = wavegrid
    along_x = 1j * (wave_y * coeffs[2] - wave_z * coeffs[1])
    along_y = 1j * (wave_z * coeffs[0] - wave_x * coeffs[2])
    along_z = 1j * (wave_x * coeffs[1] - wave_y * coeffs[0])
    return jnp.stack([along_x, along_y, along_z])


def project(coeffs, wavegrid):
    wave_x, wave_y, wave_z = wavegrid
    squared = wave_x * wave_x + wave_y * wave_y + wave_z * wave_z
    divergence = (wave_x * coeffs[0] + wave_y * coeffs[1] + wave_z * coeffs[2]) / jnp.maximum(squared, 1.0)
    return jnp.stack([coeffs[0] - wave_x * divergence, coeffs[1] - wave_y * divergence, coeffs[2] - wave_z * divergence])


def cross_product(first_field, second_field):
    return jnp.stack([
        first_field[1] * second_field[2] - first_field[2] * second_field[1],
        first_field[2] * second_field[0] - first_field[0] * second_field[2],
        first_field[0] * second_field[1] - first_field[1] * second_field[0],
    ])


def widen(coeffs, extent, contracted):
    length = coeffs.shape[contracted]
    halfway = length // 2
    low_part = lax.slice_in_dim(coeffs, 0, halfway, axis=contracted)
    high_part = lax.slice_in_dim(coeffs, halfway, length, axis=contracted)
    filler_shape = list(coeffs.shape)
    filler_shape[contracted] = extent - length
    return jnp.concatenate([low_part, jnp.zeros(filler_shape, coeffs.dtype), high_part], axis=contracted)


def narrow(coeffs, kept, contracted):
    length = coeffs.shape[contracted]
    halfway = kept // 2
    low_part = lax.slice_in_dim(coeffs, 0, halfway, axis=contracted)
    high_part = lax.slice_in_dim(coeffs, length - halfway, length, axis=contracted)
    return jnp.concatenate([low_part, high_part], axis=contracted)


def widen_last(coeffs, columns):
    filler_shape = list(coeffs.shape)
    filler_shape[3] = columns - coeffs.shape[3]
    return jnp.concatenate([coeffs, jnp.zeros(filler_shape, coeffs.dtype)], axis=3)


def to_physical(coeffs, extent):
    retained = coeffs.shape[1]
    spread = widen(widen(coeffs, extent, 1), extent, 2)
    spread = widen_last(spread, extent // 2 + 1)
    spread = jnp.fft.ifft(spread, axis=1)
    spread = jnp.fft.ifft(spread, axis=2)
    constant_column = jnp.real(spread[..., :1]).astype(spread.dtype)
    spread = jnp.concatenate([constant_column, spread[..., 1:]], axis=3)
    return jnp.fft.irfft(spread, n=extent, axis=3) * (extent ** 3 / retained ** 1.5)


def to_spectral(fields, retained):
    extent = fields.shape[-1]
    spectrum = jnp.fft.rfftn(fields, axes=(1, 2, 3))
    spectrum = narrow(narrow(spectrum, retained, 1), retained, 2)[..., : retained // 2]
    return spectrum * (retained ** 1.5 / extent ** 3)


def restrict(coeffs, kept):
    return narrow(narrow(coeffs, kept, 1), kept, 2)[..., : kept // 2]


def prolong(coeffs, retained):
    wider = widen(widen(coeffs, retained, 1), retained, 2)
    return widen_last(wider, retained // 2)


def advance(coeffs):
    retained = coeffs.shape[1]
    extent = 3 * retained // 2
    wavegrid = wavenumbers(retained)
    fields = to_physical(jnp.concatenate([coeffs, vorticity(coeffs, wavegrid)], axis=0), extent)
    product = cross_product(fields[:3], fields[3:])
    nonlinear = to_spectral(product, retained)
    wave_x, wave_y, wave_z = wavegrid
    squared = wave_x * wave_x + wave_y * wave_y + wave_z * wave_z
    damping = jnp.exp(-viscosity * time_step * squared)
    return damping * (coeffs + time_step * project(nonlinear, wavegrid))


def pack(coeffs):
    merged = jnp.concatenate([jnp.real(coeffs), jnp.imag(coeffs)], axis=-1).astype(jnp.float32)
    return merged.reshape(3, N, N // PEN, PEN, N)


def unpack(stored):
    merged = stored.reshape(3, N, N, N)
    return merged[..., : N // 2] + 1j * merged[..., N // 2:]


def reference(start_states):
    slices = start_states.shape[0]
    fine_ends = []
    corrections = []
    first_state = None
    for slice_number in range(slices):
        spectral_state = project(unpack(start_states[slice_number]), wavenumbers(N))
        if slice_number == 0:
            first_state = spectral_state
        fine_end = advance(spectral_state)
        coarse_next = advance(restrict(spectral_state, M))
        fine_ends.append(fine_end)
        corrections.append(restrict(fine_end, M) - coarse_next)
    chained = restrict(fine_ends[0], M)
    packed = [pack(first_state)]
    for slice_number in range(1, slices):
        previous = fine_ends[slice_number - 1]
        upper_band = previous - prolong(restrict(previous, M), N)
        packed.append(pack(prolong(chained, N) + upper_band))
        if slice_number < slices - 1:
            chained = advance(chained) + corrections[slice_number]
    return jnp.stack(packed)
```

```python
from functools import partial
import math

import jax
import jax.numpy as jnp
from jax import lax
import numpy as np
from jax.experimental import pallas as pl
from jax.experimental.pallas import tpu as pltpu
from jax.sharding import PartitionSpec as P

M = 64


viscosity = 0.03
time_step = 0.004
highest = lax.Precision.HIGHEST


def shifted(block, axis, distance):
    devices = range(lax.axis_size(axis))
    route = [(i - distance, i) for i in devices if i - distance in devices]
    return lax.ppermute(block, axis, route)


def signed_wave(places, length):
    return jnp.where(places < length // 2, places, places - length)


def rotate(values):
    halfway = values.shape[-1] // 2
    return jnp.concatenate([-values[..., halfway:], values[..., :halfway]], axis=-1)


def trig_pair(outer, inner, extent, factor):
    residue = jnp.mod(outer[:, None] * inner[None, :], extent)
    radians = residue.astype(jnp.float32) * (2.0 * math.pi / extent)
    return (jnp.cos(radians) * factor, jnp.sin(radians) * factor)


def complex_apply(cosine_part, sine_part, values, contracted, direction_sign):
    kernel = jnp.stack(
        [
            jnp.stack([cosine_part, -direction_sign * sine_part]),
            jnp.stack([direction_sign * sine_part, cosine_part]),
        ]
    )
    halfway = values.shape[-1] // 2
    split = values.reshape(values.shape[:-1] + (2, halfway))
    if contracted == 1:
        pattern = "pqok,fkaqh->foaph"
    else:
        pattern = "pqok,flkqh->floph"
    result = jnp.einsum(pattern, kernel, split, precision=highest)
    return result.reshape(result.shape[:-2] + (2 * halfway,))


def inverse_z(extent, retained):
    halfway = retained // 2
    columns = jnp.arange(retained, dtype=jnp.int32)
    harmonic = columns % halfway
    weight = jnp.where(harmonic == 0, 1.0, 2.0) * retained ** (-0.5)
    residue = jnp.mod(harmonic[:, None] * jnp.arange(extent, dtype=jnp.int32)[None, :], extent)
    radians = residue.astype(jnp.float32) * (2.0 * math.pi / extent)
    return (
        jnp.where((columns < halfway)[:, None], jnp.cos(radians), -jnp.sin(radians))
        * weight[:, None]
    )


def forward_z(extent, retained):
    halfway = retained // 2
    columns = jnp.arange(retained, dtype=jnp.int32)
    harmonic = columns % halfway
    residue = jnp.mod(jnp.arange(extent, dtype=jnp.int32)[:, None] * harmonic[None, :], extent)
    radians = residue.astype(jnp.float32) * (2.0 * math.pi / extent)
    return jnp.where((columns < halfway)[None, :], jnp.cos(radians), -jnp.sin(radians)) * (
        math.sqrt(retained) / extent
    )


def inverse_tail(portion, extent, sectioned, layout):
    count_py, count_pz, groups, member = layout
    retained = portion.shape[2]
    local_rows = retained // groups
    places = jnp.arange(retained, dtype=jnp.int32)
    owners = places // local_rows
    wave_y = signed_wave(places % local_rows * groups + owners, retained)
    points = jnp.arange(extent, dtype=jnp.int32)
    cosine_part, sine_part = trig_pair(points, wave_y, extent, retained ** (-0.5))
    along_y = complex_apply(cosine_part, sine_part, portion, 2, 1.0)
    return jnp.einsum("flyr,rz->flyz", along_y, inverse_z(extent, retained), precision=highest)


def forward_tail(portion, retained, sectioned, layout):
    count_py, count_pz, groups, member = layout
    extent = portion.shape[1]
    local_rows = extent // groups
    places = jnp.arange(extent, dtype=jnp.int32)
    points = places // local_rows * local_rows + places % local_rows
    wave_x = signed_wave(jnp.arange(retained, dtype=jnp.int32), retained)
    cosine_part, sine_part = trig_pair(wave_x, points, extent, math.sqrt(retained) / extent)
    return complex_apply(cosine_part, sine_part, portion, 1, -1.0)


def to_physical(coeffs, wavegrid, extent, resolution, layout):
    wave_x, wave_y, wave_z = wavegrid
    retained = coeffs.shape[1]
    seeds = jnp.concatenate([coeffs, wave_x * coeffs[1:3]], axis=0)
    points = jnp.arange(extent, dtype=jnp.int32)
    wave_rows = signed_wave(jnp.arange(retained, dtype=jnp.int32), retained)
    cosine_part, sine_part = trig_pair(points, wave_rows, extent, retained ** (-0.5))
    moved_x = complex_apply(cosine_part, sine_part, seeds, 1, 1.0)
    curl_x = rotate(wave_y * moved_x[2] - wave_z * moved_x[1])
    curl_y = rotate(wave_z * moved_x[0] - moved_x[4])
    curl_z = rotate(moved_x[3] - wave_y * moved_x[0])
    spread = jnp.concatenate([moved_x[:3], jnp.stack([curl_x, curl_y, curl_z])], axis=0)
    if resolution == "coarse":
        finish = partial(inverse_tail, extent=extent, sectioned=False, layout=layout)
        return finish(lax.all_to_all(spread, ("py", "pz"), split_axis=1, concat_axis=2, tiled=True))
    else:
        finish = partial(inverse_tail, extent=extent, sectioned=False, layout=layout)
        return finish(lax.all_to_all(spread, ("py", "pz"), split_axis=1, concat_axis=2, tiled=True))


def to_spectral(fields, retained, resolution, layout):
    count_py, count_pz, groups, member = layout
    extent = fields.shape[-1]
    along_z = jnp.einsum("flyz,zr->flyr", fields, forward_z(extent, retained), precision=highest)
    local_rows = retained // groups
    places = jnp.arange(retained, dtype=jnp.int32)
    wave_y = signed_wave(places % local_rows * groups + places // local_rows, retained)
    cosine_part, sine_part = trig_pair(
        wave_y, jnp.arange(extent, dtype=jnp.int32), extent, math.sqrt(retained) / extent
    )
    along_y = complex_apply(cosine_part, sine_part, along_z, 2, -1.0)
    if resolution == "coarse":
        finish = partial(forward_tail, retained=retained, sectioned=False, layout=layout)
        return finish(
            lax.all_to_all(along_y, ("py", "pz"), split_axis=2, concat_axis=1, tiled=True)
        )
    else:
        finish = partial(forward_tail, retained=retained, sectioned=False, layout=layout)
        return finish(
            lax.all_to_all(along_y, ("py", "pz"), split_axis=2, concat_axis=1, tiled=True)
        )


def wave_grid(retained, layout):
    count_py, count_pz, groups, member = layout
    places = jnp.arange(retained, dtype=jnp.int32)
    wave_x = signed_wave(places, retained).astype(jnp.float32)[:, None, None]
    local_places = jnp.arange(retained // groups, dtype=jnp.int32)
    wave_y = signed_wave(local_places * groups + member, retained).astype(jnp.float32)[
        None, :, None
    ]
    wave_z = (places % (retained // 2)).astype(jnp.float32)[None, None, :]
    return (wave_x, wave_y, wave_z)


def project(coeffs, wavegrid):
    wave_x, wave_y, wave_z = wavegrid
    squared = wave_x * wave_x + wave_y * wave_y + wave_z * wave_z
    divergence = (wave_x * coeffs[0] + wave_y * coeffs[1] + wave_z * coeffs[2]) / jnp.maximum(
        squared, 1.0
    )
    return jnp.stack(
        [
            coeffs[0] - wave_x * divergence,
            coeffs[1] - wave_y * divergence,
            coeffs[2] - wave_z * divergence,
        ]
    )


def cross_product(first_field, second_field):
    return jnp.stack(
        [
            first_field[1] * second_field[2] - first_field[2] * second_field[1],
            first_field[2] * second_field[0] - first_field[0] * second_field[2],
            first_field[0] * second_field[1] - first_field[1] * second_field[0],
        ]
    )


def advance(coeffs, resolution, layout):
    retained = coeffs.shape[1]
    extent = 3 * retained // 2
    wavegrid = wave_grid(retained, layout)
    fields = to_physical(coeffs, wavegrid, extent, resolution, layout)
    product = cross_product(fields[:3], fields[3:])
    nonlinear = to_spectral(product, retained, resolution, layout)
    wave_x, wave_y, wave_z = wavegrid
    squared = wave_x * wave_x + wave_y * wave_y + wave_z * wave_z
    damping = jnp.exp(-viscosity * time_step * squared)
    return damping * (coeffs + time_step * project(nonlinear, wavegrid))


def restrict(coeffs, kept, groups):
    halfway = kept // 2
    retained = coeffs.shape[1]
    rows_kept = jnp.concatenate([coeffs[:, :halfway], coeffs[:, retained - halfway :]], axis=1)
    local_rows = coeffs.shape[2]
    local_kept = kept // groups // 2
    rows_kept = jnp.concatenate(
        [rows_kept[:, :, :local_kept], rows_kept[:, :, local_rows - local_kept :]], axis=2
    )
    columns_half = coeffs.shape[3] // 2
    return jnp.concatenate(
        [rows_kept[..., :halfway], rows_kept[..., columns_half : columns_half + halfway]], axis=3
    )


def prolong(coeffs, retained, groups):
    components, kept, local_kept, width = coeffs.shape
    halfway = kept // 2
    zeros_x = jnp.zeros((components, retained - kept, local_kept, width), jnp.float32)
    wider = jnp.concatenate([coeffs[:, :halfway], zeros_x, coeffs[:, halfway:]], axis=1)
    local_rows = retained // groups
    split_rows = local_kept // 2
    zeros_y = jnp.zeros((components, retained, local_rows - local_kept, width), jnp.float32)
    wider = jnp.concatenate([wider[:, :, :split_rows], zeros_y, wider[:, :, split_rows:]], axis=2)
    zeros_z = jnp.zeros((components, retained, local_rows, retained // 2 - halfway), jnp.float32)
    return jnp.concatenate([wider[..., :halfway], zeros_z, wider[..., halfway:], zeros_z], axis=3)


def wave_table(length):
    places = np.arange(length)
    return np.where(places < length // 2, places, places - length)


def trig_table(outer, inner, extent):
    radians = 2.0 * np.pi / extent * np.mod(np.outer(outer, inner), extent)
    return np.cos(radians), np.sin(radians)


def split_table(table):
    table = np.asarray(table, np.float32)
    high = table.astype(jnp.bfloat16)
    low = (table - high.astype(np.float32)).astype(jnp.bfloat16)
    return high, low


def split(values):
    high = values.astype(jnp.bfloat16)
    low = (values - high.astype(jnp.float32)).astype(jnp.bfloat16)
    return high, low


def dot3(left, right):
    def dot(a, b):
        return jnp.dot(a, b, preferred_element_type=jnp.float32)

    return dot(left[0], right[0]) + dot(left[0], right[1]) + dot(left[1], right[0])


def z_tables(extent, retained):
    halfway = retained // 2
    columns = np.arange(retained)
    harmonic = columns % halfway
    cosine, sine = trig_table(harmonic, np.arange(extent), extent)
    table = np.where((columns < halfway)[:, None], cosine, -sine)
    weight = np.where(harmonic == 0, 1.0, 2.0)[:, None] * retained ** (-0.5)
    return table * weight, table.T * (math.sqrt(retained) / extent)


def wave_order(retained, count_py, count_pz):
    groups = count_py * count_pz
    rows, near = retained // groups, count_pz // 2
    side, band, line, z_low, inner = np.meshgrid(
        np.arange(2),
        np.arange(2),
        np.arange(count_py),
        np.arange(near),
        np.arange(rows // 2),
        indexing="ij",
    )
    owner = line * count_pz + side * near + z_low
    return ((band * (rows // 2) + inner) * groups + owner).reshape(-1)


def plane_tables(extent, retained, count_py, count_pz):
    groups = count_py * count_pz
    rows = retained // groups
    places = np.arange(retained)
    wave_in = wave_table(retained)[wave_order(retained, count_py, count_pz)]
    wave_out = wave_table(retained)[places % rows * groups + places // rows]
    cosine, sine = trig_table(np.arange(extent), wave_in, extent)
    inverse_y = np.concatenate([cosine, sine], axis=1) * retained ** (-0.5)
    cosine, sine = trig_table(wave_out, np.arange(extent), extent)
    forward_y = np.concatenate([cosine, -sine], axis=1) * (math.sqrt(retained) / extent)
    inverse_last, forward_last = z_tables(extent, retained)
    halfway = retained // 2
    lanes = np.zeros((8, retained), np.float32)
    lanes[0] = np.where(places < halfway, -1.0, 1.0)
    lanes[1] = places % halfway
    column = np.broadcast_to(wave_in[:, None], (retained, retained)).astype(np.float32)
    tables = [lanes, column]
    for table in (inverse_y, inverse_last, forward_last, forward_y):
        tables += split_table(table)
    return tables


def plane_math(fields, tables):
    lanes, wave_y, iy0, iy1, iz0, iz1, fz0, fz1, fy0, fy1 = tables
    turn, wave_z = lanes[0:1, :], lanes[1:2, :]
    retained = wave_y.shape[0]
    extent = iy0.shape[0]

    def turned(values):
        return pltpu.roll(values, retained // 2, 1) * turn

    v0, v1, v2, d1, d2 = fields
    i0 = turned(v0)
    w0 = turned(wave_y * v2 - wave_z * v1)
    w1 = wave_z * i0 - d2
    w2 = d1 - wave_y * i0
    six = (v0, v1, v2, w0, w1, w2)
    stacked = jnp.concatenate(
        [jnp.concatenate(six, axis=1), jnp.concatenate([i0] + [turned(f) for f in six[1:]], axis=1)],
        axis=0,
    )
    along_y = dot3((iy0, iy1), split(stacked))
    rows = jnp.concatenate(
        [along_y[:, f * retained : (f + 1) * retained] for f in range(6)], axis=0
    )
    physical = dot3(split(rows), (iz0, iz1))
    u0, u1, u2, w0, w1, w2 = [physical[f * extent : (f + 1) * extent] for f in range(6)]
    product = jnp.concatenate([u1 * w2 - u2 * w1, u2 * w0 - u0 * w2, u0 * w1 - u1 * w0], axis=0)
    along_z = dot3(split(product), (fz0, fz1))
    parts = [along_z[f * extent : (f + 1) * extent] for f in range(3)]
    stacked = jnp.concatenate(
        [jnp.concatenate(parts, axis=1), jnp.concatenate([turned(p) for p in parts], axis=1)],
        axis=0,
    )
    result = dot3((fy0, fy1), split(stacked))
    return [result[:, f * retained : (f + 1) * retained] for f in range(3)]


def point_place(position, side, spot, plane, near_group, planes):
    return ((position * 2 + side) * near_group + spot) * planes + plane


def x_tables(extent, retained, count_py, count_pz, halves):
    near = count_pz // 2
    near_group = count_py * near
    planes = extent // (2 * near_group * halves)
    wave_x = wave_table(retained)
    plane, spot = np.meshgrid(np.arange(planes), np.arange(near_group), indexing="ij")
    inverse = []
    for position in range(halves):
        for side in range(2):
            points = point_place(position, side, spot, plane, near_group, planes).reshape(-1)
            cosine, sine = trig_table(points, wave_x, extent)
            values = np.concatenate([cosine, sine], axis=1)
            slopes = np.concatenate([-sine * wave_x, cosine * wave_x], axis=1)
            inverse.append(np.concatenate([values, slopes], axis=0))
    inverse = np.stack(inverse) * retained ** (-0.5)
    plane, position, line, side, z_low = np.meshgrid(
        np.arange(planes),
        np.arange(halves),
        np.arange(count_py),
        np.arange(2),
        np.arange(near),
        indexing="ij",
    )
    points = point_place(position, side, line * near + z_low, plane, near_group, planes)
    points = points.reshape(planes, -1)
    early = planes - 2
    forward = []
    for some in (points[:early].reshape(-1), points[early:].reshape(-1)):
        cosine, sine = trig_table(wave_x, some, extent)
        forward.append(np.concatenate([cosine, -sine], axis=1) * (math.sqrt(retained) / extent))
    column = np.broadcast_to(wave_x[:, None], (retained, retained)).astype(np.float32)
    tables = [column]
    for table in [inverse] + forward:
        tables += split_table(table)
    return tables


def step_kernel(*refs):
    stored = refs[0]
    wave_x_ref, xi0, xi1, fa0, fa1, fb0, fb1 = refs[1:8]
    plane_refs = refs[8:18]
    out = refs[18]
    raw, modes, spread, recv, result, arrived, partial_sum = refs[19:26]
    load_sem, mode_send, own_recv, pair_recv, field_send, field_recv, back_send, back_recv = refs[26:]

    _, retained, rows, _ = stored.shape
    planes, groups = result.shape[:2]
    halves = arrived.shape[1] // groups
    count_py, count_pz = lax.axis_size("py"), lax.axis_size("pz")
    near = count_pz // 2
    near_group = count_py * near
    band = rows // 2
    pairs = planes // 2
    early = planes - 2
    position = lax.axis_index("tm")
    row, place = lax.axis_index("py"), lax.axis_index("pz")
    side, z_low = place // near, lax.rem(place, near)
    spot = row * near + z_low
    member = row * count_pz + place
    pair_place = lax.rem(place + near, count_pz)
    pair_member = row * count_pz + pair_place
    lanes = plane_refs[0]
    turn, wave_z = lanes[0:1, :], lanes[1:2, :]

    def remote(source, target, send_sem, recv_sem, device):
        return pltpu.make_async_remote_copy(
            src_ref=source,
            dst_ref=target,
            send_sem=send_sem,
            recv_sem=recv_sem,
            device_id=device,
            device_id_type=pl.DeviceIdType.MESH,
        )

    def device(half, line, z_place):
        return {"tm": half, "py": line, "pz": z_place}

    across = device(1 - position, row, place)
    beside = device(position, row, pair_place)

    def turned(values):
        return pltpu.roll(values, retained // 2, 1) * turn

    def wave_y_of(a, owner):
        place_y = a * groups + owner
        return jnp.where(place_y < retained // 2, place_y, place_y - retained).astype(jnp.float32)

    def strided(ref, f, a):
        return ref.at[f].reshape(retained * rows, retained), pl.ds(a, retained, stride=rows)

    @pl.when(position == 0)
    def _():
        pltpu.make_async_copy(stored, raw, load_sem).start()

    barrier = pltpu.get_barrier_semaphore()
    total = halves * groups
    me = position * groups + member

    def greet(step, carry):
        other = lax.rem(me + step, total)
        owner = lax.rem(other, groups)
        pl.semaphore_signal(
            barrier,
            inc=1,
            device_id=device(other // groups, owner // count_pz, lax.rem(owner, count_pz)),
            device_id_type=pl.DeviceIdType.MESH,
        )
        return carry

    lax.fori_loop(1, total, greet, 0)

    def project(values, wave_y):
        wave_x = wave_x_ref[...]
        squared = wave_x * wave_x + (wave_y * wave_y + wave_z * wave_z)
        divergence = (wave_x * values[0] + wave_y * values[1] + wave_z * values[2]) / jnp.maximum(
            squared, 1.0
        )
        projected = [
            values[0] - wave_x * divergence,
            values[1] - wave_y * divergence,
            values[2] - wave_z * divergence,
        ]
        return projected, squared

    def flat_squares(wave_y):
        squares = wave_y * wave_y + wave_z * wave_z
        return squares < 0.5, 1.0 / jnp.maximum(squares, 1.0)

    @pl.when(position == 0)
    def _():
        pltpu.make_async_copy(stored, raw, load_sem).wait()

        def first(a, carry):
            wave_y = wave_y_of(a, member)
            values = []
            for f in range(3):
                view, rows_of = strided(raw, f, a)
                values.append(view[rows_of, :])
            values, _ = project(values, wave_y)
            for f in range(3):
                view, rows_of = strided(out, f, a)
                view[rows_of, :] = values[f]
            still, inverse = flat_squares(wave_y)
            turning = (wave_y * values[2] - wave_z * values[1]) * inverse
            modes[0, a, 0:retained, :] = jnp.where(still, values[1], values[0])
            modes[0, a, retained : 2 * retained, :] = jnp.where(still, values[2], turning)
            modes[0, a, 2 * retained : 2 * retained + 8, :] = values[0][0:8]
            return carry

        lax.fori_loop(0, rows, first, 0)

    pl.semaphore_wait(barrier, total - 1)

    def rebuild(slot, a, owner):
        wave_y = wave_y_of(a, owner)
        wave_x = wave_x_ref[...]
        still, inverse = flat_squares(wave_y)
        first = modes[slot, a, 0:retained, :]
        second = modes[slot, a, retained : 2 * retained, :]
        mean = modes[slot, a, 2 * retained : 2 * retained + 1, :]
        pushed = wave_x * first
        v0 = jnp.where(still, jnp.where(wave_x == 0.0, mean, 0.0), first)
        v1 = jnp.where(still, first, -(wave_y * inverse) * pushed - wave_z * second)
        v2 = jnp.where(still, second, -(wave_z * inverse) * pushed + wave_y * second)
        return v0, v1, v2

    def own_copy(a):
        return remote(modes.at[0, a], modes.at[0, a], mode_send, own_recv.at[a], across)

    def pair_copy(a):
        return remote(modes.at[0, a], modes.at[1, a], mode_send, pair_recv.at[a], beside)

    def relay_copy(a):
        return remote(modes.at[1, a], modes.at[1, a], mode_send, pair_recv.at[a], across)

    def each(start, stop, do):
        def body(a, carry):
            do(a)
            return carry

        lax.fori_loop(start, stop, body, 0)

    def transform(step, slot, high, owner, slot_side):
        quadrant = position * 2 + side
        tables = (xi0[quadrant], xi1[quadrant])
        fields = [rebuild(slot, high * band + a, owner) for a in range(band)]
        points = planes * near_group
        for f in (1, 2, 0):
            parts = [fields[a][f] for a in range(band)]
            stacked = jnp.concatenate(
                [
                    jnp.concatenate(parts, axis=1),
                    jnp.concatenate([turned(p) for p in parts], axis=1),
                ],
                axis=0,
            )
            count = 2 if f else 1
            moved = dot3([t[: count * points] for t in tables], split(stacked))
            for p in range(planes):
                for c in range(count):
                    if f:
                        group, offset = p // 2 * 5 + p % 2 * 2 + f - 1, c
                    else:
                        group, offset = p // 2 * 5 + 4, p % 2
                    view = spread.at[step, group].reshape(near_group * rows, retained)
                    top = c * points + p * near_group
                    for a in range(band):
                        view[pl.ds(2 * a + offset, near_group, stride=rows), :] = moved[
                            top : top + near_group, a * retained : (a + 1) * retained
                        ]
        chunk = slot_side * 2 + high
        slots = chunk * near_group
        recv[:, slots + spot] = spread[step, :, spot]
        spans = [(step, 0, 5 * pairs)]
        if step == 3:
            spans = [(step + k, 5 * k, 5) for k in range(pairs)]
        for semaphore, start, count in spans:

            def push(turn_index, carry, semaphore=semaphore, start=start, count=count):
                other = lax.rem(spot + near_group - turn_index, near_group)
                remote(
                    spread.at[step, pl.ds(start, count), other],
                    recv.at[pl.ds(start, count), slots + spot],
                    field_send,
                    field_recv.at[semaphore],
                    device(position, other // near, side * near + lax.rem(other, near)),
                ).start()
                return carry

            lax.fori_loop(1, near_group, push, 0)

    @pl.when(position == 0)
    def _():
        each(band, rows, lambda a: own_copy(a).start())
        each(0, band, lambda a: pair_copy(a).start())
        each(0, band, lambda a: own_copy(a).start())

    @pl.when(position == 1)
    def _():
        def relay(a):
            own_copy(a).wait_recv()
            pair_copy(a).start()

        each(band, rows, relay)

    transform(0, 0, 1, member, side)

    def take_pair(a):
        pair_copy(a).wait_recv()
        relay_copy(a).start()

    @pl.when(position == 1)
    def _():
        def weave(a):
            take_pair(a + band)
            own_copy(a).wait_recv()

        each(0, band - 1, weave)
        own_copy(band - 1).wait_recv()

    transform(1, 0, 0, member, side)

    @pl.when(position == 0)
    def _():
        each(0, band, take_pair)

    @pl.when(position == 1)
    def _():
        take_pair(rows - 1)

    transform(2, 1, position, pair_member, 1 - side)

    @pl.when(position == 0)
    def _():
        each(band, rows, lambda a: relay_copy(a).wait_recv())

    @pl.when(position == 1)
    def _():
        each(0, band, lambda a: relay_copy(a).wait_recv())

    transform(3, 1, 1 - position, pair_member, 1 - side)

    def await_fields(semaphore, start, count):
        some = recv.at[pl.ds(start, count), pl.ds(0, near_group - 1)]
        remote(some, some, field_send, field_recv.at[semaphore], beside).wait_recv()

    for step in range(3):
        await_fields(step, 0, 5 * pairs)

    tables = [ref[...] for ref in plane_refs]

    def plane_pair(k, carry):
        await_fields(3 + k, 5 * k, 5)

        def plane(odd, carry):
            p = 2 * k + odd

            def field(group, offset):
                view = recv.at[5 * k + group].reshape(4 * near_group * rows, retained)
                return view[pl.ds(offset, retained, stride=2), :]

            v1, d1 = field(2 * odd, 0), field(2 * odd, 1)
            v2, d2 = field(2 * odd + 1, 0), field(2 * odd + 1, 1)
            v0 = field(4, odd)
            for f, values in enumerate(plane_math([v0, v1, v2, d1, d2], tables)):
                result[p, :, f] = values.reshape(groups, rows, retained)

            def push(turn_index, carry):
                to_place = lax.rem(place + near + turn_index // count_py, count_pz)
                to_row = lax.rem(row + turn_index, count_py)
                to_member = to_row * count_pz + to_place

                @pl.when(jnp.logical_or(position == 0, to_member != member))
                def _():
                    remote(
                        result.at[p, to_member],
                        arrived.at[p, position * groups + member],
                        back_send,
                        back_recv.at[p],
                        device(1, to_row, to_place),
                    ).start()

                return carry

            lax.fori_loop(0, groups, push, 0)

            @pl.when(position == 1)
            def _():
                arrived[p, groups + member] = result[p, member]

            return carry

        return lax.fori_loop(0, 2, plane, carry)

    lax.fori_loop(0, pairs, plane_pair, 0)

    def gather(start, count, a):
        view = arrived.reshape(planes * total * 3 * rows, retained)
        wide = jnp.concatenate(
            [
                view[pl.ds((start * total * 3 + f) * rows + a, count * total, stride=3 * rows), :]
                for f in range(3)
            ],
            axis=1,
        )
        back = jnp.concatenate(
            [
                turned(wide[:, f * retained : (f + 1) * retained])
                for f in range(3)
            ],
            axis=1,
        )
        return split(jnp.concatenate([wide, back], axis=0))

    @pl.when(position == 1)
    def _():
        def await_plane(p):
            some = arrived.at[p, pl.ds(0, total - 1)]
            remote(some, some, back_send, back_recv.at[p], beside).wait_recv()

        each(0, early, await_plane)

        def begin(a):
            partial_sum[a] = dot3((fa0[...], fa1[...]), gather(0, early, a))

        each(0, rows, begin)
        each(early, planes, await_plane)

        def finish(a):
            change = partial_sum[a] + dot3((fb0[...], fb1[...]), gather(early, planes - early, a))
            wave_y = wave_y_of(a, member)
            before = rebuild(0, a, member)
            values = [
                before[f] + time_step * change[:, f * retained : (f + 1) * retained]
                for f in range(3)
            ]
            values, squared = project(values, wave_y)
            damping = jnp.exp((-viscosity * time_step) * squared)
            for f in range(3):
                view, rows_of = strided(out, f, a)
                view[rows_of, :] = damping * values[f]

        each(0, rows, finish)

    some = spread.at[:, :, pl.ds(0, near_group - 1)]
    remote(some, some, field_send, field_recv.at[0], beside).wait_send()

    @pl.when(position == 0)
    def _():
        remote(modes, modes, mode_send, own_recv.at[0], beside).wait_send()
        remote(result, result, back_send, back_recv.at[0], beside).wait_send()

    @pl.when(position == 1)
    def _():
        remote(modes.at[0], modes.at[0], mode_send, own_recv.at[0], beside).wait_send()
        some = result.at[:, pl.ds(0, groups - 1)]
        remote(some, some, back_send, back_recv.at[0], beside).wait_send()


def helped_advance(stored, count_py, count_pz, halves):
    _, retained, rows, _ = stored.shape
    groups = count_py * count_pz
    extent = 3 * retained // 2
    near_group = groups // 2
    planes = extent // (groups * halves)
    pairs = planes // 2
    tables = x_tables(extent, retained, count_py, count_pz, halves)
    tables += plane_tables(extent, retained, count_py, count_pz)
    tables = [jnp.asarray(table) for table in tables]
    vmem = pl.BlockSpec(memory_space=pltpu.VMEM)
    return pl.pallas_call(
        step_kernel,
        in_specs=[pl.BlockSpec(memory_space=pl.ANY)] + [vmem] * len(tables),
        out_specs=vmem,
        out_shape=jax.ShapeDtypeStruct(stored.shape, jnp.float32),
        scratch_shapes=[
            pltpu.VMEM(stored.shape, jnp.float32),
            pltpu.VMEM((2, rows, 2 * retained + 8, retained), jnp.float32),
            pltpu.VMEM((4, 5 * pairs, near_group, rows, retained), jnp.float32),
            pltpu.VMEM((5 * pairs, 4 * near_group, rows, retained), jnp.float32),
            pltpu.VMEM((planes, groups, 3, rows, retained), jnp.float32),
            pltpu.VMEM((planes, halves * groups, 3, rows, retained), jnp.float32),
            pltpu.VMEM((rows, retained, 3 * retained), jnp.float32),
            pltpu.SemaphoreType.DMA,
            pltpu.SemaphoreType.DMA,
            pltpu.SemaphoreType.DMA((rows,)),
            pltpu.SemaphoreType.DMA((rows,)),
            pltpu.SemaphoreType.DMA,
            pltpu.SemaphoreType.DMA((3 + pairs,)),
            pltpu.SemaphoreType.DMA,
            pltpu.SemaphoreType.DMA((planes,)),
        ],
        compiler_params=pltpu.CompilerParams(
            has_side_effects=True, collective_id=0, vmem_limit_bytes=56 * 1024 * 1024
        ),
        name="step",
    )(stored, *tables)


def shards(start_states):
    count_py = lax.axis_size("py")
    count_pz = lax.axis_size("pz")
    groups = count_py * count_pz
    member = lax.axis_index("py") * count_pz + lax.axis_index("pz")
    layout = (count_py, count_pz, groups, member)
    position = lax.axis_index("tm")
    slices = lax.axis_size("tm")
    retained = start_states.shape[-1]
    stored = start_states.reshape(3, retained, start_states.shape[3], retained)
    if slices == 2:
        result = helped_advance(stored, count_py, count_pz, slices)
        return result.reshape(1, 3, retained, stored.shape[2], 1, retained)
    spectral_state = project(stored, wave_grid(retained, layout))
    fine_end = advance(spectral_state, "fine", layout)
    coarse_start = restrict(spectral_state, M, groups)
    coarse_next = advance(coarse_start, "coarse", layout)
    fine_low = restrict(fine_end, M, groups)
    correction = fine_low - coarse_next

    def relay(chained):
        return shifted(chained, "tm", 1)

    current = jnp.where(position == 1, relay(fine_low), coarse_start)

    def sweep_turn(turn_index, current):
        candidate = advance(current, "coarse", layout) + correction
        arrived = relay(candidate)
        return jnp.where(position == turn_index + 1, arrived, current)

    current = lax.fori_loop(1, slices - 1, sweep_turn, current)
    upper_band = fine_end - prolong(fine_low, retained, groups)
    previous = shifted(upper_band, "tm", 1)
    updated = prolong(current, retained, groups) + previous
    result = jnp.where(position == 0, spectral_state, updated)
    return result.reshape(1, result.shape[0], retained, result.shape[2], 1, retained)


def solution(mesh):
    in_specs = (P("tm", None, None, None, ("py", "pz"), None),)
    out_specs = P("tm", None, None, None, ("py", "pz"), None)
    return jax.shard_map(shards, mesh=mesh, in_specs=in_specs, out_specs=out_specs, check_vma=False)
```

```python
from functools import partial
import math

import jax
import jax.numpy as jnp
from jax import lax
import numpy as np
from jax.experimental import pallas as pl
from jax.experimental.pallas import tpu as pltpu
from jax.sharding import PartitionSpec as P

M = 64


viscosity = 0.03
time_step = 0.004
highest = lax.Precision.HIGHEST


def shifted(block, axis, distance):
    devices = range(lax.axis_size(axis))
    route = [(i - distance, i) for i in devices if i - distance in devices]
    return lax.ppermute(block, axis, route)


def signed_wave(places, length):
    return jnp.where(places < length // 2, places, places - length)


def rotate(values):
    halfway = values.shape[-1] // 2
    return jnp.concatenate([-values[..., halfway:], values[..., :halfway]], axis=-1)


def trig_pair(outer, inner, extent, factor):
    residue = jnp.mod(outer[:, None] * inner[None, :], extent)
    radians = residue.astype(jnp.float32) * (2.0 * math.pi / extent)
    return (jnp.cos(radians) * factor, jnp.sin(radians) * factor)


def complex_apply(cosine_part, sine_part, values, contracted, direction_sign):
    kernel = jnp.stack(
        [
            jnp.stack([cosine_part, -direction_sign * sine_part]),
            jnp.stack([direction_sign * sine_part, cosine_part]),
        ]
    )
    halfway = values.shape[-1] // 2
    split = values.reshape(values.shape[:-1] + (2, halfway))
    if contracted == 1:
        pattern = "pqok,fkaqh->foaph"
    else:
        pattern = "pqok,flkqh->floph"
    result = jnp.einsum(pattern, kernel, split, precision=highest)
    return result.reshape(result.shape[:-2] + (2 * halfway,))


def inverse_z(extent, retained):
    halfway = retained // 2
    columns = jnp.arange(retained, dtype=jnp.int32)
    harmonic = columns % halfway
    weight = jnp.where(harmonic == 0, 1.0, 2.0) * retained ** (-0.5)
    residue = jnp.mod(harmonic[:, None] * jnp.arange(extent, dtype=jnp.int32)[None, :], extent)
    radians = residue.astype(jnp.float32) * (2.0 * math.pi / extent)
    return (
        jnp.where((columns < halfway)[:, None], jnp.cos(radians), -jnp.sin(radians))
        * weight[:, None]
    )


def forward_z(extent, retained):
    halfway = retained // 2
    columns = jnp.arange(retained, dtype=jnp.int32)
    harmonic = columns % halfway
    residue = jnp.mod(jnp.arange(extent, dtype=jnp.int32)[:, None] * harmonic[None, :], extent)
    radians = residue.astype(jnp.float32) * (2.0 * math.pi / extent)
    return jnp.where((columns < halfway)[None, :], jnp.cos(radians), -jnp.sin(radians)) * (
        math.sqrt(retained) / extent
    )


def inverse_tail(portion, extent, sectioned, layout):
    count_py, count_pz, groups, member = layout
    retained = portion.shape[2]
    local_rows = retained // groups
    places = jnp.arange(retained, dtype=jnp.int32)
    owners = places // local_rows
    wave_y = signed_wave(places % local_rows * groups + owners, retained)
    points = jnp.arange(extent, dtype=jnp.int32)
    cosine_part, sine_part = trig_pair(points, wave_y, extent, retained ** (-0.5))
    along_y = complex_apply(cosine_part, sine_part, portion, 2, 1.0)
    return jnp.einsum("flyr,rz->flyz", along_y, inverse_z(extent, retained), precision=highest)


def forward_tail(portion, retained, sectioned, layout):
    count_py, count_pz, groups, member = layout
    extent = portion.shape[1]
    local_rows = extent // groups
    places = jnp.arange(extent, dtype=jnp.int32)
    points = places // local_rows * local_rows + places % local_rows
    wave_x = signed_wave(jnp.arange(retained, dtype=jnp.int32), retained)
    cosine_part, sine_part = trig_pair(wave_x, points, extent, math.sqrt(retained) / extent)
    return complex_apply(cosine_part, sine_part, portion, 1, -1.0)


def to_physical(coeffs, wavegrid, extent, resolution, layout):
    wave_x, wave_y, wave_z = wavegrid
    retained = coeffs.shape[1]
    seeds = jnp.concatenate([coeffs, wave_x * coeffs[1:3]], axis=0)
    points = jnp.arange(extent, dtype=jnp.int32)
    wave_rows = signed_wave(jnp.arange(retained, dtype=jnp.int32), retained)
    cosine_part, sine_part = trig_pair(points, wave_rows, extent, retained ** (-0.5))
    moved_x = complex_apply(cosine_part, sine_part, seeds, 1, 1.0)
    curl_x = rotate(wave_y * moved_x[2] - wave_z * moved_x[1])
    curl_y = rotate(wave_z * moved_x[0] - moved_x[4])
    curl_z = rotate(moved_x[3] - wave_y * moved_x[0])
    spread = jnp.concatenate([moved_x[:3], jnp.stack([curl_x, curl_y, curl_z])], axis=0)
    if resolution == "coarse":
        finish = partial(inverse_tail, extent=extent, sectioned=False, layout=layout)
        return finish(lax.all_to_all(spread, ("py", "pz"), split_axis=1, concat_axis=2, tiled=True))
    else:
        finish = partial(inverse_tail, extent=extent, sectioned=False, layout=layout)
        return finish(lax.all_to_all(spread, ("py", "pz"), split_axis=1, concat_axis=2, tiled=True))


def to_spectral(fields, retained, resolution, layout):
    count_py, count_pz, groups, member = layout
    extent = fields.shape[-1]
    along_z = jnp.einsum("flyz,zr->flyr", fields, forward_z(extent, retained), precision=highest)
    local_rows = retained // groups
    places = jnp.arange(retained, dtype=jnp.int32)
    wave_y = signed_wave(places % local_rows * groups + places // local_rows, retained)
    cosine_part, sine_part = trig_pair(
        wave_y, jnp.arange(extent, dtype=jnp.int32), extent, math.sqrt(retained) / extent
    )
    along_y = complex_apply(cosine_part, sine_part, along_z, 2, -1.0)
    if resolution == "coarse":
        finish = partial(forward_tail, retained=retained, sectioned=False, layout=layout)
        return finish(
            lax.all_to_all(along_y, ("py", "pz"), split_axis=2, concat_axis=1, tiled=True)
        )
    else:
        finish = partial(forward_tail, retained=retained, sectioned=False, layout=layout)
        return finish(
            lax.all_to_all(along_y, ("py", "pz"), split_axis=2, concat_axis=1, tiled=True)
        )


def wave_grid(retained, layout):
    count_py, count_pz, groups, member = layout
    places = jnp.arange(retained, dtype=jnp.int32)
    wave_x = signed_wave(places, retained).astype(jnp.float32)[:, None, None]
    local_places = jnp.arange(retained // groups, dtype=jnp.int32)
    wave_y = signed_wave(local_places * groups + member, retained).astype(jnp.float32)[
        None, :, None
    ]
    wave_z = (places % (retained // 2)).astype(jnp.float32)[None, None, :]
    return (wave_x, wave_y, wave_z)


def project(coeffs, wavegrid):
    wave_x, wave_y, wave_z = wavegrid
    squared = wave_x * wave_x + wave_y * wave_y + wave_z * wave_z
    divergence = (wave_x * coeffs[0] + wave_y * coeffs[1] + wave_z * coeffs[2]) / jnp.maximum(
        squared, 1.0
    )
    return jnp.stack(
        [
            coeffs[0] - wave_x * divergence,
            coeffs[1] - wave_y * divergence,
            coeffs[2] - wave_z * divergence,
        ]
    )


def cross_product(first_field, second_field):
    return jnp.stack(
        [
            first_field[1] * second_field[2] - first_field[2] * second_field[1],
            first_field[2] * second_field[0] - first_field[0] * second_field[2],
            first_field[0] * second_field[1] - first_field[1] * second_field[0],
        ]
    )


def advance(coeffs, resolution, layout):
    retained = coeffs.shape[1]
    extent = 3 * retained // 2
    wavegrid = wave_grid(retained, layout)
    fields = to_physical(coeffs, wavegrid, extent, resolution, layout)
    product = cross_product(fields[:3], fields[3:])
    nonlinear = to_spectral(product, retained, resolution, layout)
    wave_x, wave_y, wave_z = wavegrid
    squared = wave_x * wave_x + wave_y * wave_y + wave_z * wave_z
    damping = jnp.exp(-viscosity * time_step * squared)
    return damping * (coeffs + time_step * project(nonlinear, wavegrid))


def restrict(coeffs, kept, groups):
    halfway = kept // 2
    retained = coeffs.shape[1]
    rows_kept = jnp.concatenate([coeffs[:, :halfway], coeffs[:, retained - halfway :]], axis=1)
    local_rows = coeffs.shape[2]
    local_kept = kept // groups // 2
    rows_kept = jnp.concatenate(
        [rows_kept[:, :, :local_kept], rows_kept[:, :, local_rows - local_kept :]], axis=2
    )
    columns_half = coeffs.shape[3] // 2
    return jnp.concatenate(
        [rows_kept[..., :halfway], rows_kept[..., columns_half : columns_half + halfway]], axis=3
    )


def prolong(coeffs, retained, groups):
    components, kept, local_kept, width = coeffs.shape
    halfway = kept // 2
    zeros_x = jnp.zeros((components, retained - kept, local_kept, width), jnp.float32)
    wider = jnp.concatenate([coeffs[:, :halfway], zeros_x, coeffs[:, halfway:]], axis=1)
    local_rows = retained // groups
    split_rows = local_kept // 2
    zeros_y = jnp.zeros((components, retained, local_rows - local_kept, width), jnp.float32)
    wider = jnp.concatenate([wider[:, :, :split_rows], zeros_y, wider[:, :, split_rows:]], axis=2)
    zeros_z = jnp.zeros((components, retained, local_rows, retained // 2 - halfway), jnp.float32)
    return jnp.concatenate([wider[..., :halfway], zeros_z, wider[..., halfway:], zeros_z], axis=3)


def wave_table(length):
    places = np.arange(length)
    return np.where(places < length // 2, places, places - length)


def trig_table(outer, inner, extent):
    radians = 2.0 * np.pi / extent * np.mod(np.outer(outer, inner), extent)
    return np.cos(radians), np.sin(radians)


def split_table(table):
    table = np.asarray(table, np.float32)
    high = table.astype(jnp.bfloat16)
    low = (table - high.astype(np.float32)).astype(jnp.bfloat16)
    return high, low


def split(values):
    high = values.astype(jnp.bfloat16)
    low = (values - high.astype(jnp.float32)).astype(jnp.bfloat16)
    return high, low


def dot3(left, right):
    def dot(a, b):
        return jnp.dot(a, b, preferred_element_type=jnp.float32)

    return dot(left[0], right[0]) + dot(left[0], right[1]) + dot(left[1], right[0])


def z_tables(extent, retained):
    halfway = retained // 2
    columns = np.arange(retained)
    harmonic = columns % halfway
    cosine, sine = trig_table(harmonic, np.arange(extent), extent)
    table = np.where((columns < halfway)[:, None], cosine, -sine)
    weight = np.where(harmonic == 0, 1.0, 2.0)[:, None] * retained ** (-0.5)
    return table * weight, table.T * (math.sqrt(retained) / extent)


def wave_order(retained, count_py, count_pz):
    groups = count_py * count_pz
    rows, near = retained // groups, count_pz // 2
    side, band, line, z_low, inner = np.meshgrid(
        np.arange(2),
        np.arange(2),
        np.arange(count_py),
        np.arange(near),
        np.arange(rows // 2),
        indexing="ij",
    )
    owner = line * count_pz + side * near + z_low
    return ((band * (rows // 2) + inner) * groups + owner).reshape(-1)


def plane_tables(extent, retained, count_py, count_pz):
    groups = count_py * count_pz
    rows = retained // groups
    places = np.arange(retained)
    wave_in = wave_table(retained)[wave_order(retained, count_py, count_pz)]
    wave_out = wave_table(retained)[places % rows * groups + places // rows]
    cosine, sine = trig_table(np.arange(extent), wave_in, extent)
    inverse_y = np.concatenate([cosine, sine], axis=1) * retained ** (-0.5)
    cosine, sine = trig_table(wave_out, np.arange(extent), extent)
    forward_y = np.concatenate([cosine, -sine], axis=1) * (math.sqrt(retained) / extent)
    inverse_last, forward_last = z_tables(extent, retained)
    halfway = retained // 2
    lanes = np.zeros((8, retained), np.float32)
    lanes[0] = np.where(places < halfway, -1.0, 1.0)
    lanes[1] = places % halfway
    column = np.broadcast_to(wave_in[:, None], (retained, retained)).astype(np.float32)
    tables = [lanes, column]
    for table in (inverse_y, inverse_last, forward_last, forward_y):
        tables += split_table(table)
    return tables


def plane_math(fields, tables):
    lanes, wave_y, iy0, iy1, iz0, iz1, fz0, fz1, fy0, fy1 = tables
    turn, wave_z = lanes[0:1, :], lanes[1:2, :]
    retained = wave_y.shape[0]
    extent = iy0.shape[0]

    def turned(values):
        return pltpu.roll(values, retained // 2, 1) * turn

    v0, v1, v2, d1, d2 = fields
    i0 = turned(v0)
    w0 = turned(wave_y * v2 - wave_z * v1)
    w1 = wave_z * i0 - d2
    w2 = d1 - wave_y * i0
    six = (v0, v1, v2, w0, w1, w2)
    stacked = jnp.concatenate(
        [jnp.concatenate(six, axis=1), jnp.concatenate([i0] + [turned(f) for f in six[1:]], axis=1)],
        axis=0,
    )
    along_y = dot3((iy0, iy1), split(stacked))
    rows = jnp.concatenate(
        [along_y[:, f * retained : (f + 1) * retained] for f in range(6)], axis=0
    )
    physical = dot3(split(rows), (iz0, iz1))
    u0, u1, u2, w0, w1, w2 = [physical[f * extent : (f + 1) * extent] for f in range(6)]
    product = jnp.concatenate([u1 * w2 - u2 * w1, u2 * w0 - u0 * w2, u0 * w1 - u1 * w0], axis=0)
    along_z = dot3(split(product), (fz0, fz1))
    parts = [along_z[f * extent : (f + 1) * extent] for f in range(3)]
    stacked = jnp.concatenate(
        [jnp.concatenate(parts, axis=1), jnp.concatenate([turned(p) for p in parts], axis=1)],
        axis=0,
    )
    result = dot3((fy0, fy1), split(stacked))
    return [result[:, f * retained : (f + 1) * retained] for f in range(3)]


def point_place(position, side, spot, plane, near_group, planes):
    return ((position * 2 + side) * near_group + spot) * planes + plane


def x_tables(extent, retained, count_py, count_pz, halves):
    near = count_pz // 2
    near_group = count_py * near
    planes = extent // (2 * near_group * halves)
    wave_x = wave_table(retained)
    plane, spot = np.meshgrid(np.arange(planes), np.arange(near_group), indexing="ij")
    inverse = []
    for position in range(halves):
        for side in range(2):
            points = point_place(position, side, spot, plane, near_group, planes).reshape(-1)
            cosine, sine = trig_table(points, wave_x, extent)
            values = np.concatenate([cosine, sine], axis=1)
            slopes = np.concatenate([-sine * wave_x, cosine * wave_x], axis=1)
            inverse.append(np.concatenate([values, slopes], axis=0))
    inverse = np.stack(inverse) * retained ** (-0.5)
    plane, position, line, side, z_low = np.meshgrid(
        np.arange(planes),
        np.arange(halves),
        np.arange(count_py),
        np.arange(2),
        np.arange(near),
        indexing="ij",
    )
    points = point_place(position, side, line * near + z_low, plane, near_group, planes)
    points = points.reshape(planes, -1)
    early = planes - 2
    forward = []
    for some in (points[:early].reshape(-1), points[early:].reshape(-1)):
        cosine, sine = trig_table(wave_x, some, extent)
        forward.append(np.concatenate([cosine, -sine], axis=1) * (math.sqrt(retained) / extent))
    column = np.broadcast_to(wave_x[:, None], (retained, retained)).astype(np.float32)
    tables = [column]
    for table in [inverse] + forward:
        tables += split_table(table)
    return tables


def step_kernel(*refs):
    stored = refs[0]
    kept_tables = refs[1:18]
    out = refs[18]
    loaded = refs[19:36]
    wave_x_ref, xi0, xi1, fa0, fa1, fb0, fb1 = loaded[:7]
    plane_refs = loaded[7:]
    raw, modes, spread, recv, result, arrived, partial_sum = refs[36:43]
    load_sem, table_sem, mode_send, own_recv, pair_recv = refs[43:48]
    field_send, field_recv, back_send, back_recv, ready = refs[48:]

    _, retained, rows, _ = stored.shape
    planes, groups = result.shape[:2]
    halves = arrived.shape[1] // groups
    count_py, count_pz = lax.axis_size("py"), lax.axis_size("pz")
    near = count_pz // 2
    near_group = count_py * near
    band = rows // 2
    pairs = planes // 2
    early = planes - 2
    position = lax.axis_index("tm")
    row, place = lax.axis_index("py"), lax.axis_index("pz")
    side, z_low = place // near, lax.rem(place, near)
    spot = row * near + z_low
    member = row * count_pz + place
    pair_place = lax.rem(place + near, count_pz)
    pair_member = row * count_pz + pair_place

    def remote(source, target, send_sem, recv_sem, device):
        return pltpu.make_async_remote_copy(
            src_ref=source,
            dst_ref=target,
            send_sem=send_sem,
            recv_sem=recv_sem,
            device_id=device,
            device_id_type=pl.DeviceIdType.MESH,
        )

    def device(half, line, z_place):
        return {"tm": half, "py": line, "pz": z_place}

    across = device(1 - position, row, place)
    beside = device(position, row, pair_place)

    def turned(values):
        return pltpu.roll(values, retained // 2, 1) * turn

    def wave_y_of(a, owner):
        place_y = a * groups + owner
        return jnp.where(place_y < retained // 2, place_y, place_y - retained).astype(jnp.float32)

    def strided(ref, f, a):
        return ref.at[f].reshape(retained * rows, retained), pl.ds(a, retained, stride=rows)

    total = halves * groups
    barrier = pltpu.get_barrier_semaphore()

    def hello(other):
        pl.semaphore_signal(
            barrier, inc=1, device_id=other, device_id_type=pl.DeviceIdType.MESH
        )

    def greet(step, carry):
        other = lax.rem(spot + step, near_group)
        hello(device(position, other // near, side * near + lax.rem(other, near)))
        return carry

    hello(across)
    hello(beside)
    lax.fori_loop(1, near_group, greet, 0)

    @pl.when(position == 0)
    def _():
        pltpu.make_async_copy(stored, raw, load_sem).start()

    loads = [
        pltpu.make_async_copy(source, target, table_sem.at[i])
        for i, (source, target) in enumerate(zip(kept_tables, loaded))
    ]
    for load in loads:
        load.start()
    for load in loads:
        load.wait()
    lanes = plane_refs[0]
    turn, wave_z = lanes[0:1, :], lanes[1:2, :]

    def project(values, wave_y):
        wave_x = wave_x_ref[...]
        squared = wave_x * wave_x + (wave_y * wave_y + wave_z * wave_z)
        divergence = (wave_x * values[0] + wave_y * values[1] + wave_z * values[2]) / jnp.maximum(
            squared, 1.0
        )
        projected = [
            values[0] - wave_x * divergence,
            values[1] - wave_y * divergence,
            values[2] - wave_z * divergence,
        ]
        return projected, squared

    def flat_squares(wave_y):
        squares = wave_y * wave_y + wave_z * wave_z
        return squares < 0.5, 1.0 / jnp.maximum(squares, 1.0)

    @pl.when(position == 0)
    def _():
        pltpu.make_async_copy(stored, raw, load_sem).wait()

        def first(a, carry):
            wave_y = wave_y_of(a, member)
            values = []
            for f in range(3):
                view, rows_of = strided(raw, f, a)
                values.append(view[rows_of, :])
            values, _ = project(values, wave_y)
            for f in range(3):
                view, rows_of = strided(out, f, a)
                view[rows_of, :] = values[f]
            still, inverse = flat_squares(wave_y)
            turning = (wave_y * values[2] - wave_z * values[1]) * inverse
            modes[0, a, 0:retained, :] = jnp.where(still, values[1], values[0])
            modes[0, a, retained : 2 * retained, :] = jnp.where(still, values[2], turning)
            modes[0, a, 2 * retained : 2 * retained + 8, :] = values[0][0:8]
            return carry

        lax.fori_loop(0, rows, first, 0)

    pl.semaphore_wait(barrier, near_group + 1)

    def rebuild(slot, a, owner):
        wave_y = wave_y_of(a, owner)
        wave_x = wave_x_ref[...]
        still, inverse = flat_squares(wave_y)
        first = modes[slot, a, 0:retained, :]
        second = modes[slot, a, retained : 2 * retained, :]
        mean = modes[slot, a, 2 * retained : 2 * retained + 1, :]
        pushed = wave_x * first
        v0 = jnp.where(still, jnp.where(wave_x == 0.0, mean, 0.0), first)
        v1 = jnp.where(still, first, -(wave_y * inverse) * pushed - wave_z * second)
        v2 = jnp.where(still, second, -(wave_z * inverse) * pushed + wave_y * second)
        return v0, v1, v2

    def own_copy(a):
        return remote(modes.at[0, a], modes.at[0, a], mode_send, own_recv.at[a], across)

    def pair_copy(a):
        return remote(modes.at[0, a], modes.at[1, a], mode_send, pair_recv.at[a], beside)

    def relay_copy(a):
        return remote(modes.at[1, a], modes.at[1, a], mode_send, pair_recv.at[a], across)

    def each(start, stop, do):
        def body(a, carry):
            do(a)
            return carry

        lax.fori_loop(start, stop, body, 0)

    def transform(step, slot, high, owner, slot_side):
        quadrant = position * 2 + side
        tables = (xi0[quadrant], xi1[quadrant])
        fields = [rebuild(slot, high * band + a, owner) for a in range(band)]
        points = planes * near_group
        for f in (1, 2, 0):
            parts = [fields[a][f] for a in range(band)]
            stacked = jnp.concatenate(
                [
                    jnp.concatenate(parts, axis=1),
                    jnp.concatenate([turned(p) for p in parts], axis=1),
                ],
                axis=0,
            )
            count = 2 if f else 1
            moved = dot3([t[: count * points] for t in tables], split(stacked))
            for p in range(planes):
                for c in range(count):
                    if f:
                        group, offset = p // 2 * 5 + p % 2 * 2 + f - 1, c
                    else:
                        group, offset = p // 2 * 5 + 4, p % 2
                    view = spread.at[step, group].reshape(near_group * rows, retained)
                    top = c * points + p * near_group
                    for a in range(band):
                        view[pl.ds(2 * a + offset, near_group, stride=rows), :] = moved[
                            top : top + near_group, a * retained : (a + 1) * retained
                        ]
        chunk = slot_side * 2 + high
        slots = chunk * near_group
        recv[:, slots + spot] = spread[step, :, spot]
        spans = [(step, 0, 5 * pairs)]
        if step == 3:
            spans = [(step + k, 5 * k, 5) for k in range(pairs)]
        for semaphore, start, count in spans:

            def push(turn_index, carry, semaphore=semaphore, start=start, count=count):
                other = lax.rem(spot + near_group - turn_index, near_group)
                remote(
                    spread.at[step, pl.ds(start, count), other],
                    recv.at[pl.ds(start, count), slots + spot],
                    field_send,
                    field_recv.at[semaphore],
                    device(position, other // near, side * near + lax.rem(other, near)),
                ).start()
                return carry

            lax.fori_loop(1, near_group, push, 0)

    def take_own(a):
        own_copy(a).wait_recv()
        pair_copy(a).start()

    def take_pair(a):
        pair_copy(a).wait_recv()
        relay_copy(a).start()

    @pl.when(position == 0)
    def _():
        each(band + 1, rows, lambda a: own_copy(a).start())
        own_copy(band).start()
        own_copy(band - 1).start()
        each(0, band - 1, lambda a: own_copy(a).start())
        each(0, band // 2, lambda a: pair_copy(a).start())

    @pl.when(position == 1)
    def _():
        each(band + 1, rows, take_own)
        take_own(band)

    transform(0, 0, 1, member, side)

    @pl.when(position == 0)
    def _():
        each(band // 2, band, lambda a: pair_copy(a).start())

    @pl.when(position == 1)
    def _():
        take_own(band - 1)

        def weave(a):
            take_pair(a + band + 1)
            own_copy(a).wait_recv()

        each(0, band - 1, weave)

    transform(1, 0, 0, member, side)

    @pl.when(position == 0)
    def _():
        pair_copy(band).start()
        each(0, band - 1, take_pair)
        pair_copy(band - 1).wait_recv()

    @pl.when(position == 1)
    def _():
        pair_copy(band).wait_recv()

    transform(2, 1, position, pair_member, 1 - side)

    @pl.when(position == 0)
    def _():
        each(band, rows, lambda a: pair_copy(a).wait_recv())

    @pl.when(position == 1)
    def _():
        each(0, band, lambda a: pair_copy(a).wait_recv())

    transform(3, 1, 1 - position, pair_member, 1 - side)

    def await_fields(semaphore, start, count):
        some = recv.at[pl.ds(start, count), pl.ds(0, near_group - 1)]
        remote(some, some, field_send, field_recv.at[semaphore], beside).wait_recv()

    for step in range(3):
        await_fields(step, 0, 5 * pairs)

    tables = [ref[...] for ref in plane_refs]

    def plane_pair(k, carry):
        await_fields(3 + k, 5 * k, 5)

        @pl.when(jnp.logical_and(position == 1, k == 0))
        def _():
            pl.semaphore_signal(
                ready, inc=1, device_id=across, device_id_type=pl.DeviceIdType.MESH
            )

        def plane(odd, carry):
            p = 2 * k + odd

            def field(group, offset):
                view = recv.at[5 * k + group].reshape(4 * near_group * rows, retained)
                return view[pl.ds(offset, retained, stride=2), :]

            v1, d1 = field(2 * odd, 0), field(2 * odd, 1)
            v2, d2 = field(2 * odd + 1, 0), field(2 * odd + 1, 1)
            v0 = field(4, odd)
            for f, values in enumerate(plane_math([v0, v1, v2, d1, d2], tables)):
                result[p, :, f] = values.reshape(groups, rows, retained)

            @pl.when(jnp.logical_and(position == 0, p == 0))
            def _():
                pl.semaphore_wait(ready, 1)

            def push(turn_index, carry):
                to_place = lax.rem(place + near + turn_index // count_py, count_pz)
                to_row = lax.rem(row + turn_index, count_py)
                to_member = to_row * count_pz + to_place

                @pl.when(jnp.logical_or(position == 0, to_member != member))
                def _():
                    remote(
                        result.at[p, to_member],
                        arrived.at[p, position * groups + member],
                        back_send,
                        back_recv.at[p],
                        device(1, to_row, to_place),
                    ).start()

                return carry

            lax.fori_loop(0, groups, push, 0)

            @pl.when(position == 1)
            def _():
                arrived[p, groups + member] = result[p, member]

            return carry

        return lax.fori_loop(0, 2, plane, carry)

    lax.fori_loop(0, pairs, plane_pair, 0)

    def gather(start, count, a):
        view = arrived.reshape(planes * total * 3 * rows, retained)
        wide = jnp.concatenate(
            [
                view[pl.ds((start * total * 3 + f) * rows + a, count * total, stride=3 * rows), :]
                for f in range(3)
            ],
            axis=1,
        )
        back = jnp.concatenate(
            [
                turned(wide[:, f * retained : (f + 1) * retained])
                for f in range(3)
            ],
            axis=1,
        )
        return split(jnp.concatenate([wide, back], axis=0))

    @pl.when(position == 1)
    def _():
        def await_plane(p):
            some = arrived.at[p, pl.ds(0, total - 1)]
            remote(some, some, back_send, back_recv.at[p], beside).wait_recv()

        each(0, early, await_plane)

        def begin(a):
            before = jnp.concatenate(rebuild(0, a, member), axis=1)
            change = dot3((fa0[...], fa1[...]), gather(0, early, a))
            partial_sum[a] = before + time_step * change

        each(0, rows, begin)
        each(early, planes, await_plane)

        def finish(a):
            change = dot3((fb0[...], fb1[...]), gather(early, planes - early, a))
            after = partial_sum[a] + time_step * change
            values, squared = project(
                [after[:, f * retained : (f + 1) * retained] for f in range(3)],
                wave_y_of(a, member),
            )
            damping = jnp.exp((-viscosity * time_step) * squared)
            for f in range(3):
                view, rows_of = strided(out, f, a)
                view[rows_of, :] = damping * values[f]

        each(0, rows, finish)

    some = spread.at[:, :, pl.ds(0, near_group - 1)]
    remote(some, some, field_send, field_recv.at[0], beside).wait_send()

    @pl.when(position == 0)
    def _():
        remote(modes, modes, mode_send, own_recv.at[0], beside).wait_send()
        remote(result, result, back_send, back_recv.at[0], beside).wait_send()

    @pl.when(position == 1)
    def _():
        remote(modes.at[0], modes.at[0], mode_send, own_recv.at[0], beside).wait_send()
        some = result.at[:, pl.ds(0, groups - 1)]
        remote(some, some, back_send, back_recv.at[0], beside).wait_send()


def helped_advance(stored, count_py, count_pz, halves):
    _, retained, rows, _ = stored.shape
    groups = count_py * count_pz
    extent = 3 * retained // 2
    near_group = groups // 2
    planes = extent // (groups * halves)
    pairs = planes // 2
    tables = x_tables(extent, retained, count_py, count_pz, halves)
    tables += plane_tables(extent, retained, count_py, count_pz)
    tables = [jnp.asarray(table) for table in tables]
    vmem = pl.BlockSpec(memory_space=pltpu.VMEM)
    return pl.pallas_call(
        step_kernel,
        in_specs=[pl.BlockSpec(memory_space=pl.ANY)] * (1 + len(tables)),
        out_specs=vmem,
        out_shape=jax.ShapeDtypeStruct(stored.shape, jnp.float32),
        scratch_shapes=[pltpu.VMEM(table.shape, table.dtype) for table in tables]
        + [
            pltpu.VMEM(stored.shape, jnp.float32),
            pltpu.VMEM((2, rows, 2 * retained + 8, retained), jnp.float32),
            pltpu.VMEM((4, 5 * pairs, near_group, rows, retained), jnp.float32),
            pltpu.VMEM((5 * pairs, 4 * near_group, rows, retained), jnp.float32),
            pltpu.VMEM((planes, groups, 3, rows, retained), jnp.float32),
            pltpu.VMEM((planes, halves * groups, 3, rows, retained), jnp.float32),
            pltpu.VMEM((rows, retained, 3 * retained), jnp.float32),
            pltpu.SemaphoreType.DMA,
            pltpu.SemaphoreType.DMA((len(tables),)),
            pltpu.SemaphoreType.DMA,
            pltpu.SemaphoreType.DMA((rows,)),
            pltpu.SemaphoreType.DMA((rows,)),
            pltpu.SemaphoreType.DMA,
            pltpu.SemaphoreType.DMA((3 + pairs,)),
            pltpu.SemaphoreType.DMA,
            pltpu.SemaphoreType.DMA((planes,)),
            pltpu.SemaphoreType.REGULAR,
        ],
        compiler_params=pltpu.CompilerParams(
            has_side_effects=True, collective_id=0, vmem_limit_bytes=56 * 1024 * 1024
        ),
        name="step",
    )(stored, *tables)


def shards(start_states):
    count_py = lax.axis_size("py")
    count_pz = lax.axis_size("pz")
    groups = count_py * count_pz
    member = lax.axis_index("py") * count_pz + lax.axis_index("pz")
    layout = (count_py, count_pz, groups, member)
    position = lax.axis_index("tm")
    slices = lax.axis_size("tm")
    retained = start_states.shape[-1]
    stored = start_states.reshape(3, retained, start_states.shape[3], retained)
    if slices == 2:
        result = helped_advance(stored, count_py, count_pz, slices)
        return result.reshape(1, 3, retained, stored.shape[2], 1, retained)
    spectral_state = project(stored, wave_grid(retained, layout))
    fine_end = advance(spectral_state, "fine", layout)
    coarse_start = restrict(spectral_state, M, groups)
    coarse_next = advance(coarse_start, "coarse", layout)
    fine_low = restrict(fine_end, M, groups)
    correction = fine_low - coarse_next

    def relay(chained):
        return shifted(chained, "tm", 1)

    current = jnp.where(position == 1, relay(fine_low), coarse_start)

    def sweep_turn(turn_index, current):
        candidate = advance(current, "coarse", layout) + correction
        arrived = relay(candidate)
        return jnp.where(position == turn_index + 1, arrived, current)

    current = lax.fori_loop(1, slices - 1, sweep_turn, current)
    upper_band = fine_end - prolong(fine_low, retained, groups)
    previous = shifted(upper_band, "tm", 1)
    updated = prolong(current, retained, groups) + previous
    result = jnp.where(position == 0, spectral_state, updated)
    return result.reshape(1, result.shape[0], retained, result.shape[2], 1, retained)


def solution(mesh):
    in_specs = (P("tm", None, None, None, ("py", "pz"), None),)
    out_specs = P("tm", None, None, None, ("py", "pz"), None)
    return jax.shard_map(shards, mesh=mesh, in_specs=in_specs, out_specs=out_specs, check_vma=False)
```

```python
from functools import partial
import math

import jax
import jax.numpy as jnp
from jax import lax
import numpy as np
from jax.experimental import pallas as pl
from jax.experimental.pallas import tpu as pltpu
from jax.sharding import PartitionSpec as P

M = 64


viscosity = 0.03
time_step = 0.004
highest = lax.Precision.HIGHEST


def shifted(block, axis, distance):
    devices = range(lax.axis_size(axis))
    route = [(i - distance, i) for i in devices if i - distance in devices]
    return lax.ppermute(block, axis, route)


def signed_wave(places, length):
    return jnp.where(places < length // 2, places, places - length)


def rotate(values):
    halfway = values.shape[-1] // 2
    return jnp.concatenate([-values[..., halfway:], values[..., :halfway]], axis=-1)


def trig_pair(outer, inner, extent, factor):
    residue = jnp.mod(outer[:, None] * inner[None, :], extent)
    radians = residue.astype(jnp.float32) * (2.0 * math.pi / extent)
    return (jnp.cos(radians) * factor, jnp.sin(radians) * factor)


def complex_apply(cosine_part, sine_part, values, contracted, direction_sign):
    kernel = jnp.stack(
        [
            jnp.stack([cosine_part, -direction_sign * sine_part]),
            jnp.stack([direction_sign * sine_part, cosine_part]),
        ]
    )
    halfway = values.shape[-1] // 2
    split = values.reshape(values.shape[:-1] + (2, halfway))
    if contracted == 1:
        pattern = "pqok,fkaqh->foaph"
    else:
        pattern = "pqok,flkqh->floph"
    result = jnp.einsum(pattern, kernel, split, precision=highest)
    return result.reshape(result.shape[:-2] + (2 * halfway,))


def inverse_z(extent, retained):
    halfway = retained // 2
    columns = jnp.arange(retained, dtype=jnp.int32)
    harmonic = columns % halfway
    weight = jnp.where(harmonic == 0, 1.0, 2.0) * retained ** (-0.5)
    residue = jnp.mod(harmonic[:, None] * jnp.arange(extent, dtype=jnp.int32)[None, :], extent)
    radians = residue.astype(jnp.float32) * (2.0 * math.pi / extent)
    return (
        jnp.where((columns < halfway)[:, None], jnp.cos(radians), -jnp.sin(radians))
        * weight[:, None]
    )


def forward_z(extent, retained):
    halfway = retained // 2
    columns = jnp.arange(retained, dtype=jnp.int32)
    harmonic = columns % halfway
    residue = jnp.mod(jnp.arange(extent, dtype=jnp.int32)[:, None] * harmonic[None, :], extent)
    radians = residue.astype(jnp.float32) * (2.0 * math.pi / extent)
    return jnp.where((columns < halfway)[None, :], jnp.cos(radians), -jnp.sin(radians)) * (
        math.sqrt(retained) / extent
    )


def inverse_tail(portion, extent, sectioned, layout):
    count_py, count_pz, groups, member = layout
    retained = portion.shape[2]
    local_rows = retained // groups
    places = jnp.arange(retained, dtype=jnp.int32)
    owners = places // local_rows
    wave_y = signed_wave(places % local_rows * groups + owners, retained)
    points = jnp.arange(extent, dtype=jnp.int32)
    cosine_part, sine_part = trig_pair(points, wave_y, extent, retained ** (-0.5))
    along_y = complex_apply(cosine_part, sine_part, portion, 2, 1.0)
    return jnp.einsum("flyr,rz->flyz", along_y, inverse_z(extent, retained), precision=highest)


def forward_tail(portion, retained, sectioned, layout):
    count_py, count_pz, groups, member = layout
    extent = portion.shape[1]
    local_rows = extent // groups
    places = jnp.arange(extent, dtype=jnp.int32)
    points = places // local_rows * local_rows + places % local_rows
    wave_x = signed_wave(jnp.arange(retained, dtype=jnp.int32), retained)
    cosine_part, sine_part = trig_pair(wave_x, points, extent, math.sqrt(retained) / extent)
    return complex_apply(cosine_part, sine_part, portion, 1, -1.0)


def to_physical(coeffs, wavegrid, extent, resolution, layout):
    wave_x, wave_y, wave_z = wavegrid
    retained = coeffs.shape[1]
    seeds = jnp.concatenate([coeffs, wave_x * coeffs[1:3]], axis=0)
    points = jnp.arange(extent, dtype=jnp.int32)
    wave_rows = signed_wave(jnp.arange(retained, dtype=jnp.int32), retained)
    cosine_part, sine_part = trig_pair(points, wave_rows, extent, retained ** (-0.5))
    moved_x = complex_apply(cosine_part, sine_part, seeds, 1, 1.0)
    curl_x = rotate(wave_y * moved_x[2] - wave_z * moved_x[1])
    curl_y = rotate(wave_z * moved_x[0] - moved_x[4])
    curl_z = rotate(moved_x[3] - wave_y * moved_x[0])
    spread = jnp.concatenate([moved_x[:3], jnp.stack([curl_x, curl_y, curl_z])], axis=0)
    if resolution == "coarse":
        finish = partial(inverse_tail, extent=extent, sectioned=False, layout=layout)
        return finish(lax.all_to_all(spread, ("py", "pz"), split_axis=1, concat_axis=2, tiled=True))
    else:
        finish = partial(inverse_tail, extent=extent, sectioned=False, layout=layout)
        return finish(lax.all_to_all(spread, ("py", "pz"), split_axis=1, concat_axis=2, tiled=True))


def to_spectral(fields, retained, resolution, layout):
    count_py, count_pz, groups, member = layout
    extent = fields.shape[-1]
    along_z = jnp.einsum("flyz,zr->flyr", fields, forward_z(extent, retained), precision=highest)
    local_rows = retained // groups
    places = jnp.arange(retained, dtype=jnp.int32)
    wave_y = signed_wave(places % local_rows * groups + places // local_rows, retained)
    cosine_part, sine_part = trig_pair(
        wave_y, jnp.arange(extent, dtype=jnp.int32), extent, math.sqrt(retained) / extent
    )
    along_y = complex_apply(cosine_part, sine_part, along_z, 2, -1.0)
    if resolution == "coarse":
        finish = partial(forward_tail, retained=retained, sectioned=False, layout=layout)
        return finish(
            lax.all_to_all(along_y, ("py", "pz"), split_axis=2, concat_axis=1, tiled=True)
        )
    else:
        finish = partial(forward_tail, retained=retained, sectioned=False, layout=layout)
        return finish(
            lax.all_to_all(along_y, ("py", "pz"), split_axis=2, concat_axis=1, tiled=True)
        )


def wave_grid(retained, layout):
    count_py, count_pz, groups, member = layout
    places = jnp.arange(retained, dtype=jnp.int32)
    wave_x = signed_wave(places, retained).astype(jnp.float32)[:, None, None]
    local_places = jnp.arange(retained // groups, dtype=jnp.int32)
    wave_y = signed_wave(local_places * groups + member, retained).astype(jnp.float32)[
        None, :, None
    ]
    wave_z = (places % (retained // 2)).astype(jnp.float32)[None, None, :]
    return (wave_x, wave_y, wave_z)


def project(coeffs, wavegrid):
    wave_x, wave_y, wave_z = wavegrid
    squared = wave_x * wave_x + wave_y * wave_y + wave_z * wave_z
    divergence = (wave_x * coeffs[0] + wave_y * coeffs[1] + wave_z * coeffs[2]) / jnp.maximum(
        squared, 1.0
    )
    return jnp.stack(
        [
            coeffs[0] - wave_x * divergence,
            coeffs[1] - wave_y * divergence,
            coeffs[2] - wave_z * divergence,
        ]
    )


def cross_product(first_field, second_field):
    return jnp.stack(
        [
            first_field[1] * second_field[2] - first_field[2] * second_field[1],
            first_field[2] * second_field[0] - first_field[0] * second_field[2],
            first_field[0] * second_field[1] - first_field[1] * second_field[0],
        ]
    )


def advance(coeffs, resolution, layout):
    retained = coeffs.shape[1]
    extent = 3 * retained // 2
    wavegrid = wave_grid(retained, layout)
    fields = to_physical(coeffs, wavegrid, extent, resolution, layout)
    product = cross_product(fields[:3], fields[3:])
    nonlinear = to_spectral(product, retained, resolution, layout)
    wave_x, wave_y, wave_z = wavegrid
    squared = wave_x * wave_x + wave_y * wave_y + wave_z * wave_z
    damping = jnp.exp(-viscosity * time_step * squared)
    return damping * (coeffs + time_step * project(nonlinear, wavegrid))


def restrict(coeffs, kept, groups):
    halfway = kept // 2
    retained = coeffs.shape[1]
    rows_kept = jnp.concatenate([coeffs[:, :halfway], coeffs[:, retained - halfway :]], axis=1)
    local_rows = coeffs.shape[2]
    local_kept = kept // groups // 2
    rows_kept = jnp.concatenate(
        [rows_kept[:, :, :local_kept], rows_kept[:, :, local_rows - local_kept :]], axis=2
    )
    columns_half = coeffs.shape[3] // 2
    return jnp.concatenate(
        [rows_kept[..., :halfway], rows_kept[..., columns_half : columns_half + halfway]], axis=3
    )


def prolong(coeffs, retained, groups):
    components, kept, local_kept, width = coeffs.shape
    halfway = kept // 2
    zeros_x = jnp.zeros((components, retained - kept, local_kept, width), jnp.float32)
    wider = jnp.concatenate([coeffs[:, :halfway], zeros_x, coeffs[:, halfway:]], axis=1)
    local_rows = retained // groups
    split_rows = local_kept // 2
    zeros_y = jnp.zeros((components, retained, local_rows - local_kept, width), jnp.float32)
    wider = jnp.concatenate([wider[:, :, :split_rows], zeros_y, wider[:, :, split_rows:]], axis=2)
    zeros_z = jnp.zeros((components, retained, local_rows, retained // 2 - halfway), jnp.float32)
    return jnp.concatenate([wider[..., :halfway], zeros_z, wider[..., halfway:], zeros_z], axis=3)


def wave_table(length):
    places = np.arange(length)
    return np.where(places < length // 2, places, places - length)


def trig_table(outer, inner, extent):
    radians = 2.0 * np.pi / extent * np.mod(np.outer(outer, inner), extent)
    return np.cos(radians), np.sin(radians)


def split_table(table):
    table = np.asarray(table, np.float32)
    high = table.astype(jnp.bfloat16)
    low = (table - high.astype(np.float32)).astype(jnp.bfloat16)
    return high, low


def split(values):
    high = values.astype(jnp.bfloat16)
    low = (values - high.astype(jnp.float32)).astype(jnp.bfloat16)
    return high, low


def dot3(left, right):
    def dot(a, b):
        return jnp.dot(a, b, preferred_element_type=jnp.float32)

    return dot(left[0], right[0]) + dot(left[0], right[1]) + dot(left[1], right[0])


def z_tables(extent, retained):
    halfway = retained // 2
    columns = np.arange(retained)
    harmonic = columns % halfway
    cosine, sine = trig_table(harmonic, np.arange(extent), extent)
    table = np.where((columns < halfway)[:, None], cosine, -sine)
    weight = np.where(harmonic == 0, 1.0, 2.0)[:, None] * retained ** (-0.5)
    return table * weight, table.T * (math.sqrt(retained) / extent)


def wave_order(retained, count_py, count_pz):
    groups = count_py * count_pz
    rows, near = retained // groups, count_pz // 2
    side, band, line, z_low, inner = np.meshgrid(
        np.arange(2),
        np.arange(2),
        np.arange(count_py),
        np.arange(near),
        np.arange(rows // 2),
        indexing="ij",
    )
    owner = line * count_pz + side * near + z_low
    return ((band * (rows // 2) + inner) * groups + owner).reshape(-1)


def plane_tables(extent, retained, count_py, count_pz):
    groups = count_py * count_pz
    rows = retained // groups
    places = np.arange(retained)
    wave_in = wave_table(retained)[wave_order(retained, count_py, count_pz)]
    wave_out = wave_table(retained)[places % rows * groups + places // rows]
    cosine, sine = trig_table(np.arange(extent), wave_in, extent)
    inverse_y = np.concatenate([cosine, sine], axis=1) * retained ** (-0.5)
    cosine, sine = trig_table(wave_out, np.arange(extent), extent)
    forward_y = np.concatenate([cosine, -sine], axis=1) * (math.sqrt(retained) / extent)
    inverse_last, forward_last = z_tables(extent, retained)
    halfway = retained // 2
    lanes = np.zeros((8, retained), np.float32)
    lanes[0] = np.where(places < halfway, -1.0, 1.0)
    lanes[1] = places % halfway
    column = np.broadcast_to(wave_in[:, None], (retained, retained)).astype(np.float32)
    tables = [lanes, column]
    for table in (inverse_y, inverse_last, forward_last, forward_y):
        tables += split_table(table)
    return tables


def plane_math(fields, tables):
    lanes, wave_y, iy0, iy1, iz0, iz1, fz0, fz1, fy0, fy1 = tables
    turn, wave_z = lanes[0:1, :], lanes[1:2, :]
    retained = wave_y.shape[0]
    extent = iy0.shape[0]

    def turned(values):
        return pltpu.roll(values, retained // 2, 1) * turn

    v0, v1, v2, d1, d2 = fields
    i0 = turned(v0)
    w0 = turned(wave_y * v2 - wave_z * v1)
    w1 = wave_z * i0 - d2
    w2 = d1 - wave_y * i0
    six = (v0, v1, v2, w0, w1, w2)
    stacked = jnp.concatenate(
        [jnp.concatenate(six, axis=1), jnp.concatenate([i0] + [turned(f) for f in six[1:]], axis=1)],
        axis=0,
    )
    along_y = dot3((iy0, iy1), split(stacked))
    rows = jnp.concatenate(
        [along_y[:, f * retained : (f + 1) * retained] for f in range(6)], axis=0
    )
    physical = dot3(split(rows), (iz0, iz1))
    u0, u1, u2, w0, w1, w2 = [physical[f * extent : (f + 1) * extent] for f in range(6)]
    product = jnp.concatenate([u1 * w2 - u2 * w1, u2 * w0 - u0 * w2, u0 * w1 - u1 * w0], axis=0)
    along_z = dot3(split(product), (fz0, fz1))
    parts = [along_z[f * extent : (f + 1) * extent] for f in range(3)]
    stacked = jnp.concatenate(
        [jnp.concatenate(parts, axis=1), jnp.concatenate([turned(p) for p in parts], axis=1)],
        axis=0,
    )
    result = dot3((fy0, fy1), split(stacked))
    return [result[:, f * retained : (f + 1) * retained] for f in range(3)]


def point_place(position, side, spot, plane, near_group, planes):
    return ((position * 2 + side) * near_group + spot) * planes + plane


def x_tables(extent, retained, count_py, count_pz, halves):
    near = count_pz // 2
    near_group = count_py * near
    planes = extent // (2 * near_group * halves)
    wave_x = wave_table(retained)
    plane, spot = np.meshgrid(np.arange(planes), np.arange(near_group), indexing="ij")
    inverse = []
    for position in range(halves):
        for side in range(2):
            points = point_place(position, side, spot, plane, near_group, planes).reshape(-1)
            cosine, sine = trig_table(points, wave_x, extent)
            values = np.concatenate([cosine, sine], axis=1)
            slopes = np.concatenate([-sine * wave_x, cosine * wave_x], axis=1)
            inverse.append(np.concatenate([values, slopes], axis=0))
    inverse = np.stack(inverse) * retained ** (-0.5)
    plane, position, line, side, z_low = np.meshgrid(
        np.arange(planes),
        np.arange(halves),
        np.arange(count_py),
        np.arange(2),
        np.arange(near),
        indexing="ij",
    )
    points = point_place(position, side, line * near + z_low, plane, near_group, planes)
    points = points.reshape(planes, -1)
    early = planes - 2
    forward = []
    for some in (points[:early].reshape(-1), points[early:].reshape(-1)):
        cosine, sine = trig_table(wave_x, some, extent)
        forward.append(np.concatenate([cosine, -sine], axis=1) * (math.sqrt(retained) / extent))
    column = np.broadcast_to(wave_x[:, None], (retained, retained)).astype(np.float32)
    tables = [column]
    for table in [inverse] + forward:
        tables += split_table(table)
    return tables


def step_kernel(*refs):
    stored = refs[0]
    kept_tables = refs[1:18]
    out = refs[18]
    loaded = refs[19:36]
    wave_x_ref, xi0, xi1, fa0, fa1, fb0, fb1 = loaded[:7]
    plane_refs = loaded[7:]
    raw, modes, spread, recv, result, arrived, partial_sum = refs[36:43]
    load_sem, table_sem, mode_send, own_recv, pair_recv = refs[43:48]
    field_send, field_recv, back_send, back_recv, ready = refs[48:]

    _, retained, rows, _ = stored.shape
    planes, groups = result.shape[:2]
    halves = arrived.shape[1] // groups
    count_py, count_pz = lax.axis_size("py"), lax.axis_size("pz")
    near = count_pz // 2
    near_group = count_py * near
    band = rows // 2
    pairs = planes // 2
    early = planes - 2
    position = lax.axis_index("tm")
    row, place = lax.axis_index("py"), lax.axis_index("pz")
    side, z_low = place // near, lax.rem(place, near)
    spot = row * near + z_low
    member = row * count_pz + place
    pair_place = lax.rem(place + near, count_pz)
    pair_member = row * count_pz + pair_place

    def remote(source, target, send_sem, recv_sem, device):
        return pltpu.make_async_remote_copy(
            src_ref=source,
            dst_ref=target,
            send_sem=send_sem,
            recv_sem=recv_sem,
            device_id=device,
            device_id_type=pl.DeviceIdType.MESH,
        )

    def device(half, line, z_place):
        return {"tm": half, "py": line, "pz": z_place}

    across = device(1 - position, row, place)
    beside = device(position, row, pair_place)

    def turned(values):
        return pltpu.roll(values, retained // 2, 1) * turn

    def wave_y_of(a, owner):
        place_y = a * groups + owner
        return jnp.where(place_y < retained // 2, place_y, place_y - retained).astype(jnp.float32)

    def strided(ref, f, a):
        return ref.at[f].reshape(retained * rows, retained), pl.ds(a, retained, stride=rows)

    total = halves * groups
    barrier = pltpu.get_barrier_semaphore()

    def hello(other):
        pl.semaphore_signal(
            barrier, inc=1, device_id=other, device_id_type=pl.DeviceIdType.MESH
        )

    def greet(step, carry):
        other = lax.rem(spot + step, near_group)
        hello(device(position, other // near, side * near + lax.rem(other, near)))
        return carry

    hello(across)
    hello(beside)
    lax.fori_loop(1, near_group, greet, 0)

    @pl.when(position == 0)
    def _():
        pltpu.make_async_copy(stored, raw, load_sem).start()

    loads = [
        pltpu.make_async_copy(source, target, table_sem.at[i])
        for i, (source, target) in enumerate(zip(kept_tables, loaded))
    ]
    for load in loads:
        load.start()
    for load in loads:
        load.wait()
    lanes = plane_refs[0]
    turn, wave_z = lanes[0:1, :], lanes[1:2, :]

    def project(values, wave_y):
        wave_x = wave_x_ref[...]
        squared = wave_x * wave_x + (wave_y * wave_y + wave_z * wave_z)
        divergence = (wave_x * values[0] + wave_y * values[1] + wave_z * values[2]) / jnp.maximum(
            squared, 1.0
        )
        projected = [
            values[0] - wave_x * divergence,
            values[1] - wave_y * divergence,
            values[2] - wave_z * divergence,
        ]
        return projected, squared

    def flat_squares(wave_y):
        squares = wave_y * wave_y + wave_z * wave_z
        return squares < 0.5, 1.0 / jnp.maximum(squares, 1.0)

    @pl.when(position == 0)
    def _():
        pltpu.make_async_copy(stored, raw, load_sem).wait()

        def first(a, carry):
            wave_y = wave_y_of(a, member)
            values = []
            for f in range(3):
                view, rows_of = strided(raw, f, a)
                values.append(view[rows_of, :])
            values, _ = project(values, wave_y)
            for f in range(3):
                view, rows_of = strided(out, f, a)
                view[rows_of, :] = values[f]
            still, inverse = flat_squares(wave_y)
            turning = (wave_y * values[2] - wave_z * values[1]) * inverse
            modes[0, a, 0:retained, :] = jnp.where(still, values[1], values[0])
            modes[0, a, retained : 2 * retained, :] = jnp.where(still, values[2], turning)
            modes[0, a, 2 * retained : 2 * retained + 8, :] = values[0][0:8]
            return carry

        lax.fori_loop(0, rows, first, 0)

    pl.semaphore_wait(barrier, near_group + 1)

    def rebuild(slot, a, owner):
        wave_y = wave_y_of(a, owner)
        wave_x = wave_x_ref[...]
        still, inverse = flat_squares(wave_y)
        first = modes[slot, a, 0:retained, :]
        second = modes[slot, a, retained : 2 * retained, :]
        mean = modes[slot, a, 2 * retained : 2 * retained + 1, :]
        pushed = wave_x * first
        v0 = jnp.where(still, jnp.where(wave_x == 0.0, mean, 0.0), first)
        v1 = jnp.where(still, first, -(wave_y * inverse) * pushed - wave_z * second)
        v2 = jnp.where(still, second, -(wave_z * inverse) * pushed + wave_y * second)
        return v0, v1, v2

    def own_copy(a):
        return remote(modes.at[0, a], modes.at[0, a], mode_send, own_recv.at[a], across)

    def pair_copy(a):
        return remote(modes.at[0, a], modes.at[1, a], mode_send, pair_recv.at[a], beside)

    def relay_copy(a):
        return remote(modes.at[1, a], modes.at[1, a], mode_send, pair_recv.at[a], across)

    def each(start, stop, do):
        def body(a, carry):
            do(a)
            return carry

        lax.fori_loop(start, stop, body, 0)

    def transform(step, slot, high, owner, slot_side):
        quadrant = position * 2 + side
        tables = (xi0[quadrant], xi1[quadrant])
        fields = [rebuild(slot, high * band + a, owner) for a in range(band)]
        points = planes * near_group
        for f in (1, 2, 0):
            parts = [fields[a][f] for a in range(band)]
            stacked = jnp.concatenate(
                [
                    jnp.concatenate(parts, axis=1),
                    jnp.concatenate([turned(p) for p in parts], axis=1),
                ],
                axis=0,
            )
            count = 2 if f else 1
            moved = dot3([t[: count * points] for t in tables], split(stacked))
            for p in range(planes):
                for c in range(count):
                    if f:
                        group, offset = p // 2 * 5 + p % 2 * 2 + f - 1, c
                    else:
                        group, offset = p // 2 * 5 + 4, p % 2
                    view = spread.at[step, group].reshape(near_group * rows, retained)
                    top = c * points + p * near_group
                    for a in range(band):
                        view[pl.ds(2 * a + offset, near_group, stride=rows), :] = moved[
                            top : top + near_group, a * retained : (a + 1) * retained
                        ]
        chunk = slot_side * 2 + high
        slots = chunk * near_group
        recv[:, slots + spot] = spread[step, :, spot]
        spans = [(step, 0, 5 * pairs)]
        if step == 3:
            spans = [(step + k, 5 * k, 5) for k in range(pairs)]
        for semaphore, start, count in spans:

            def push(turn_index, carry, semaphore=semaphore, start=start, count=count):
                other = lax.rem(spot + near_group - turn_index, near_group)
                remote(
                    spread.at[step, pl.ds(start, count), other],
                    recv.at[pl.ds(start, count), slots + spot],
                    field_send,
                    field_recv.at[semaphore],
                    device(position, other // near, side * near + lax.rem(other, near)),
                ).start()
                return carry

            lax.fori_loop(1, near_group, push, 0)

    def take_own(a):
        own_copy(a).wait_recv()
        pair_copy(a).start()

    def take_pair(a):
        pair_copy(a).wait_recv()
        relay_copy(a).start()

    @pl.when(position == 0)
    def _():
        each(band + 1, rows, lambda a: own_copy(a).start())
        own_copy(band).start()
        own_copy(band - 1).start()
        each(0, band - 1, lambda a: own_copy(a).start())
        each(0, band // 2, lambda a: pair_copy(a).start())

    @pl.when(position == 1)
    def _():
        each(band + 1, rows, take_own)
        take_own(band)

    transform(0, 0, 1, member, side)

    @pl.when(position == 0)
    def _():
        each(band // 2, band, lambda a: pair_copy(a).start())

    @pl.when(position == 1)
    def _():
        take_own(band - 1)

        def weave(a):
            take_pair(a + band + 1)
            own_copy(a).wait_recv()

        each(0, band - 1, weave)

    transform(1, 0, 0, member, side)

    @pl.when(position == 0)
    def _():
        pair_copy(band).start()
        each(0, band - 1, take_pair)
        pair_copy(band - 1).wait_recv()

    @pl.when(position == 1)
    def _():
        pair_copy(band).wait_recv()

    transform(2, 1, position, pair_member, 1 - side)

    @pl.when(position == 0)
    def _():
        each(band, rows, lambda a: pair_copy(a).wait_recv())

    @pl.when(position == 1)
    def _():
        each(0, band, lambda a: pair_copy(a).wait_recv())

    transform(3, 1, 1 - position, pair_member, 1 - side)

    def await_fields(semaphore, start, count):
        some = recv.at[pl.ds(start, count), pl.ds(0, near_group - 1)]
        remote(some, some, field_send, field_recv.at[semaphore], beside).wait_recv()

    for step in range(3):
        await_fields(step, 0, 5 * pairs)

    tables = [ref[...] for ref in plane_refs]

    def plane_pair(k, carry):
        await_fields(3 + k, 5 * k, 5)

        @pl.when(jnp.logical_and(position == 1, k == 0))
        def _():
            pl.semaphore_signal(
                ready, inc=1, device_id=across, device_id_type=pl.DeviceIdType.MESH
            )

        def plane(odd, carry):
            p = 2 * k + odd

            def field(group, offset):
                view = recv.at[5 * k + group].reshape(4 * near_group * rows, retained)
                return view[pl.ds(offset, retained, stride=2), :]

            v1, d1 = field(2 * odd, 0), field(2 * odd, 1)
            v2, d2 = field(2 * odd + 1, 0), field(2 * odd + 1, 1)
            v0 = field(4, odd)
            for f, values in enumerate(plane_math([v0, v1, v2, d1, d2], tables)):
                result[p, :, f] = values.reshape(groups, rows, retained)

            @pl.when(jnp.logical_and(position == 0, p == 0))
            def _():
                pl.semaphore_wait(ready, 1)

            def push(turn_index, carry):
                to_place = lax.rem(place + near + turn_index // count_py, count_pz)
                to_row = lax.rem(row + turn_index, count_py)
                to_member = to_row * count_pz + to_place

                @pl.when(jnp.logical_or(position == 0, to_member != member))
                def _():
                    remote(
                        result.at[p, to_member],
                        arrived.at[p, position * groups + member],
                        back_send,
                        back_recv.at[p],
                        device(1, to_row, to_place),
                    ).start()

                return carry

            lax.fori_loop(0, groups, push, 0)

            @pl.when(position == 1)
            def _():
                arrived[p, groups + member] = result[p, member]

            return carry

        return lax.fori_loop(0, 2, plane, carry)

    lax.fori_loop(0, pairs, plane_pair, 0)

    def gather(start, count, a):
        view = arrived.reshape(planes * total * 3 * rows, retained)
        wide = jnp.concatenate(
            [
                view[pl.ds((start * total * 3 + f) * rows + a, count * total, stride=3 * rows), :]
                for f in range(3)
            ],
            axis=1,
        )
        back = jnp.concatenate(
            [
                turned(wide[:, f * retained : (f + 1) * retained])
                for f in range(3)
            ],
            axis=1,
        )
        return split(jnp.concatenate([wide, back], axis=0))

    @pl.when(position == 1)
    def _():
        def await_plane(p):
            some = arrived.at[p, pl.ds(0, total - 1)]
            remote(some, some, back_send, back_recv.at[p], beside).wait_recv()

        each(0, early, await_plane)

        def begin(a):
            before = jnp.concatenate(rebuild(0, a, member), axis=1)
            change = dot3((fa0[...], fa1[...]), gather(0, early, a))
            partial_sum[a] = before + time_step * change

        each(0, rows, begin)
        each(early, planes, await_plane)

        def finish(a):
            change = dot3((fb0[...], fb1[...]), gather(early, planes - early, a))
            after = partial_sum[a] + time_step * change
            values, squared = project(
                [after[:, f * retained : (f + 1) * retained] for f in range(3)],
                wave_y_of(a, member),
            )
            damping = jnp.exp((-viscosity * time_step) * squared)
            for f in range(3):
                view, rows_of = strided(out, f, a)
                view[rows_of, :] = damping * values[f]

        each(0, rows, finish)

    some = spread.at[:, :, pl.ds(0, near_group - 1)]
    remote(some, some, field_send, field_recv.at[0], beside).wait_send()

    @pl.when(position == 0)
    def _():
        remote(modes, modes, mode_send, own_recv.at[0], beside).wait_send()
        remote(result, result, back_send, back_recv.at[0], beside).wait_send()

    @pl.when(position == 1)
    def _():
        remote(modes.at[0], modes.at[0], mode_send, own_recv.at[0], beside).wait_send()
        some = result.at[:, pl.ds(0, groups - 1)]
        remote(some, some, back_send, back_recv.at[0], beside).wait_send()


def helped_advance(stored, count_py, count_pz, halves):
    _, retained, rows, _ = stored.shape
    groups = count_py * count_pz
    extent = 3 * retained // 2
    near_group = groups // 2
    planes = extent // (groups * halves)
    pairs = planes // 2
    tables = x_tables(extent, retained, count_py, count_pz, halves)
    tables += plane_tables(extent, retained, count_py, count_pz)
    tables = [jnp.asarray(table) for table in tables]
    vmem = pl.BlockSpec(memory_space=pltpu.VMEM)
    return pl.pallas_call(
        step_kernel,
        in_specs=[pl.BlockSpec(memory_space=pl.ANY)] * (1 + len(tables)),
        out_specs=vmem,
        out_shape=pltpu.VMEM(stored.shape, jnp.float32),
        scratch_shapes=[pltpu.VMEM(table.shape, table.dtype) for table in tables]
        + [
            pltpu.VMEM(stored.shape, jnp.float32),
            pltpu.VMEM((2, rows, 2 * retained + 8, retained), jnp.float32),
            pltpu.VMEM((4, 5 * pairs, near_group, rows, retained), jnp.float32),
            pltpu.VMEM((5 * pairs, 4 * near_group, rows, retained), jnp.float32),
            pltpu.VMEM((planes, groups, 3, rows, retained), jnp.float32),
            pltpu.VMEM((planes, halves * groups, 3, rows, retained), jnp.float32),
            pltpu.VMEM((rows, retained, 3 * retained), jnp.float32),
            pltpu.SemaphoreType.DMA,
            pltpu.SemaphoreType.DMA((len(tables),)),
            pltpu.SemaphoreType.DMA,
            pltpu.SemaphoreType.DMA((rows,)),
            pltpu.SemaphoreType.DMA((rows,)),
            pltpu.SemaphoreType.DMA,
            pltpu.SemaphoreType.DMA((3 + pairs,)),
            pltpu.SemaphoreType.DMA,
            pltpu.SemaphoreType.DMA((planes,)),
            pltpu.SemaphoreType.REGULAR,
        ],
        compiler_params=pltpu.CompilerParams(
            has_side_effects=True, collective_id=0, vmem_limit_bytes=56 * 1024 * 1024
        ),
        name="step",
    )(stored, *tables)


def shards(start_states):
    count_py = lax.axis_size("py")
    count_pz = lax.axis_size("pz")
    groups = count_py * count_pz
    member = lax.axis_index("py") * count_pz + lax.axis_index("pz")
    layout = (count_py, count_pz, groups, member)
    position = lax.axis_index("tm")
    slices = lax.axis_size("tm")
    retained = start_states.shape[-1]
    stored = start_states.reshape(3, retained, start_states.shape[3], retained)
    if slices == 2:
        result = helped_advance(stored, count_py, count_pz, slices)
        return result.reshape(1, 3, retained, stored.shape[2], 1, retained)
    spectral_state = project(stored, wave_grid(retained, layout))
    fine_end = advance(spectral_state, "fine", layout)
    coarse_start = restrict(spectral_state, M, groups)
    coarse_next = advance(coarse_start, "coarse", layout)
    fine_low = restrict(fine_end, M, groups)
    correction = fine_low - coarse_next

    def relay(chained):
        return shifted(chained, "tm", 1)

    current = jnp.where(position == 1, relay(fine_low), coarse_start)

    def sweep_turn(turn_index, current):
        candidate = advance(current, "coarse", layout) + correction
        arrived = relay(candidate)
        return jnp.where(position == turn_index + 1, arrived, current)

    current = lax.fori_loop(1, slices - 1, sweep_turn, current)
    upper_band = fine_end - prolong(fine_low, retained, groups)
    previous = shifted(upper_band, "tm", 1)
    updated = prolong(current, retained, groups) + previous
    result = jnp.where(position == 0, spectral_state, updated)
    return result.reshape(1, result.shape[0], retained, result.shape[2], 1, retained)


def solution(mesh):
    in_specs = (P("tm", None, None, None, ("py", "pz"), None),)
    out_specs = P("tm", None, None, None, ("py", "pz"), None)
    return jax.shard_map(shards, mesh=mesh, in_specs=in_specs, out_specs=out_specs, check_vma=False)
```

```python
from functools import partial
import math

import jax
import jax.numpy as jnp
from jax import lax
import numpy as np
from jax.experimental import pallas as pl
from jax.experimental.pallas import tpu as pltpu
from jax.sharding import PartitionSpec as P

M = 64


viscosity = 0.03
time_step = 0.004
highest = lax.Precision.HIGHEST


def shifted(block, axis, distance):
    devices = range(lax.axis_size(axis))
    route = [(i - distance, i) for i in devices if i - distance in devices]
    return lax.ppermute(block, axis, route)


def signed_wave(places, length):
    return jnp.where(places < length // 2, places, places - length)


def rotate(values):
    halfway = values.shape[-1] // 2
    return jnp.concatenate([-values[..., halfway:], values[..., :halfway]], axis=-1)


def trig_pair(outer, inner, extent, factor):
    residue = jnp.mod(outer[:, None] * inner[None, :], extent)
    radians = residue.astype(jnp.float32) * (2.0 * math.pi / extent)
    return (jnp.cos(radians) * factor, jnp.sin(radians) * factor)


def complex_apply(cosine_part, sine_part, values, contracted, direction_sign):
    kernel = jnp.stack(
        [
            jnp.stack([cosine_part, -direction_sign * sine_part]),
            jnp.stack([direction_sign * sine_part, cosine_part]),
        ]
    )
    halfway = values.shape[-1] // 2
    split = values.reshape(values.shape[:-1] + (2, halfway))
    if contracted == 1:
        pattern = "pqok,fkaqh->foaph"
    else:
        pattern = "pqok,flkqh->floph"
    result = jnp.einsum(pattern, kernel, split, precision=highest)
    return result.reshape(result.shape[:-2] + (2 * halfway,))


def inverse_z(extent, retained):
    halfway = retained // 2
    columns = jnp.arange(retained, dtype=jnp.int32)
    harmonic = columns % halfway
    weight = jnp.where(harmonic == 0, 1.0, 2.0) * retained ** (-0.5)
    residue = jnp.mod(harmonic[:, None] * jnp.arange(extent, dtype=jnp.int32)[None, :], extent)
    radians = residue.astype(jnp.float32) * (2.0 * math.pi / extent)
    return (
        jnp.where((columns < halfway)[:, None], jnp.cos(radians), -jnp.sin(radians))
        * weight[:, None]
    )


def forward_z(extent, retained):
    halfway = retained // 2
    columns = jnp.arange(retained, dtype=jnp.int32)
    harmonic = columns % halfway
    residue = jnp.mod(jnp.arange(extent, dtype=jnp.int32)[:, None] * harmonic[None, :], extent)
    radians = residue.astype(jnp.float32) * (2.0 * math.pi / extent)
    return jnp.where((columns < halfway)[None, :], jnp.cos(radians), -jnp.sin(radians)) * (
        math.sqrt(retained) / extent
    )


def inverse_tail(portion, extent, sectioned, layout):
    count_py, count_pz, groups, member = layout
    retained = portion.shape[2]
    local_rows = retained // groups
    places = jnp.arange(retained, dtype=jnp.int32)
    owners = places // local_rows
    wave_y = signed_wave(places % local_rows * groups + owners, retained)
    points = jnp.arange(extent, dtype=jnp.int32)
    cosine_part, sine_part = trig_pair(points, wave_y, extent, retained ** (-0.5))
    along_y = complex_apply(cosine_part, sine_part, portion, 2, 1.0)
    return jnp.einsum("flyr,rz->flyz", along_y, inverse_z(extent, retained), precision=highest)


def forward_tail(portion, retained, sectioned, layout):
    count_py, count_pz, groups, member = layout
    extent = portion.shape[1]
    local_rows = extent // groups
    places = jnp.arange(extent, dtype=jnp.int32)
    points = places // local_rows * local_rows + places % local_rows
    wave_x = signed_wave(jnp.arange(retained, dtype=jnp.int32), retained)
    cosine_part, sine_part = trig_pair(wave_x, points, extent, math.sqrt(retained) / extent)
    return complex_apply(cosine_part, sine_part, portion, 1, -1.0)


def to_physical(coeffs, wavegrid, extent, resolution, layout):
    wave_x, wave_y, wave_z = wavegrid
    retained = coeffs.shape[1]
    seeds = jnp.concatenate([coeffs, wave_x * coeffs[1:3]], axis=0)
    points = jnp.arange(extent, dtype=jnp.int32)
    wave_rows = signed_wave(jnp.arange(retained, dtype=jnp.int32), retained)
    cosine_part, sine_part = trig_pair(points, wave_rows, extent, retained ** (-0.5))
    moved_x = complex_apply(cosine_part, sine_part, seeds, 1, 1.0)
    curl_x = rotate(wave_y * moved_x[2] - wave_z * moved_x[1])
    curl_y = rotate(wave_z * moved_x[0] - moved_x[4])
    curl_z = rotate(moved_x[3] - wave_y * moved_x[0])
    spread = jnp.concatenate([moved_x[:3], jnp.stack([curl_x, curl_y, curl_z])], axis=0)
    if resolution == "coarse":
        finish = partial(inverse_tail, extent=extent, sectioned=False, layout=layout)
        return finish(lax.all_to_all(spread, ("py", "pz"), split_axis=1, concat_axis=2, tiled=True))
    else:
        finish = partial(inverse_tail, extent=extent, sectioned=False, layout=layout)
        return finish(lax.all_to_all(spread, ("py", "pz"), split_axis=1, concat_axis=2, tiled=True))


def to_spectral(fields, retained, resolution, layout):
    count_py, count_pz, groups, member = layout
    extent = fields.shape[-1]
    along_z = jnp.einsum("flyz,zr->flyr", fields, forward_z(extent, retained), precision=highest)
    local_rows = retained // groups
    places = jnp.arange(retained, dtype=jnp.int32)
    wave_y = signed_wave(places % local_rows * groups + places // local_rows, retained)
    cosine_part, sine_part = trig_pair(
        wave_y, jnp.arange(extent, dtype=jnp.int32), extent, math.sqrt(retained) / extent
    )
    along_y = complex_apply(cosine_part, sine_part, along_z, 2, -1.0)
    if resolution == "coarse":
        finish = partial(forward_tail, retained=retained, sectioned=False, layout=layout)
        return finish(
            lax.all_to_all(along_y, ("py", "pz"), split_axis=2, concat_axis=1, tiled=True)
        )
    else:
        finish = partial(forward_tail, retained=retained, sectioned=False, layout=layout)
        return finish(
            lax.all_to_all(along_y, ("py", "pz"), split_axis=2, concat_axis=1, tiled=True)
        )


def wave_grid(retained, layout):
    count_py, count_pz, groups, member = layout
    places = jnp.arange(retained, dtype=jnp.int32)
    wave_x = signed_wave(places, retained).astype(jnp.float32)[:, None, None]
    local_places = jnp.arange(retained // groups, dtype=jnp.int32)
    wave_y = signed_wave(local_places * groups + member, retained).astype(jnp.float32)[
        None, :, None
    ]
    wave_z = (places % (retained // 2)).astype(jnp.float32)[None, None, :]
    return (wave_x, wave_y, wave_z)


def project(coeffs, wavegrid):
    wave_x, wave_y, wave_z = wavegrid
    squared = wave_x * wave_x + wave_y * wave_y + wave_z * wave_z
    divergence = (wave_x * coeffs[0] + wave_y * coeffs[1] + wave_z * coeffs[2]) / jnp.maximum(
        squared, 1.0
    )
    return jnp.stack(
        [
            coeffs[0] - wave_x * divergence,
            coeffs[1] - wave_y * divergence,
            coeffs[2] - wave_z * divergence,
        ]
    )


def cross_product(first_field, second_field):
    return jnp.stack(
        [
            first_field[1] * second_field[2] - first_field[2] * second_field[1],
            first_field[2] * second_field[0] - first_field[0] * second_field[2],
            first_field[0] * second_field[1] - first_field[1] * second_field[0],
        ]
    )


def advance(coeffs, resolution, layout):
    retained = coeffs.shape[1]
    extent = 3 * retained // 2
    wavegrid = wave_grid(retained, layout)
    fields = to_physical(coeffs, wavegrid, extent, resolution, layout)
    product = cross_product(fields[:3], fields[3:])
    nonlinear = to_spectral(product, retained, resolution, layout)
    wave_x, wave_y, wave_z = wavegrid
    squared = wave_x * wave_x + wave_y * wave_y + wave_z * wave_z
    damping = jnp.exp(-viscosity * time_step * squared)
    return damping * (coeffs + time_step * project(nonlinear, wavegrid))


def restrict(coeffs, kept, groups):
    halfway = kept // 2
    retained = coeffs.shape[1]
    rows_kept = jnp.concatenate([coeffs[:, :halfway], coeffs[:, retained - halfway :]], axis=1)
    local_rows = coeffs.shape[2]
    local_kept = kept // groups // 2
    rows_kept = jnp.concatenate(
        [rows_kept[:, :, :local_kept], rows_kept[:, :, local_rows - local_kept :]], axis=2
    )
    columns_half = coeffs.shape[3] // 2
    return jnp.concatenate(
        [rows_kept[..., :halfway], rows_kept[..., columns_half : columns_half + halfway]], axis=3
    )


def prolong(coeffs, retained, groups):
    components, kept, local_kept, width = coeffs.shape
    halfway = kept // 2
    zeros_x = jnp.zeros((components, retained - kept, local_kept, width), jnp.float32)
    wider = jnp.concatenate([coeffs[:, :halfway], zeros_x, coeffs[:, halfway:]], axis=1)
    local_rows = retained // groups
    split_rows = local_kept // 2
    zeros_y = jnp.zeros((components, retained, local_rows - local_kept, width), jnp.float32)
    wider = jnp.concatenate([wider[:, :, :split_rows], zeros_y, wider[:, :, split_rows:]], axis=2)
    zeros_z = jnp.zeros((components, retained, local_rows, retained // 2 - halfway), jnp.float32)
    return jnp.concatenate([wider[..., :halfway], zeros_z, wider[..., halfway:], zeros_z], axis=3)


def wave_table(length):
    places = np.arange(length)
    return np.where(places < length // 2, places, places - length)


def trig_table(outer, inner, extent):
    radians = 2.0 * np.pi / extent * np.mod(np.outer(outer, inner), extent)
    return np.cos(radians), np.sin(radians)


def split_table(table):
    table = np.asarray(table, np.float32)
    high = table.astype(jnp.bfloat16)
    low = (table - high.astype(np.float32)).astype(jnp.bfloat16)
    return high, low


def split(values):
    high = values.astype(jnp.bfloat16)
    low = (values - high.astype(jnp.float32)).astype(jnp.bfloat16)
    return high, low


def dot3(left, right):
    def dot(a, b):
        return jnp.dot(a, b, preferred_element_type=jnp.float32)

    return dot(left[0], right[0]) + dot(left[0], right[1]) + dot(left[1], right[0])


def z_tables(extent, retained):
    halfway = retained // 2
    columns = np.arange(retained)
    harmonic = columns % halfway
    cosine, sine = trig_table(harmonic, np.arange(extent), extent)
    table = np.where((columns < halfway)[:, None], cosine, -sine)
    weight = np.where(harmonic == 0, 1.0, 2.0)[:, None] * retained ** (-0.5)
    return table * weight, table.T * (math.sqrt(retained) / extent)


def wave_order(retained, count_py, count_pz):
    groups = count_py * count_pz
    rows, near = retained // groups, count_pz // 2
    half, side, high, line, z_low, inner = np.meshgrid(
        np.arange(2),
        np.arange(2),
        np.arange(2),
        np.arange(count_py),
        np.arange(near),
        np.arange(rows // 4),
        indexing="ij",
    )
    owner = line * count_pz + side * near + z_low
    return (((high * 2 + half) * (rows // 4) + inner) * groups + owner).reshape(-1)


def plane_tables(extent, retained, count_py, count_pz):
    groups = count_py * count_pz
    rows = retained // groups
    places = np.arange(retained)
    wave_in = wave_table(retained)[wave_order(retained, count_py, count_pz)]
    wave_out = wave_table(retained)[places % rows * groups + places // rows]
    cosine, sine = trig_table(np.arange(extent), wave_in, extent)
    inverse_y = np.concatenate([cosine, sine], axis=1) * retained ** (-0.5)
    cosine, sine = trig_table(wave_out, np.arange(extent), extent)
    forward_y = np.concatenate([cosine, -sine], axis=1) * (math.sqrt(retained) / extent)
    inverse_last, forward_last = z_tables(extent, retained)
    halfway = retained // 2
    lanes = np.zeros((8, retained), np.float32)
    lanes[0] = np.where(places < halfway, -1.0, 1.0)
    lanes[1] = places % halfway
    column = np.broadcast_to(wave_in[:, None], (retained, retained)).astype(np.float32)
    tables = [lanes, column]
    for table in (inverse_y, inverse_last, forward_last, forward_y):
        tables += split_table(table)
    return tables


def plane_math(fields, tables):
    lanes, wave_y, iy0, iy1, iz0, iz1, fz0, fz1, fy0, fy1 = tables
    turn, wave_z = lanes[0:1, :], lanes[1:2, :]
    retained = wave_y.shape[0]
    extent = iy0.shape[0]

    def turned(values):
        return pltpu.roll(values, retained // 2, 1) * turn

    v0, v1, v2, d1, d2 = fields
    i0 = turned(v0)
    w0 = turned(wave_y * v2 - wave_z * v1)
    w1 = wave_z * i0 - d2
    w2 = d1 - wave_y * i0
    six = (v0, v1, v2, w0, w1, w2)
    stacked = jnp.concatenate(
        [jnp.concatenate(six, axis=1), jnp.concatenate([i0] + [turned(f) for f in six[1:]], axis=1)],
        axis=0,
    )
    along_y = dot3((iy0, iy1), split(stacked))
    rows = jnp.concatenate(
        [along_y[:, f * retained : (f + 1) * retained] for f in range(6)], axis=0
    )
    physical = dot3(split(rows), (iz0, iz1))
    u0, u1, u2, w0, w1, w2 = [physical[f * extent : (f + 1) * extent] for f in range(6)]
    product = jnp.concatenate([u1 * w2 - u2 * w1, u2 * w0 - u0 * w2, u0 * w1 - u1 * w0], axis=0)
    along_z = dot3(split(product), (fz0, fz1))
    parts = [along_z[f * extent : (f + 1) * extent] for f in range(3)]
    stacked = jnp.concatenate(
        [jnp.concatenate(parts, axis=1), jnp.concatenate([turned(p) for p in parts], axis=1)],
        axis=0,
    )
    result = dot3((fy0, fy1), split(stacked))
    return [result[:, f * retained : (f + 1) * retained] for f in range(3)]


def point_place(position, side, spot, plane, near_group, planes):
    return ((position * 2 + side) * near_group + spot) * planes + plane


def x_tables(extent, retained, count_py, count_pz, halves):
    near = count_pz // 2
    near_group = count_py * near
    planes = extent // (2 * near_group * halves)
    wave_x = wave_table(retained)
    plane, spot = np.meshgrid(np.arange(planes), np.arange(near_group), indexing="ij")
    inverse = []
    for position in range(halves):
        for side in range(2):
            points = point_place(position, side, spot, plane, near_group, planes).reshape(-1)
            cosine, sine = trig_table(points, wave_x, extent)
            values = np.concatenate([cosine, sine], axis=1)
            slopes = np.concatenate([-sine * wave_x, cosine * wave_x], axis=1)
            inverse.append(np.concatenate([values, slopes], axis=0))
    inverse = np.stack(inverse) * retained ** (-0.5)
    plane, position, line, side, z_low = np.meshgrid(
        np.arange(planes),
        np.arange(halves),
        np.arange(count_py),
        np.arange(2),
        np.arange(near),
        indexing="ij",
    )
    points = point_place(position, side, line * near + z_low, plane, near_group, planes)
    points = points.reshape(planes, -1)
    early = planes - 2
    forward = []
    for some in (points[:early].reshape(-1), points[early:].reshape(-1)):
        cosine, sine = trig_table(wave_x, some, extent)
        forward.append(np.concatenate([cosine, -sine], axis=1) * (math.sqrt(retained) / extent))
    column = np.broadcast_to(wave_x[:, None], (retained, retained)).astype(np.float32)
    tables = [column]
    for table in [inverse] + forward:
        tables += split_table(table)
    return tables


def step_kernel(*refs):
    stored = refs[0]
    kept_tables = refs[1:18]
    out = refs[18]
    loaded = refs[19:36]
    wave_x_ref, xi0, xi1, fa0, fa1, fb0, fb1 = loaded[:7]
    plane_refs = loaded[7:]
    raw, modes, spread, spread_mean, recv, recv_mean = refs[36:42]
    result, arrived, partial_sum = refs[42:45]
    load_sem, table_sem, mode_send, own_recv, pair_recv = refs[45:50]
    field_send, field_recv, mean_recv, back_send, back_recv, ready = refs[50:]

    _, retained, rows, _ = stored.shape
    planes, groups = result.shape[:2]
    halves = arrived.shape[1] // groups
    count_py, count_pz = lax.axis_size("py"), lax.axis_size("pz")
    near = count_pz // 2
    near_group = count_py * near
    band = rows // 2
    pairs = planes // 2
    early = planes - 2
    position = lax.axis_index("tm")
    row, place = lax.axis_index("py"), lax.axis_index("pz")
    side, z_low = place // near, lax.rem(place, near)
    spot = row * near + z_low
    member = row * count_pz + place
    pair_place = lax.rem(place + near, count_pz)
    pair_member = row * count_pz + pair_place

    def remote(source, target, send_sem, recv_sem, device):
        return pltpu.make_async_remote_copy(
            src_ref=source,
            dst_ref=target,
            send_sem=send_sem,
            recv_sem=recv_sem,
            device_id=device,
            device_id_type=pl.DeviceIdType.MESH,
        )

    def device(half, line, z_place):
        return {"tm": half, "py": line, "pz": z_place}

    across = device(1 - position, row, place)
    beside = device(position, row, pair_place)

    def turned(values):
        return pltpu.roll(values, retained // 2, 1) * turn

    def wave_y_of(a, owner):
        place_y = a * groups + owner
        return jnp.where(place_y < retained // 2, place_y, place_y - retained).astype(jnp.float32)

    def strided(ref, f, a):
        return ref.at[f].reshape(retained * rows, retained), pl.ds(a, retained, stride=rows)

    total = halves * groups
    barrier = pltpu.get_barrier_semaphore()

    def hello(other):
        pl.semaphore_signal(
            barrier, inc=1, device_id=other, device_id_type=pl.DeviceIdType.MESH
        )

    def greet(step, carry):
        other = lax.rem(spot + step, near_group)
        hello(device(position, other // near, side * near + lax.rem(other, near)))
        return carry

    hello(across)
    hello(beside)
    lax.fori_loop(1, near_group, greet, 0)

    @pl.when(position == 0)
    def _():
        pltpu.make_async_copy(stored, raw, load_sem).start()

    loads = [
        pltpu.make_async_copy(source, target, table_sem.at[i])
        for i, (source, target) in enumerate(zip(kept_tables, loaded))
    ]
    for load in loads:
        load.start()
    for load in loads:
        load.wait()
    lanes = plane_refs[0]
    turn, wave_z = lanes[0:1, :], lanes[1:2, :]

    def project(values, wave_y):
        wave_x = wave_x_ref[...]
        squared = wave_x * wave_x + (wave_y * wave_y + wave_z * wave_z)
        divergence = (wave_x * values[0] + wave_y * values[1] + wave_z * values[2]) / jnp.maximum(
            squared, 1.0
        )
        projected = [
            values[0] - wave_x * divergence,
            values[1] - wave_y * divergence,
            values[2] - wave_z * divergence,
        ]
        return projected, squared

    def flat_squares(wave_y):
        squares = wave_y * wave_y + wave_z * wave_z
        return squares < 0.5, 1.0 / jnp.maximum(squares, 1.0)

    @pl.when(position == 0)
    def _():
        pltpu.make_async_copy(stored, raw, load_sem).wait()

        def first(a, carry):
            wave_y = wave_y_of(a, member)
            values = []
            for f in range(3):
                view, rows_of = strided(raw, f, a)
                values.append(view[rows_of, :])
            values, _ = project(values, wave_y)
            for f in range(3):
                view, rows_of = strided(out, f, a)
                view[rows_of, :] = values[f]
            still, inverse = flat_squares(wave_y)
            turning = (wave_y * values[2] - wave_z * values[1]) * inverse
            modes[0, a, 0:retained, :] = jnp.where(still, values[1], values[0])
            modes[0, a, retained : 2 * retained, :] = jnp.where(still, values[2], turning)
            modes[0, a, 2 * retained : 2 * retained + 8, :] = values[0][0:8]
            return carry

        lax.fori_loop(0, rows, first, 0)

    pl.semaphore_wait(barrier, near_group + 1)

    def rebuild(slot, a, owner):
        wave_y = wave_y_of(a, owner)
        wave_x = wave_x_ref[...]
        still, inverse = flat_squares(wave_y)
        first = modes[slot, a, 0:retained, :]
        second = modes[slot, a, retained : 2 * retained, :]
        mean = modes[slot, a, 2 * retained : 2 * retained + 1, :]
        pushed = wave_x * first
        v0 = jnp.where(still, jnp.where(wave_x == 0.0, mean, 0.0), first)
        v1 = jnp.where(still, first, -(wave_y * inverse) * pushed - wave_z * second)
        v2 = jnp.where(still, second, -(wave_z * inverse) * pushed + wave_y * second)
        return v0, v1, v2

    def own_copy(a):
        return remote(modes.at[0, a], modes.at[0, a], mode_send, own_recv.at[a], across)

    def pair_copy(a):
        return remote(modes.at[0, a], modes.at[1, a], mode_send, pair_recv.at[a], beside)

    def relay_copy(a):
        return remote(modes.at[1, a], modes.at[1, a], mode_send, pair_recv.at[a], across)

    def each(start, stop, do):
        def body(a, carry):
            do(a)
            return carry

        lax.fori_loop(start, stop, body, 0)

    few = band // 2
    last = 7

    def transform(step, slot, high, half):
        owner = pair_member if slot else member
        quadrant = position * 2 + side
        tables = (xi0[quadrant], xi1[quadrant])
        top_row = high * band + half * few
        fields = [rebuild(slot, top_row + a, owner) for a in range(few)]
        points = planes * near_group
        chunk = (1 - side if slot else side) * 2 + high
        for f in (1, 2, 0):
            parts = [fields[a][f] for a in range(few)]
            stacked = jnp.concatenate(
                [
                    jnp.concatenate(parts, axis=1),
                    jnp.concatenate([turned(p) for p in parts], axis=1),
                ],
                axis=0,
            )
            count = 2 if f else 1
            moved = dot3([t[: count * points] for t in tables], split(stacked))
            for p in range(planes):
                for c in range(count):
                    if f:
                        view, offset = spread.at[step, p], 2 * (f - 1) + c
                    else:
                        view, offset = spread_mean.at[step // 2, p // 2], 2 * half + p % 2
                    view = view.reshape(near_group * rows, retained)
                    top = c * points + p * near_group
                    for a in range(few):
                        view[pl.ds(4 * a + offset, near_group, stride=rows), :] = moved[
                            top : top + near_group, a * retained : (a + 1) * retained
                        ]
        slots = (half * 4 + chunk) * near_group
        mean_slots = chunk * near_group
        complete = step % 2 == 1
        recv[:, slots + spot] = spread[step, :, spot]
        if complete:
            recv_mean[:, mean_slots + spot] = spread_mean[step // 2, :, spot]

        def send(other, first, count, index, mean_index):
            to = device(position, other // near, side * near + lax.rem(other, near))
            remote(
                spread.at[step, pl.ds(2 * first, 2 * count), other],
                recv.at[pl.ds(2 * first, 2 * count), slots + spot],
                field_send,
                field_recv.at[index],
                to,
            ).start()
            if complete:
                remote(
                    spread_mean.at[step // 2, pl.ds(first, count), other],
                    recv_mean.at[pl.ds(first, count), mean_slots + spot],
                    field_send,
                    mean_recv.at[mean_index],
                    to,
                ).start()

        spans = [(0, pairs, step, step // 2)]
        if step == last:
            spans = [(k, 1, last + k, last // 2 + k) for k in range(pairs)]
        for first, count, index, mean_index in spans:

            def push(turn_index, carry, span=(first, count, index, mean_index)):
                send(lax.rem(spot + near_group - turn_index, near_group), *span)
                return carry

            lax.fori_loop(1, near_group, push, 0)

    def await_fields(first, count, index):
        some = recv.at[pl.ds(2 * first, 2 * count), pl.ds(0, near_group - 1)]
        remote(some, some, field_send, field_recv.at[index], beside).wait_recv()

    def await_means(first, count, index):
        some = recv_mean.at[pl.ds(first, count), pl.ds(0, near_group - 1)]
        remote(some, some, field_send, mean_recv.at[index], beside).wait_recv()

    low, high = list(range(band)), list(range(band, rows))
    own_order = high + low[::-1]

    def send_pair(rows_of):
        for a in rows_of:
            pair_copy(a).start()

    def take_own(rows_of):
        for a in rows_of:
            own_copy(a).wait_recv()
            if a in high:
                pair_copy(a).start()

    def take_pair(rows_of):
        for a in rows_of:
            pair_copy(a).wait_recv()

            @pl.when(position == (0 if a in low else 1))
            def _():
                relay_copy(a).start()

    def on(which, do):
        @pl.when(position == which)
        def _():
            do()

    def start_first():
        for a in own_order:
            own_copy(a).start()
        send_pair(low[:2])

    on(0, start_first)
    on(1, lambda: take_own(high[:few]))
    transform(0, 0, 1, 0)
    on(0, lambda: send_pair(low[2:3]))
    on(1, lambda: take_own(high[few:]))
    transform(1, 0, 1, 1)
    on(0, lambda: send_pair(low[3:]))
    on(1, lambda: take_own(low[few:][::-1]))
    on(1, lambda: take_pair(high[:1]))
    transform(2, 0, 0, 1)
    on(1, lambda: take_own(low[:few][::-1]))
    transform(3, 0, 0, 0)
    on(0, lambda: take_pair(low[:few]))
    on(1, lambda: take_pair(high[1:few]))
    transform(4, 1, position, 0)
    on(0, lambda: take_pair(low[few:]))
    on(1, lambda: take_pair(high[few:]))
    transform(5, 1, position, 1)
    on(0, lambda: take_pair(high[:few]))
    on(1, lambda: take_pair(low[:few]))
    transform(6, 1, 1 - position, 0)
    on(0, lambda: take_pair(high[few:]))
    on(1, lambda: take_pair(low[few:]))
    transform(7, 1, 1 - position, 1)

    for step in range(last):
        await_fields(0, pairs, step)
    for step in range(last // 2):
        await_means(0, pairs, step)

    tables = [ref[...] for ref in plane_refs]

    def plane_pair(k, carry):
        await_fields(k, 1, last + k)
        await_means(k, 1, last // 2 + k)

        @pl.when(jnp.logical_and(position == 1, k == 0))
        def _():
            pl.semaphore_signal(
                ready, inc=1, device_id=across, device_id_type=pl.DeviceIdType.MESH
            )

        def plane(odd, carry):
            p = 2 * k + odd

            view = recv.at[p].reshape(8 * near_group * rows, retained)
            v1, d1, v2, d2 = [view[pl.ds(i, retained, stride=4), :] for i in range(4)]
            view = recv_mean.at[k].reshape(4 * near_group * rows, retained)
            v0 = jnp.concatenate(
                [
                    view[pl.ds(2 * half + odd, retained // 2, stride=4), :]
                    for half in range(2)
                ],
                axis=0,
            )
            for f, values in enumerate(plane_math([v0, v1, v2, d1, d2], tables)):
                result[p, :, f] = values.reshape(groups, rows, retained)

            @pl.when(jnp.logical_and(position == 0, p == 0))
            def _():
                pl.semaphore_wait(ready, 1)

            def push(turn_index, carry):
                to_place = lax.rem(place + near + turn_index // count_py, count_pz)
                to_row = lax.rem(row + turn_index, count_py)
                to_member = to_row * count_pz + to_place

                @pl.when(jnp.logical_or(position == 0, to_member != member))
                def _():
                    remote(
                        result.at[p, to_member],
                        arrived.at[p, position * groups + member],
                        back_send,
                        back_recv.at[p],
                        device(1, to_row, to_place),
                    ).start()

                return carry

            lax.fori_loop(0, groups, push, 0)

            @pl.when(position == 1)
            def _():
                arrived[p, groups + member] = result[p, member]

            return carry

        return lax.fori_loop(0, 2, plane, carry)

    lax.fori_loop(0, pairs, plane_pair, 0)

    def gather(start, count, a):
        view = arrived.reshape(planes * total * 3 * rows, retained)
        wide = jnp.concatenate(
            [
                view[pl.ds((start * total * 3 + f) * rows + a, count * total, stride=3 * rows), :]
                for f in range(3)
            ],
            axis=1,
        )
        back = jnp.concatenate(
            [
                turned(wide[:, f * retained : (f + 1) * retained])
                for f in range(3)
            ],
            axis=1,
        )
        return split(jnp.concatenate([wide, back], axis=0))

    @pl.when(position == 1)
    def _():
        def await_plane(p):
            some = arrived.at[p, pl.ds(0, total - 1)]
            remote(some, some, back_send, back_recv.at[p], beside).wait_recv()

        each(0, early, await_plane)

        def begin(a):
            before = jnp.concatenate(rebuild(0, a, member), axis=1)
            change = dot3((fa0[...], fa1[...]), gather(0, early, a))
            partial_sum[a] = before + time_step * change

        each(0, rows, begin)
        each(early, planes, await_plane)

        def finish(a):
            change = dot3((fb0[...], fb1[...]), gather(early, planes - early, a))
            after = partial_sum[a] + time_step * change
            values, squared = project(
                [after[:, f * retained : (f + 1) * retained] for f in range(3)],
                wave_y_of(a, member),
            )
            damping = jnp.exp((-viscosity * time_step) * squared)
            for f in range(3):
                view, rows_of = strided(out, f, a)
                view[rows_of, :] = damping * values[f]

        each(0, rows, finish)

    for sent in (spread, spread_mean):
        some = sent.at[:, :, pl.ds(0, near_group - 1)]
        remote(some, some, field_send, field_recv.at[0], beside).wait_send()

    @pl.when(position == 0)
    def _():
        remote(modes, modes, mode_send, own_recv.at[0], beside).wait_send()
        remote(result, result, back_send, back_recv.at[0], beside).wait_send()

    @pl.when(position == 1)
    def _():
        remote(modes.at[0], modes.at[0], mode_send, own_recv.at[0], beside).wait_send()
        some = result.at[:, pl.ds(0, groups - 1)]
        remote(some, some, back_send, back_recv.at[0], beside).wait_send()


def helped_advance(stored, count_py, count_pz, halves):
    _, retained, rows, _ = stored.shape
    groups = count_py * count_pz
    extent = 3 * retained // 2
    near_group = groups // 2
    planes = extent // (groups * halves)
    pairs = planes // 2
    tables = x_tables(extent, retained, count_py, count_pz, halves)
    tables += plane_tables(extent, retained, count_py, count_pz)
    tables = [jnp.asarray(table) for table in tables]
    vmem = pl.BlockSpec(memory_space=pltpu.VMEM)
    return pl.pallas_call(
        step_kernel,
        in_specs=[pl.BlockSpec(memory_space=pl.ANY)] * (1 + len(tables)),
        out_specs=vmem,
        out_shape=pltpu.VMEM(stored.shape, jnp.float32),
        scratch_shapes=[pltpu.VMEM(table.shape, table.dtype) for table in tables]
        + [
            pltpu.VMEM(stored.shape, jnp.float32),
            pltpu.VMEM((2, rows, 2 * retained + 8, retained), jnp.float32),
            pltpu.VMEM((8, planes, near_group, rows, retained), jnp.float32),
            pltpu.VMEM((4, pairs, near_group, rows, retained), jnp.float32),
            pltpu.VMEM((planes, 8 * near_group, rows, retained), jnp.float32),
            pltpu.VMEM((pairs, 4 * near_group, rows, retained), jnp.float32),
            pltpu.VMEM((planes, groups, 3, rows, retained), jnp.float32),
            pltpu.VMEM((planes, halves * groups, 3, rows, retained), jnp.float32),
            pltpu.VMEM((rows, retained, 3 * retained), jnp.float32),
            pltpu.SemaphoreType.DMA,
            pltpu.SemaphoreType.DMA((len(tables),)),
            pltpu.SemaphoreType.DMA,
            pltpu.SemaphoreType.DMA((rows,)),
            pltpu.SemaphoreType.DMA((rows,)),
            pltpu.SemaphoreType.DMA,
            pltpu.SemaphoreType.DMA((7 + pairs,)),
            pltpu.SemaphoreType.DMA((3 + pairs,)),
            pltpu.SemaphoreType.DMA,
            pltpu.SemaphoreType.DMA((planes,)),
            pltpu.SemaphoreType.REGULAR,
        ],
        compiler_params=pltpu.CompilerParams(
            has_side_effects=True, collective_id=0, vmem_limit_bytes=56 * 1024 * 1024
        ),
        name="step",
    )(stored, *tables)


def shards(start_states):
    count_py = lax.axis_size("py")
    count_pz = lax.axis_size("pz")
    groups = count_py * count_pz
    member = lax.axis_index("py") * count_pz + lax.axis_index("pz")
    layout = (count_py, count_pz, groups, member)
    position = lax.axis_index("tm")
    slices = lax.axis_size("tm")
    retained = start_states.shape[-1]
    stored = start_states.reshape(3, retained, start_states.shape[3], retained)
    if slices == 2:
        result = helped_advance(stored, count_py, count_pz, slices)
        return result.reshape(1, 3, retained, stored.shape[2], 1, retained)
    spectral_state = project(stored, wave_grid(retained, layout))
    fine_end = advance(spectral_state, "fine", layout)
    coarse_start = restrict(spectral_state, M, groups)
    coarse_next = advance(coarse_start, "coarse", layout)
    fine_low = restrict(fine_end, M, groups)
    correction = fine_low - coarse_next

    def relay(chained):
        return shifted(chained, "tm", 1)

    current = jnp.where(position == 1, relay(fine_low), coarse_start)

    def sweep_turn(turn_index, current):
        candidate = advance(current, "coarse", layout) + correction
        arrived = relay(candidate)
        return jnp.where(position == turn_index + 1, arrived, current)

    current = lax.fori_loop(1, slices - 1, sweep_turn, current)
    upper_band = fine_end - prolong(fine_low, retained, groups)
    previous = shifted(upper_band, "tm", 1)
    updated = prolong(current, retained, groups) + previous
    result = jnp.where(position == 0, spectral_state, updated)
    return result.reshape(1, result.shape[0], retained, result.shape[2], 1, retained)


def solution(mesh):
    in_specs = (P("tm", None, None, None, ("py", "pz"), None),)
    out_specs = P("tm", None, None, None, ("py", "pz"), None)
    return jax.shard_map(shards, mesh=mesh, in_specs=in_specs, out_specs=out_specs, check_vma=False)
```

```python
from functools import partial
import math

import jax
import jax.numpy as jnp
from jax import lax
import numpy as np
from jax.experimental import pallas as pl
from jax.experimental.pallas import tpu as pltpu
from jax.sharding import PartitionSpec as P

M = 64


viscosity = 0.03
time_step = 0.004
highest = lax.Precision.HIGHEST


def shifted(block, axis, distance):
    devices = range(lax.axis_size(axis))
    route = [(i - distance, i) for i in devices if i - distance in devices]
    return lax.ppermute(block, axis, route)


def signed_wave(places, length):
    return jnp.where(places < length // 2, places, places - length)


def rotate(values):
    halfway = values.shape[-1] // 2
    return jnp.concatenate([-values[..., halfway:], values[..., :halfway]], axis=-1)


def trig_pair(outer, inner, extent, factor):
    residue = jnp.mod(outer[:, None] * inner[None, :], extent)
    radians = residue.astype(jnp.float32) * (2.0 * math.pi / extent)
    return (jnp.cos(radians) * factor, jnp.sin(radians) * factor)


def complex_apply(cosine_part, sine_part, values, contracted, direction_sign):
    kernel = jnp.stack(
        [
            jnp.stack([cosine_part, -direction_sign * sine_part]),
            jnp.stack([direction_sign * sine_part, cosine_part]),
        ]
    )
    halfway = values.shape[-1] // 2
    split = values.reshape(values.shape[:-1] + (2, halfway))
    if contracted == 1:
        pattern = "pqok,fkaqh->foaph"
    else:
        pattern = "pqok,flkqh->floph"
    result = jnp.einsum(pattern, kernel, split, precision=highest)
    return result.reshape(result.shape[:-2] + (2 * halfway,))


def inverse_z(extent, retained):
    halfway = retained // 2
    columns = jnp.arange(retained, dtype=jnp.int32)
    harmonic = columns % halfway
    weight = jnp.where(harmonic == 0, 1.0, 2.0) * retained ** (-0.5)
    residue = jnp.mod(harmonic[:, None] * jnp.arange(extent, dtype=jnp.int32)[None, :], extent)
    radians = residue.astype(jnp.float32) * (2.0 * math.pi / extent)
    return (
        jnp.where((columns < halfway)[:, None], jnp.cos(radians), -jnp.sin(radians))
        * weight[:, None]
    )


def forward_z(extent, retained):
    halfway = retained // 2
    columns = jnp.arange(retained, dtype=jnp.int32)
    harmonic = columns % halfway
    residue = jnp.mod(jnp.arange(extent, dtype=jnp.int32)[:, None] * harmonic[None, :], extent)
    radians = residue.astype(jnp.float32) * (2.0 * math.pi / extent)
    return jnp.where((columns < halfway)[None, :], jnp.cos(radians), -jnp.sin(radians)) * (
        math.sqrt(retained) / extent
    )


def inverse_tail(portion, extent, sectioned, layout):
    count_py, count_pz, groups, member = layout
    retained = portion.shape[2]
    local_rows = retained // groups
    places = jnp.arange(retained, dtype=jnp.int32)
    owners = places // local_rows
    wave_y = signed_wave(places % local_rows * groups + owners, retained)
    points = jnp.arange(extent, dtype=jnp.int32)
    cosine_part, sine_part = trig_pair(points, wave_y, extent, retained ** (-0.5))
    along_y = complex_apply(cosine_part, sine_part, portion, 2, 1.0)
    return jnp.einsum("flyr,rz->flyz", along_y, inverse_z(extent, retained), precision=highest)


def forward_tail(portion, retained, sectioned, layout):
    count_py, count_pz, groups, member = layout
    extent = portion.shape[1]
    local_rows = extent // groups
    places = jnp.arange(extent, dtype=jnp.int32)
    points = places // local_rows * local_rows + places % local_rows
    wave_x = signed_wave(jnp.arange(retained, dtype=jnp.int32), retained)
    cosine_part, sine_part = trig_pair(wave_x, points, extent, math.sqrt(retained) / extent)
    return complex_apply(cosine_part, sine_part, portion, 1, -1.0)


def to_physical(coeffs, wavegrid, extent, resolution, layout):
    wave_x, wave_y, wave_z = wavegrid
    retained = coeffs.shape[1]
    seeds = jnp.concatenate([coeffs, wave_x * coeffs[1:3]], axis=0)
    points = jnp.arange(extent, dtype=jnp.int32)
    wave_rows = signed_wave(jnp.arange(retained, dtype=jnp.int32), retained)
    cosine_part, sine_part = trig_pair(points, wave_rows, extent, retained ** (-0.5))
    moved_x = complex_apply(cosine_part, sine_part, seeds, 1, 1.0)
    curl_x = rotate(wave_y * moved_x[2] - wave_z * moved_x[1])
    curl_y = rotate(wave_z * moved_x[0] - moved_x[4])
    curl_z = rotate(moved_x[3] - wave_y * moved_x[0])
    spread = jnp.concatenate([moved_x[:3], jnp.stack([curl_x, curl_y, curl_z])], axis=0)
    if resolution == "coarse":
        finish = partial(inverse_tail, extent=extent, sectioned=False, layout=layout)
        return finish(lax.all_to_all(spread, ("py", "pz"), split_axis=1, concat_axis=2, tiled=True))
    else:
        finish = partial(inverse_tail, extent=extent, sectioned=False, layout=layout)
        return finish(lax.all_to_all(spread, ("py", "pz"), split_axis=1, concat_axis=2, tiled=True))


def to_spectral(fields, retained, resolution, layout):
    count_py, count_pz, groups, member = layout
    extent = fields.shape[-1]
    along_z = jnp.einsum("flyz,zr->flyr", fields, forward_z(extent, retained), precision=highest)
    local_rows = retained // groups
    places = jnp.arange(retained, dtype=jnp.int32)
    wave_y = signed_wave(places % local_rows * groups + places // local_rows, retained)
    cosine_part, sine_part = trig_pair(
        wave_y, jnp.arange(extent, dtype=jnp.int32), extent, math.sqrt(retained) / extent
    )
    along_y = complex_apply(cosine_part, sine_part, along_z, 2, -1.0)
    if resolution == "coarse":
        finish = partial(forward_tail, retained=retained, sectioned=False, layout=layout)
        return finish(
            lax.all_to_all(along_y, ("py", "pz"), split_axis=2, concat_axis=1, tiled=True)
        )
    else:
        finish = partial(forward_tail, retained=retained, sectioned=False, layout=layout)
        return finish(
            lax.all_to_all(along_y, ("py", "pz"), split_axis=2, concat_axis=1, tiled=True)
        )


def wave_grid(retained, layout):
    count_py, count_pz, groups, member = layout
    places = jnp.arange(retained, dtype=jnp.int32)
    wave_x = signed_wave(places, retained).astype(jnp.float32)[:, None, None]
    local_places = jnp.arange(retained // groups, dtype=jnp.int32)
    wave_y = signed_wave(local_places * groups + member, retained).astype(jnp.float32)[
        None, :, None
    ]
    wave_z = (places % (retained // 2)).astype(jnp.float32)[None, None, :]
    return (wave_x, wave_y, wave_z)


def project(coeffs, wavegrid):
    wave_x, wave_y, wave_z = wavegrid
    squared = wave_x * wave_x + wave_y * wave_y + wave_z * wave_z
    divergence = (wave_x * coeffs[0] + wave_y * coeffs[1] + wave_z * coeffs[2]) / jnp.maximum(
        squared, 1.0
    )
    return jnp.stack(
        [
            coeffs[0] - wave_x * divergence,
            coeffs[1] - wave_y * divergence,
            coeffs[2] - wave_z * divergence,
        ]
    )


def cross_product(first_field, second_field):
    return jnp.stack(
        [
            first_field[1] * second_field[2] - first_field[2] * second_field[1],
            first_field[2] * second_field[0] - first_field[0] * second_field[2],
            first_field[0] * second_field[1] - first_field[1] * second_field[0],
        ]
    )


def advance(coeffs, resolution, layout):
    retained = coeffs.shape[1]
    extent = 3 * retained // 2
    wavegrid = wave_grid(retained, layout)
    fields = to_physical(coeffs, wavegrid, extent, resolution, layout)
    product = cross_product(fields[:3], fields[3:])
    nonlinear = to_spectral(product, retained, resolution, layout)
    wave_x, wave_y, wave_z = wavegrid
    squared = wave_x * wave_x + wave_y * wave_y + wave_z * wave_z
    damping = jnp.exp(-viscosity * time_step * squared)
    return damping * (coeffs + time_step * project(nonlinear, wavegrid))


def restrict(coeffs, kept, groups):
    halfway = kept // 2
    retained = coeffs.shape[1]
    rows_kept = jnp.concatenate([coeffs[:, :halfway], coeffs[:, retained - halfway :]], axis=1)
    local_rows = coeffs.shape[2]
    local_kept = kept // groups // 2
    rows_kept = jnp.concatenate(
        [rows_kept[:, :, :local_kept], rows_kept[:, :, local_rows - local_kept :]], axis=2
    )
    columns_half = coeffs.shape[3] // 2
    return jnp.concatenate(
        [rows_kept[..., :halfway], rows_kept[..., columns_half : columns_half + halfway]], axis=3
    )


def prolong(coeffs, retained, groups):
    components, kept, local_kept, width = coeffs.shape
    halfway = kept // 2
    zeros_x = jnp.zeros((components, retained - kept, local_kept, width), jnp.float32)
    wider = jnp.concatenate([coeffs[:, :halfway], zeros_x, coeffs[:, halfway:]], axis=1)
    local_rows = retained // groups
    split_rows = local_kept // 2
    zeros_y = jnp.zeros((components, retained, local_rows - local_kept, width), jnp.float32)
    wider = jnp.concatenate([wider[:, :, :split_rows], zeros_y, wider[:, :, split_rows:]], axis=2)
    zeros_z = jnp.zeros((components, retained, local_rows, retained // 2 - halfway), jnp.float32)
    return jnp.concatenate([wider[..., :halfway], zeros_z, wider[..., halfway:], zeros_z], axis=3)


def wave_table(length):
    places = np.arange(length)
    return np.where(places < length // 2, places, places - length)


def trig_table(outer, inner, extent):
    radians = 2.0 * np.pi / extent * np.mod(np.outer(outer, inner), extent)
    return np.cos(radians), np.sin(radians)


def split_table(table):
    table = np.asarray(table, np.float32)
    high = table.astype(jnp.bfloat16)
    low = (table - high.astype(np.float32)).astype(jnp.bfloat16)
    return high, low


def split(values):
    high = values.astype(jnp.bfloat16)
    low = (values - high.astype(jnp.float32)).astype(jnp.bfloat16)
    return high, low


def dot3(left, right):
    def dot(a, b):
        return jnp.dot(a, b, preferred_element_type=jnp.float32)

    return dot(left[0], right[0]) + dot(left[0], right[1]) + dot(left[1], right[0])


def z_tables(extent, retained):
    halfway = retained // 2
    columns = np.arange(retained)
    harmonic = columns % halfway
    cosine, sine = trig_table(harmonic, np.arange(extent), extent)
    table = np.where((columns < halfway)[:, None], cosine, -sine)
    weight = np.where(harmonic == 0, 1.0, 2.0)[:, None] * retained ** (-0.5)
    return table * weight, table.T * (math.sqrt(retained) / extent)


def wave_order(retained, count_py, count_pz):
    groups = count_py * count_pz
    rows, near = retained // groups, count_pz // 2
    half, side, high, line, z_low, inner = np.meshgrid(
        np.arange(2),
        np.arange(2),
        np.arange(2),
        np.arange(count_py),
        np.arange(near),
        np.arange(rows // 4),
        indexing="ij",
    )
    owner = line * count_pz + side * near + z_low
    return (((high * 2 + half) * (rows // 4) + inner) * groups + owner).reshape(-1)


def plane_tables(extent, retained, count_py, count_pz):
    groups = count_py * count_pz
    rows = retained // groups
    places = np.arange(retained)
    wave_in = wave_table(retained)[wave_order(retained, count_py, count_pz)]
    wave_out = wave_table(retained)[places % rows * groups + places // rows]
    cosine, sine = trig_table(np.arange(extent), wave_in, extent)
    inverse_y = np.concatenate([cosine, sine], axis=1) * retained ** (-0.5)
    cosine, sine = trig_table(wave_out, np.arange(extent), extent)
    forward_y = np.concatenate([cosine, -sine], axis=1) * (math.sqrt(retained) / extent)
    inverse_last, forward_last = z_tables(extent, retained)
    halfway = retained // 2
    lanes = np.zeros((8, retained), np.float32)
    lanes[0] = np.where(places < halfway, -1.0, 1.0)
    lanes[1] = places % halfway
    column = np.broadcast_to(wave_in[:, None], (retained, retained)).astype(np.float32)
    tables = [lanes, column]
    for table in (inverse_y, inverse_last, forward_last, forward_y):
        tables += split_table(table)
    return tables


def plane_math(fields, tables):
    lanes, wave_y, iy0, iy1, iz0, iz1, fz0, fz1, fy0, fy1 = tables
    turn, wave_z = lanes[0:1, :], lanes[1:2, :]
    retained = wave_y.shape[0]
    extent = iy0.shape[0]

    def turned(values):
        return pltpu.roll(values, retained // 2, 1) * turn

    v0, v1, v2, d1, d2 = fields
    i0 = turned(v0)
    w0 = turned(wave_y * v2 - wave_z * v1)
    w1 = wave_z * i0 - d2
    w2 = d1 - wave_y * i0
    six = (v0, v1, v2, w0, w1, w2)
    stacked = jnp.concatenate(
        [jnp.concatenate(six, axis=1), jnp.concatenate([i0] + [turned(f) for f in six[1:]], axis=1)],
        axis=0,
    )
    along_y = dot3((iy0, iy1), split(stacked))
    rows = jnp.concatenate(
        [along_y[:, f * retained : (f + 1) * retained] for f in range(6)], axis=0
    )
    physical = dot3(split(rows), (iz0, iz1))
    u0, u1, u2, w0, w1, w2 = [physical[f * extent : (f + 1) * extent] for f in range(6)]
    product = jnp.concatenate([u1 * w2 - u2 * w1, u2 * w0 - u0 * w2, u0 * w1 - u1 * w0], axis=0)
    along_z = dot3(split(product), (fz0, fz1))
    parts = [along_z[f * extent : (f + 1) * extent] for f in range(3)]
    stacked = jnp.concatenate(
        [jnp.concatenate(parts, axis=1), jnp.concatenate([turned(p) for p in parts], axis=1)],
        axis=0,
    )
    result = dot3((fy0, fy1), split(stacked))
    return [result[:, f * retained : (f + 1) * retained] for f in range(3)]


def point_place(position, side, spot, plane, near_group, planes):
    return ((position * 2 + side) * near_group + spot) * planes + plane


def x_tables(extent, retained, count_py, count_pz, halves):
    near = count_pz // 2
    near_group = count_py * near
    planes = extent // (2 * near_group * halves)
    wave_x = wave_table(retained)
    plane, spot = np.meshgrid(np.arange(planes), np.arange(near_group), indexing="ij")
    inverse = []
    for position in range(halves):
        for side in range(2):
            points = point_place(position, side, spot, plane, near_group, planes).reshape(-1)
            cosine, sine = trig_table(points, wave_x, extent)
            values = np.concatenate([cosine, sine], axis=1)
            slopes = np.concatenate([-sine * wave_x, cosine * wave_x], axis=1)
            inverse.append(np.concatenate([values, slopes], axis=0))
    inverse = np.stack(inverse) * retained ** (-0.5)
    plane, position, line, side, z_low = np.meshgrid(
        np.arange(planes),
        np.arange(halves),
        np.arange(count_py),
        np.arange(2),
        np.arange(near),
        indexing="ij",
    )
    points = point_place(position, side, line * near + z_low, plane, near_group, planes)
    points = points.reshape(planes, -1)
    early = planes - 2
    forward = []
    for some in (points[:early].reshape(-1), points[early:].reshape(-1)):
        cosine, sine = trig_table(wave_x, some, extent)
        forward.append(np.concatenate([cosine, -sine], axis=1) * (math.sqrt(retained) / extent))
    column = np.broadcast_to(wave_x[:, None], (retained, retained)).astype(np.float32)
    tables = [column]
    for table in [inverse] + forward:
        tables += split_table(table)
    return tables


def step_kernel(*refs):
    stored = refs[0]
    kept_tables = refs[1:18]
    out = refs[18]
    loaded = refs[19:36]
    wave_x_ref, xi0, xi1, fa0, fa1, fb0, fb1 = loaded[:7]
    plane_refs = loaded[7:]
    raw, modes, spread, spread_mean, recv, recv_mean = refs[36:42]
    result, arrived, partial_sum, scales = refs[42:46]
    load_sem, table_sem, mode_send, own_recv, pair_recv = refs[46:51]
    field_send, field_recv, mean_recv, back_send, back_recv = refs[51:]

    _, retained, rows, _ = stored.shape
    planes, groups = result.shape[:2]
    halves = arrived.shape[1] // groups
    count_py, count_pz = lax.axis_size("py"), lax.axis_size("pz")
    near = count_pz // 2
    near_group = count_py * near
    band = rows // 2
    pairs = planes // 2
    early = planes - 2
    position = lax.axis_index("tm")
    row, place = lax.axis_index("py"), lax.axis_index("pz")
    side, z_low = place // near, lax.rem(place, near)
    spot = row * near + z_low
    member = row * count_pz + place
    pair_place = lax.rem(place + near, count_pz)
    pair_member = row * count_pz + pair_place

    def remote(source, target, send_sem, recv_sem, device):
        return pltpu.make_async_remote_copy(
            src_ref=source,
            dst_ref=target,
            send_sem=send_sem,
            recv_sem=recv_sem,
            device_id=device,
            device_id_type=pl.DeviceIdType.MESH,
        )

    def device(half, line, z_place):
        return {"tm": half, "py": line, "pz": z_place}

    across = device(1 - position, row, place)
    beside = device(position, row, pair_place)

    def turned(values):
        return pltpu.roll(values, retained // 2, 1) * turn

    def wave_y_of(a, owner):
        place_y = a * groups + owner
        return jnp.where(place_y < retained // 2, place_y, place_y - retained).astype(jnp.float32)

    def strided(ref, f, a):
        return ref.at[f].reshape(retained * rows, retained), pl.ds(a, retained, stride=rows)

    total = halves * groups
    barrier = pltpu.get_barrier_semaphore()

    def hello(other):
        pl.semaphore_signal(
            barrier, inc=1, device_id=other, device_id_type=pl.DeviceIdType.MESH
        )

    def greet(step, carry):
        other = lax.rem(spot + step, near_group)
        for half in range(halves):
            hello(device(half, other // near, side * near + lax.rem(other, near)))
        return carry

    hello(across)
    hello(beside)
    lax.fori_loop(1, near_group, greet, 0)

    @pl.when(position == 0)
    def _():
        pltpu.make_async_copy(stored, raw, load_sem).start()

    loads = [
        pltpu.make_async_copy(source, target, table_sem.at[i])
        for i, (source, target) in enumerate(zip(kept_tables, loaded))
    ]
    needed = (0, 7)
    for i in needed:
        loads[i].start()
    for i in needed:
        loads[i].wait()
    lanes = plane_refs[0]
    turn, wave_z = lanes[0:1, :], lanes[1:2, :]

    def project(values, wave_y):
        wave_x = wave_x_ref[...]
        squared = wave_x * wave_x + (wave_y * wave_y + wave_z * wave_z)
        divergence = (wave_x * values[0] + wave_y * values[1] + wave_z * values[2]) / jnp.maximum(
            squared, 1.0
        )
        projected = [
            values[0] - wave_x * divergence,
            values[1] - wave_y * divergence,
            values[2] - wave_z * divergence,
        ]
        return projected

    def flat_squares(wave_y):
        squares = wave_y * wave_y + wave_z * wave_z
        return squares < 0.5, 1.0 / jnp.maximum(squares, 1.0)

    @pl.when(position == 0)
    def _():
        pltpu.make_async_copy(stored, raw, load_sem).wait()

    for i, load in enumerate(loads):
        if i not in needed:
            load.start()

    def enter(start, stop):
        def first(a, carry):
            wave_y = wave_y_of(a, member)
            values = []
            for f in range(3):
                view, rows_of = strided(raw, f, a)
                values.append(view[rows_of, :])
            values = project(values, wave_y)
            for f in range(3):
                view, rows_of = strided(out, f, a)
                view[rows_of, :] = values[f]
            still, inverse = flat_squares(wave_y)
            turning = (wave_y * values[2] - wave_z * values[1]) * inverse
            modes[0, a, 0:retained, :] = jnp.where(still, values[1], values[0])
            modes[0, a, retained : 2 * retained, :] = jnp.where(still, values[2], turning)
            modes[0, a, 2 * retained : 2 * retained + 8, :] = values[0][0:8]
            return carry

        lax.fori_loop(start, stop, first, 0)

    @pl.when(position == 0)
    def _():
        enter(band, rows)

    pl.semaphore_wait(barrier, 2 * near_group)

    def rebuild(slot, a, owner):
        wave_y = wave_y_of(a, owner)
        wave_x = wave_x_ref[...]
        still, inverse = flat_squares(wave_y)
        first = modes[slot, a, 0:retained, :]
        second = modes[slot, a, retained : 2 * retained, :]
        mean = modes[slot, a, 2 * retained : 2 * retained + 1, :]
        pushed = wave_x * first
        v0 = jnp.where(still, jnp.where(wave_x == 0.0, mean, 0.0), first)
        v1 = jnp.where(still, first, -(wave_y * inverse) * pushed - wave_z * second)
        v2 = jnp.where(still, second, -(wave_z * inverse) * pushed + wave_y * second)
        return v0, v1, v2

    def own_copy(a):
        return remote(modes.at[0, a], modes.at[0, a], mode_send, own_recv.at[a], across)

    def pair_copy(a):
        return remote(modes.at[0, a], modes.at[1, a], mode_send, pair_recv.at[a], beside)

    def relay_copy(a):
        return remote(modes.at[1, a], modes.at[1, a], mode_send, pair_recv.at[a], across)

    def each(start, stop, do):
        def body(a, carry):
            do(a)
            return carry

        lax.fori_loop(start, stop, body, 0)

    few = band // 2
    final = 5
    crossing = 6
    late = 8

    def transform(step, slot, high, half):
        owner = pair_member if slot else member
        top_row = high * band + half * few
        fields = [rebuild(slot, top_row + a, owner) for a in range(few)]
        points = planes * near_group
        chunk = (1 - side if slot else side) * 2 + high
        slots = (half * 4 + chunk) * near_group
        mean_slots = chunk * near_group
        complete = step % 2 == 1
        operands = []
        for f in (1, 2, 0):
            parts = [fields[a][f] for a in range(few)]
            stacked = jnp.concatenate(
                [
                    jnp.concatenate(parts, axis=1),
                    jnp.concatenate([turned(p) for p in parts], axis=1),
                ],
                axis=0,
            )
            operands.append((f, split(stacked)))

        def deliver(target, place_in, away):
            tables = (xi0[target * 2 + side], xi1[target * 2 + side])
            for f, stacked in operands:
                count = 2 if f else 1
                moved = dot3([t[: count * points] for t in tables], stacked)
                for p in range(planes):
                    for c in range(count):
                        if f:
                            view, offset = spread.at[place_in, p], 2 * (f - 1) + c
                        else:
                            view, offset = spread_mean.at[place_in // 2, p // 2], 2 * half + p % 2
                        view = view.reshape(near_group * rows, retained)
                        top = c * points + p * near_group
                        for a in range(few):
                            view[pl.ds(4 * a + offset, near_group, stride=rows), :] = moved[
                                top : top + near_group, a * retained : (a + 1) * retained
                            ]
            if not away:
                recv[:, slots + spot] = spread[place_in, :, spot]
                if complete:
                    recv_mean[:, mean_slots + spot] = spread_mean[place_in // 2, :, spot]

            def send(other, first, count, index, mean_index):
                to = device(target, other // near, side * near + lax.rem(other, near))
                remote(
                    spread.at[place_in, pl.ds(2 * first, 2 * count), other],
                    recv.at[pl.ds(2 * first, 2 * count), slots + spot],
                    field_send,
                    field_recv.at[index],
                    to,
                ).start()
                if complete:
                    remote(
                        spread_mean.at[place_in // 2, pl.ds(first, count), other],
                        recv_mean.at[pl.ds(first, count), mean_slots + spot],
                        field_send,
                        mean_recv.at[mean_index],
                        to,
                    ).start()

            index, mean_index = field_index(place_in), mean_index_of(place_in)
            spans = [(0, pairs, index, mean_index)]
            if step in (final, late + 1):
                spans = [(k, 1, index + k, mean_index + k) for k in range(pairs)]
            for span in spans:

                def push(turn_index, carry, span=span, send=send):
                    send(lax.rem(spot + near_group - turn_index, near_group), *span)
                    return carry

                lax.fori_loop(0 if away else 1, near_group, push, 0)

        if step in (final - 1, final):

            @pl.when(position == 0)
            def _():
                deliver(1, step + 2, True)

        deliver(position, step, False)

    def field_index(place_in):
        if place_in >= late:
            place_in -= 2
        return place_in if place_in <= final else place_in - 1 + pairs

    def mean_index_of(place_in):
        return place_in // 2 if place_in <= final else final // 2 + pairs

    def await_fields(first, count, index, senders):
        some = recv.at[pl.ds(2 * first, 2 * count), pl.ds(0, senders)]
        remote(some, some, field_send, field_recv.at[index], beside).wait_recv()

    def await_means(first, count, index, senders):
        some = recv_mean.at[pl.ds(first, count), pl.ds(0, senders)]
        remote(some, some, field_send, mean_recv.at[index], beside).wait_recv()

    low, high = list(range(band)), list(range(band, rows))
    own_order = high + low[::-1]

    def send_pair(rows_of):
        for a in rows_of:
            pair_copy(a).start()

    def take_own(rows_of):
        for a in rows_of:
            own_copy(a).wait_recv()
            if a in high:
                pair_copy(a).start()

    def take_pair(rows_of):
        for a in rows_of:
            pair_copy(a).wait_recv()
            if a in high:

                @pl.when(position == 1)
                def _():
                    relay_copy(a).start()

    def on(which, do):
        @pl.when(position == which)
        def _():
            do()

    def start_first():
        for a in high:
            own_copy(a).start()
        enter(0, band)
        send_pair(low[:2])
        for a in low[::-1]:
            own_copy(a).start()

    on(0, start_first)
    for i, load in enumerate(loads):
        if i not in needed:
            load.wait()
    on(1, lambda: take_own(high[:few]))
    transform(0, 0, 1, 0)
    on(0, lambda: send_pair(low[2:3]))
    on(1, lambda: take_own(high[few:]))
    transform(1, 0, 1, 1)
    on(0, lambda: send_pair(low[3:]))
    on(1, lambda: take_own(low[few:][::-1]))
    on(1, lambda: take_pair(high[:1]))
    transform(2, 0, 0, 1)
    on(1, lambda: take_own(low[:few][::-1]))
    transform(3, 0, 0, 0)
    on(0, lambda: take_pair(low[:few]))
    on(1, lambda: take_pair(high[1:few]))
    transform(4, 1, position, 0)
    on(0, lambda: take_pair(low[few:]))
    on(1, lambda: take_pair(high[few:]))
    transform(5, 1, position, 1)

    def finish_late():
        take_pair(high[:few])
        transform(late, 1, 1, 0)
        take_pair(high[few:])
        transform(late + 1, 1, 1, 1)

    on(0, finish_late)

    for step in range(final):
        await_fields(0, pairs, step, near_group - 1)
    for step in range(final // 2):
        await_means(0, pairs, step, near_group - 1)
    on(0, lambda: await_fields(0, pairs, field_index(crossing), near_group - 1))
    on(1, lambda: await_fields(0, pairs, field_index(crossing), near_group))

    tables = [ref[...] for ref in plane_refs]

    def plane_pair(k, carry):
        await_fields(k, 1, final + k, near_group - 1)
        await_means(k, 1, final // 2 + k, near_group - 1)

        def await_last(senders):
            await_fields(k, 1, field_index(crossing + 1) + k, senders)
            await_means(k, 1, mean_index_of(crossing) + k, senders)

        on(0, lambda: await_last(near_group - 1))
        on(1, lambda: await_last(near_group))

        def plane(odd, carry):
            p = 2 * k + odd

            view = recv.at[p].reshape(8 * near_group * rows, retained)
            v1, d1, v2, d2 = [view[pl.ds(i, retained, stride=4), :] for i in range(4)]
            view = recv_mean.at[k].reshape(4 * near_group * rows, retained)
            v0 = jnp.concatenate(
                [
                    view[pl.ds(2 * half + odd, retained // 2, stride=4), :]
                    for half in range(2)
                ],
                axis=0,
            )
            for f, values in enumerate(plane_math([v0, v1, v2, d1, d2], tables)):
                result[p, :, f] = values.reshape(groups, rows, retained)

            def push(turn_index, carry):
                to_place = lax.rem(place + near + turn_index // count_py, count_pz)
                to_row = lax.rem(row + turn_index, count_py)
                to_member = to_row * count_pz + to_place

                @pl.when(jnp.logical_or(position == 0, to_member != member))
                def _():
                    remote(
                        result.at[p, to_member],
                        arrived.at[p, position * groups + member],
                        back_send,
                        back_recv.at[p],
                        device(1, to_row, to_place),
                    ).start()

                return carry

            lax.fori_loop(0, groups, push, 0)

            @pl.when(position == 1)
            def _():
                arrived[p, groups + member] = result[p, member]

            return carry

        return lax.fori_loop(0, 2, plane, carry)

    lax.fori_loop(0, pairs, plane_pair, 0)

    def gather(start, count, a):
        view = arrived.reshape(planes * total * 3 * rows, retained)
        wide = jnp.concatenate(
            [
                view[pl.ds((start * total * 3 + f) * rows + a, count * total, stride=3 * rows), :]
                for f in range(3)
            ],
            axis=1,
        )
        back = jnp.concatenate(
            [
                turned(wide[:, f * retained : (f + 1) * retained])
                for f in range(3)
            ],
            axis=1,
        )
        return split(jnp.concatenate([wide, back], axis=0))

    @pl.when(position == 1)
    def _():
        def await_plane(p):
            some = arrived.at[p, pl.ds(0, total - 1)]
            remote(some, some, back_send, back_recv.at[p], beside).wait_recv()

        each(0, early, await_plane)

        def begin(a):
            before = jnp.concatenate(rebuild(0, a, member), axis=1)
            change = dot3((fa0[...], fa1[...]), gather(0, early, a))
            partial_sum[a] = before + time_step * change
            wave_x, wave_y = wave_x_ref[...], wave_y_of(a, member)
            squared = wave_x * wave_x + (wave_y * wave_y + wave_z * wave_z)
            damping = jnp.exp((-viscosity * time_step) * squared)
            scales[0, a] = damping
            scales[1, a] = damping / jnp.maximum(squared, 1.0)

        each(0, rows, begin)
        each(early, planes, await_plane)

        def finish(pair):
            sides = [gather(early, planes - early, 2 * pair + i) for i in range(2)]
            both = [jnp.concatenate(parts, axis=1) for parts in zip(*sides)]
            change = dot3((fb0[...], fb1[...]), both)
            for i in range(2):
                a = 2 * pair + i
                after = partial_sum[a] + time_step * change[:, 3 * i * retained : 3 * (i + 1) * retained]
                values = [after[:, f * retained : (f + 1) * retained] for f in range(3)]
                waves = (wave_x_ref[...], wave_y_of(a, member), wave_z)
                inner = sum(wave * value for wave, value in zip(waves, values)) * scales[1, a]
                for f in range(3):
                    view, rows_of = strided(out, f, a)
                    view[rows_of, :] = scales[0, a] * values[f] - waves[f] * inner

        each(0, rows // 2, finish)

    def await_sends(*sent):
        for some in sent:
            remote(some, some, field_send, field_recv.at[0], beside).wait_send()

    others = pl.ds(0, near_group - 1)
    await_sends(
        spread.at[pl.ds(0, crossing), :, others],
        spread_mean.at[pl.ds(0, crossing // 2), :, others],
    )

    @pl.when(position == 0)
    def _():
        await_sends(
            spread.at[pl.ds(crossing, 2)],
            spread_mean.at[crossing // 2],
            spread.at[pl.ds(late, 2), :, others],
            spread_mean.at[late // 2, :, others],
        )

    some = modes.at[1, pl.ds(0, band)]
    remote(modes.at[0], modes.at[0], mode_send, own_recv.at[0], beside).wait_send()

    @pl.when(position == 0)
    def _():
        remote(some, some, mode_send, own_recv.at[0], beside).wait_send()
        remote(result, result, back_send, back_recv.at[0], beside).wait_send()

    @pl.when(position == 1)
    def _():
        some = result.at[:, pl.ds(0, groups - 1)]
        remote(some, some, back_send, back_recv.at[0], beside).wait_send()


def helped_advance(stored, count_py, count_pz, halves):
    _, retained, rows, _ = stored.shape
    groups = count_py * count_pz
    extent = 3 * retained // 2
    near_group = groups // 2
    planes = extent // (groups * halves)
    pairs = planes // 2
    tables = x_tables(extent, retained, count_py, count_pz, halves)
    tables += plane_tables(extent, retained, count_py, count_pz)
    tables = [jnp.asarray(table) for table in tables]
    vmem = pl.BlockSpec(memory_space=pltpu.VMEM)
    return pl.pallas_call(
        step_kernel,
        in_specs=[pl.BlockSpec(memory_space=pl.ANY)] * (1 + len(tables)),
        out_specs=vmem,
        out_shape=pltpu.VMEM(stored.shape, jnp.float32),
        scratch_shapes=[pltpu.VMEM(table.shape, table.dtype) for table in tables]
        + [
            pltpu.VMEM(stored.shape, jnp.float32),
            pltpu.VMEM((2, rows, 2 * retained + 8, retained), jnp.float32),
            pltpu.VMEM((10, planes, near_group, rows, retained), jnp.float32),
            pltpu.VMEM((5, pairs, near_group, rows, retained), jnp.float32),
            pltpu.VMEM((planes, 8 * near_group, rows, retained), jnp.float32),
            pltpu.VMEM((pairs, 4 * near_group, rows, retained), jnp.float32),
            pltpu.VMEM((planes, groups, 3, rows, retained), jnp.float32),
            pltpu.VMEM((planes, halves * groups, 3, rows, retained), jnp.float32),
            pltpu.VMEM((rows, retained, 3 * retained), jnp.float32),
            pltpu.VMEM((2, rows, retained, retained), jnp.float32),
            pltpu.SemaphoreType.DMA,
            pltpu.SemaphoreType.DMA((len(tables),)),
            pltpu.SemaphoreType.DMA,
            pltpu.SemaphoreType.DMA((rows,)),
            pltpu.SemaphoreType.DMA((rows,)),
            pltpu.SemaphoreType.DMA,
            pltpu.SemaphoreType.DMA((6 + 2 * pairs,)),
            pltpu.SemaphoreType.DMA((2 + 2 * pairs,)),
            pltpu.SemaphoreType.DMA,
            pltpu.SemaphoreType.DMA((planes,)),
        ],
        compiler_params=pltpu.CompilerParams(
            has_side_effects=True, collective_id=0, vmem_limit_bytes=56 * 1024 * 1024
        ),
        name="step",
    )(stored, *tables)


def shards(start_states):
    count_py = lax.axis_size("py")
    count_pz = lax.axis_size("pz")
    groups = count_py * count_pz
    member = lax.axis_index("py") * count_pz + lax.axis_index("pz")
    layout = (count_py, count_pz, groups, member)
    position = lax.axis_index("tm")
    slices = lax.axis_size("tm")
    retained = start_states.shape[-1]
    stored = start_states.reshape(3, retained, start_states.shape[3], retained)
    if slices == 2:
        result = helped_advance(stored, count_py, count_pz, slices)
        return result.reshape(1, 3, retained, stored.shape[2], 1, retained)
    spectral_state = project(stored, wave_grid(retained, layout))
    fine_end = advance(spectral_state, "fine", layout)
    coarse_start = restrict(spectral_state, M, groups)
    coarse_next = advance(coarse_start, "coarse", layout)
    fine_low = restrict(fine_end, M, groups)
    correction = fine_low - coarse_next

    def relay(chained):
        return shifted(chained, "tm", 1)

    current = jnp.where(position == 1, relay(fine_low), coarse_start)

    def sweep_turn(turn_index, current):
        candidate = advance(current, "coarse", layout) + correction
        arrived = relay(candidate)
        return jnp.where(position == turn_index + 1, arrived, current)

    current = lax.fori_loop(1, slices - 1, sweep_turn, current)
    upper_band = fine_end - prolong(fine_low, retained, groups)
    previous = shifted(upper_band, "tm", 1)
    updated = prolong(current, retained, groups) + previous
    result = jnp.where(position == 0, spectral_state, updated)
    return result.reshape(1, result.shape[0], retained, result.shape[2], 1, retained)


def solution(mesh):
    in_specs = (P("tm", None, None, None, ("py", "pz"), None),)
    out_specs = P("tm", None, None, None, ("py", "pz"), None)
    return jax.shard_map(shards, mesh=mesh, in_specs=in_specs, out_specs=out_specs, check_vma=False)
```

```python
from functools import partial
import math

import jax
import jax.numpy as jnp
from jax import lax
import numpy as np
from jax.experimental import pallas as pl
from jax.experimental.pallas import tpu as pltpu
from jax.sharding import PartitionSpec as P

M = 64


viscosity = 0.03
time_step = 0.004
highest = lax.Precision.HIGHEST


def shifted(block, axis, distance):
    devices = range(lax.axis_size(axis))
    route = [(i - distance, i) for i in devices if i - distance in devices]
    return lax.ppermute(block, axis, route)


def signed_wave(places, length):
    return jnp.where(places < length // 2, places, places - length)


def rotate(values):
    halfway = values.shape[-1] // 2
    return jnp.concatenate([-values[..., halfway:], values[..., :halfway]], axis=-1)


def trig_pair(outer, inner, extent, factor):
    residue = jnp.mod(outer[:, None] * inner[None, :], extent)
    radians = residue.astype(jnp.float32) * (2.0 * math.pi / extent)
    return (jnp.cos(radians) * factor, jnp.sin(radians) * factor)


def complex_apply(cosine_part, sine_part, values, contracted, direction_sign):
    kernel = jnp.stack(
        [
            jnp.stack([cosine_part, -direction_sign * sine_part]),
            jnp.stack([direction_sign * sine_part, cosine_part]),
        ]
    )
    halfway = values.shape[-1] // 2
    split = values.reshape(values.shape[:-1] + (2, halfway))
    if contracted == 1:
        pattern = "pqok,fkaqh->foaph"
    else:
        pattern = "pqok,flkqh->floph"
    result = jnp.einsum(pattern, kernel, split, precision=highest)
    return result.reshape(result.shape[:-2] + (2 * halfway,))


def inverse_z(extent, retained):
    halfway = retained // 2
    columns = jnp.arange(retained, dtype=jnp.int32)
    harmonic = columns % halfway
    weight = jnp.where(harmonic == 0, 1.0, 2.0) * retained ** (-0.5)
    residue = jnp.mod(harmonic[:, None] * jnp.arange(extent, dtype=jnp.int32)[None, :], extent)
    radians = residue.astype(jnp.float32) * (2.0 * math.pi / extent)
    return (
        jnp.where((columns < halfway)[:, None], jnp.cos(radians), -jnp.sin(radians))
        * weight[:, None]
    )


def forward_z(extent, retained):
    halfway = retained // 2
    columns = jnp.arange(retained, dtype=jnp.int32)
    harmonic = columns % halfway
    residue = jnp.mod(jnp.arange(extent, dtype=jnp.int32)[:, None] * harmonic[None, :], extent)
    radians = residue.astype(jnp.float32) * (2.0 * math.pi / extent)
    return jnp.where((columns < halfway)[None, :], jnp.cos(radians), -jnp.sin(radians)) * (
        math.sqrt(retained) / extent
    )


def inverse_tail(portion, extent, sectioned, layout):
    count_py, count_pz, groups, member = layout
    retained = portion.shape[2]
    local_rows = retained // groups
    places = jnp.arange(retained, dtype=jnp.int32)
    owners = places // local_rows
    wave_y = signed_wave(places % local_rows * groups + owners, retained)
    points = jnp.arange(extent, dtype=jnp.int32)
    cosine_part, sine_part = trig_pair(points, wave_y, extent, retained ** (-0.5))
    along_y = complex_apply(cosine_part, sine_part, portion, 2, 1.0)
    return jnp.einsum("flyr,rz->flyz", along_y, inverse_z(extent, retained), precision=highest)


def forward_tail(portion, retained, sectioned, layout):
    count_py, count_pz, groups, member = layout
    extent = portion.shape[1]
    local_rows = extent // groups
    places = jnp.arange(extent, dtype=jnp.int32)
    points = places // local_rows * local_rows + places % local_rows
    wave_x = signed_wave(jnp.arange(retained, dtype=jnp.int32), retained)
    cosine_part, sine_part = trig_pair(wave_x, points, extent, math.sqrt(retained) / extent)
    return complex_apply(cosine_part, sine_part, portion, 1, -1.0)


def to_physical(coeffs, wavegrid, extent, resolution, layout):
    wave_x, wave_y, wave_z = wavegrid
    retained = coeffs.shape[1]
    seeds = jnp.concatenate([coeffs, wave_x * coeffs[1:3]], axis=0)
    points = jnp.arange(extent, dtype=jnp.int32)
    wave_rows = signed_wave(jnp.arange(retained, dtype=jnp.int32), retained)
    cosine_part, sine_part = trig_pair(points, wave_rows, extent, retained ** (-0.5))
    moved_x = complex_apply(cosine_part, sine_part, seeds, 1, 1.0)
    curl_x = rotate(wave_y * moved_x[2] - wave_z * moved_x[1])
    curl_y = rotate(wave_z * moved_x[0] - moved_x[4])
    curl_z = rotate(moved_x[3] - wave_y * moved_x[0])
    spread = jnp.concatenate([moved_x[:3], jnp.stack([curl_x, curl_y, curl_z])], axis=0)
    if resolution == "coarse":
        finish = partial(inverse_tail, extent=extent, sectioned=False, layout=layout)
        return finish(lax.all_to_all(spread, ("py", "pz"), split_axis=1, concat_axis=2, tiled=True))
    else:
        finish = partial(inverse_tail, extent=extent, sectioned=False, layout=layout)
        return finish(lax.all_to_all(spread, ("py", "pz"), split_axis=1, concat_axis=2, tiled=True))


def to_spectral(fields, retained, resolution, layout):
    count_py, count_pz, groups, member = layout
    extent = fields.shape[-1]
    along_z = jnp.einsum("flyz,zr->flyr", fields, forward_z(extent, retained), precision=highest)
    local_rows = retained // groups
    places = jnp.arange(retained, dtype=jnp.int32)
    wave_y = signed_wave(places % local_rows * groups + places // local_rows, retained)
    cosine_part, sine_part = trig_pair(
        wave_y, jnp.arange(extent, dtype=jnp.int32), extent, math.sqrt(retained) / extent
    )
    along_y = complex_apply(cosine_part, sine_part, along_z, 2, -1.0)
    if resolution == "coarse":
        finish = partial(forward_tail, retained=retained, sectioned=False, layout=layout)
        return finish(
            lax.all_to_all(along_y, ("py", "pz"), split_axis=2, concat_axis=1, tiled=True)
        )
    else:
        finish = partial(forward_tail, retained=retained, sectioned=False, layout=layout)
        return finish(
            lax.all_to_all(along_y, ("py", "pz"), split_axis=2, concat_axis=1, tiled=True)
        )


def wave_grid(retained, layout):
    count_py, count_pz, groups, member = layout
    places = jnp.arange(retained, dtype=jnp.int32)
    wave_x = signed_wave(places, retained).astype(jnp.float32)[:, None, None]
    local_places = jnp.arange(retained // groups, dtype=jnp.int32)
    wave_y = signed_wave(local_places * groups + member, retained).astype(jnp.float32)[
        None, :, None
    ]
    wave_z = (places % (retained // 2)).astype(jnp.float32)[None, None, :]
    return (wave_x, wave_y, wave_z)


def project(coeffs, wavegrid):
    wave_x, wave_y, wave_z = wavegrid
    squared = wave_x * wave_x + wave_y * wave_y + wave_z * wave_z
    divergence = (wave_x * coeffs[0] + wave_y * coeffs[1] + wave_z * coeffs[2]) / jnp.maximum(
        squared, 1.0
    )
    return jnp.stack(
        [
            coeffs[0] - wave_x * divergence,
            coeffs[1] - wave_y * divergence,
            coeffs[2] - wave_z * divergence,
        ]
    )


def cross_product(first_field, second_field):
    return jnp.stack(
        [
            first_field[1] * second_field[2] - first_field[2] * second_field[1],
            first_field[2] * second_field[0] - first_field[0] * second_field[2],
            first_field[0] * second_field[1] - first_field[1] * second_field[0],
        ]
    )


def advance(coeffs, resolution, layout):
    retained = coeffs.shape[1]
    extent = 3 * retained // 2
    wavegrid = wave_grid(retained, layout)
    fields = to_physical(coeffs, wavegrid, extent, resolution, layout)
    product = cross_product(fields[:3], fields[3:])
    nonlinear = to_spectral(product, retained, resolution, layout)
    wave_x, wave_y, wave_z = wavegrid
    squared = wave_x * wave_x + wave_y * wave_y + wave_z * wave_z
    damping = jnp.exp(-viscosity * time_step * squared)
    return damping * (coeffs + time_step * project(nonlinear, wavegrid))


def restrict(coeffs, kept, groups):
    halfway = kept // 2
    retained = coeffs.shape[1]
    rows_kept = jnp.concatenate([coeffs[:, :halfway], coeffs[:, retained - halfway :]], axis=1)
    local_rows = coeffs.shape[2]
    local_kept = kept // groups // 2
    rows_kept = jnp.concatenate(
        [rows_kept[:, :, :local_kept], rows_kept[:, :, local_rows - local_kept :]], axis=2
    )
    columns_half = coeffs.shape[3] // 2
    return jnp.concatenate(
        [rows_kept[..., :halfway], rows_kept[..., columns_half : columns_half + halfway]], axis=3
    )


def prolong(coeffs, retained, groups):
    components, kept, local_kept, width = coeffs.shape
    halfway = kept // 2
    zeros_x = jnp.zeros((components, retained - kept, local_kept, width), jnp.float32)
    wider = jnp.concatenate([coeffs[:, :halfway], zeros_x, coeffs[:, halfway:]], axis=1)
    local_rows = retained // groups
    split_rows = local_kept // 2
    zeros_y = jnp.zeros((components, retained, local_rows - local_kept, width), jnp.float32)
    wider = jnp.concatenate([wider[:, :, :split_rows], zeros_y, wider[:, :, split_rows:]], axis=2)
    zeros_z = jnp.zeros((components, retained, local_rows, retained // 2 - halfway), jnp.float32)
    return jnp.concatenate([wider[..., :halfway], zeros_z, wider[..., halfway:], zeros_z], axis=3)


def wave_table(length):
    places = np.arange(length)
    return np.where(places < length // 2, places, places - length)


def trig_table(outer, inner, extent):
    radians = 2.0 * np.pi / extent * np.mod(np.outer(outer, inner), extent)
    return np.cos(radians), np.sin(radians)


def split_table(table):
    table = np.asarray(table, np.float32)
    high = table.astype(jnp.bfloat16)
    low = (table - high.astype(np.float32)).astype(jnp.bfloat16)
    return high, low


def split(values):
    high = values.astype(jnp.bfloat16)
    low = (values - high.astype(jnp.float32)).astype(jnp.bfloat16)
    return high, low


def dot3(left, right):
    def dot(a, b):
        return jnp.dot(a, b, preferred_element_type=jnp.float32)

    return dot(left[0], right[0]) + dot(left[0], right[1]) + dot(left[1], right[0])


def z_tables(extent, retained):
    halfway = retained // 2
    columns = np.arange(retained)
    harmonic = columns % halfway
    cosine, sine = trig_table(harmonic, np.arange(extent), extent)
    table = np.where((columns < halfway)[:, None], cosine, -sine)
    weight = np.where(harmonic == 0, 1.0, 2.0)[:, None] * retained ** (-0.5)
    return table * weight, table.T * (math.sqrt(retained) / extent)


def wave_order(retained, count_py, count_pz):
    groups = count_py * count_pz
    rows, near = retained // groups, count_pz // 2
    half, side, high, line, z_low, inner = np.meshgrid(
        np.arange(2),
        np.arange(2),
        np.arange(2),
        np.arange(count_py),
        np.arange(near),
        np.arange(rows // 4),
        indexing="ij",
    )
    owner = line * count_pz + side * near + z_low
    return (((high * 2 + half) * (rows // 4) + inner) * groups + owner).reshape(-1)


def plane_tables(extent, retained, count_py, count_pz):
    groups = count_py * count_pz
    rows = retained // groups
    places = np.arange(retained)
    wave_in = wave_table(retained)[wave_order(retained, count_py, count_pz)]
    wave_out = wave_table(retained)[places % rows * groups + places // rows]
    cosine, sine = trig_table(np.arange(extent), wave_in, extent)
    inverse_y = np.concatenate([cosine, sine], axis=1) * retained ** (-0.5)
    cosine, sine = trig_table(wave_out, np.arange(extent), extent)
    forward_y = np.concatenate([cosine, -sine], axis=1) * (math.sqrt(retained) / extent)
    inverse_last, forward_last = z_tables(extent, retained)
    halfway = retained // 2
    lanes = np.zeros((8, retained), np.float32)
    lanes[0] = np.where(places < halfway, -1.0, 1.0)
    lanes[1] = places % halfway
    column = np.broadcast_to(wave_in[:, None], (retained, retained)).astype(np.float32)
    tables = [lanes, column]
    for table in (inverse_y, inverse_last, forward_last, forward_y):
        tables += split_table(table)
    return tables


def plane_math(fields, tables):
    lanes, wave_y, iy0, iy1, iz0, iz1, fz0, fz1, fy0, fy1 = tables
    turn, wave_z = lanes[0:1, :], lanes[1:2, :]
    retained = wave_y.shape[0]
    extent = iy0.shape[0]

    def turned(values):
        return pltpu.roll(values, retained // 2, 1) * turn

    v0, v1, v2, d1, d2 = fields
    i0 = turned(v0)
    w0 = turned(wave_y * v2 - wave_z * v1)
    w1 = wave_z * i0 - d2
    w2 = d1 - wave_y * i0
    six = (v0, v1, v2, w0, w1, w2)
    stacked = jnp.concatenate(
        [jnp.concatenate(six, axis=1), jnp.concatenate([i0] + [turned(f) for f in six[1:]], axis=1)],
        axis=0,
    )
    along_y = dot3((iy0, iy1), split(stacked))
    rows = jnp.concatenate(
        [along_y[:, f * retained : (f + 1) * retained] for f in range(6)], axis=0
    )
    physical = dot3(split(rows), (iz0, iz1))
    u0, u1, u2, w0, w1, w2 = [physical[f * extent : (f + 1) * extent] for f in range(6)]
    product = jnp.concatenate([u1 * w2 - u2 * w1, u2 * w0 - u0 * w2, u0 * w1 - u1 * w0], axis=0)
    along_z = dot3(split(product), (fz0, fz1))
    parts = [along_z[f * extent : (f + 1) * extent] for f in range(3)]
    stacked = jnp.concatenate(
        [jnp.concatenate(parts, axis=1), jnp.concatenate([turned(p) for p in parts], axis=1)],
        axis=0,
    )
    result = dot3((fy0, fy1), split(stacked))
    return [result[:, f * retained : (f + 1) * retained] for f in range(3)]


def point_place(position, side, spot, plane, near_group, planes):
    return ((position * 2 + side) * near_group + spot) * planes + plane


def x_tables(extent, retained, count_py, count_pz, halves):
    near = count_pz // 2
    near_group = count_py * near
    planes = extent // (2 * near_group * halves)
    wave_x = wave_table(retained)
    plane, spot = np.meshgrid(np.arange(planes), np.arange(near_group), indexing="ij")
    inverse = []
    for position in range(halves):
        for side in range(2):
            points = point_place(position, side, spot, plane, near_group, planes).reshape(-1)
            cosine, sine = trig_table(points, wave_x, extent)
            values = np.concatenate([cosine, sine], axis=1)
            slopes = np.concatenate([-sine * wave_x, cosine * wave_x], axis=1)
            inverse.append(np.concatenate([values, slopes], axis=0))
    inverse = np.stack(inverse) * retained ** (-0.5)
    plane, position, line, side, z_low = np.meshgrid(
        np.arange(planes),
        np.arange(halves),
        np.arange(count_py),
        np.arange(2),
        np.arange(near),
        indexing="ij",
    )
    points = point_place(position, side, line * near + z_low, plane, near_group, planes)
    points = points.reshape(planes, -1)
    early = planes - 2
    forward = []
    for some in (points[:early].reshape(-1), points[early:].reshape(-1)):
        cosine, sine = trig_table(wave_x, some, extent)
        forward.append(np.concatenate([cosine, -sine], axis=1) * (math.sqrt(retained) / extent))
    column = np.broadcast_to(wave_x[:, None], (retained, retained)).astype(np.float32)
    tables = [column]
    for table in [inverse] + forward:
        tables += split_table(table)
    return tables


def step_kernel(*refs):
    stored = refs[0]
    kept_tables = refs[1:18]
    out = refs[18]
    loaded = refs[19:36]
    wave_x_ref, xi0, xi1, fa0, fa1, fb0, fb1 = loaded[:7]
    plane_refs = loaded[7:]
    raw, modes, spread, spread_mean, recv, recv_mean = refs[36:42]
    result, arrived, partial_sum, scales = refs[42:46]
    load_sem, table_sem, mode_send, own_recv, pair_recv = refs[46:51]
    field_send, field_recv, mean_recv, back_send, back_recv = refs[51:]

    _, retained, rows, _ = stored.shape
    planes, groups = result.shape[:2]
    halves = arrived.shape[1] // groups
    count_py, count_pz = lax.axis_size("py"), lax.axis_size("pz")
    near = count_pz // 2
    near_group = count_py * near
    band = rows // 2
    pairs = planes // 2
    early = planes - 2
    position = lax.axis_index("tm")
    row, place = lax.axis_index("py"), lax.axis_index("pz")
    side, z_low = place // near, lax.rem(place, near)
    spot = row * near + z_low
    member = row * count_pz + place
    pair_place = lax.rem(place + near, count_pz)
    pair_member = row * count_pz + pair_place

    def remote(source, target, send_sem, recv_sem, device):
        return pltpu.make_async_remote_copy(
            src_ref=source,
            dst_ref=target,
            send_sem=send_sem,
            recv_sem=recv_sem,
            device_id=device,
            device_id_type=pl.DeviceIdType.MESH,
        )

    def device(half, line, z_place):
        return {"tm": half, "py": line, "pz": z_place}

    across = device(1 - position, row, place)
    beside = device(position, row, pair_place)

    def turned(values):
        return pltpu.roll(values, retained // 2, 1) * turn

    def wave_y_of(a, owner):
        place_y = a * groups + owner
        return jnp.where(place_y < retained // 2, place_y, place_y - retained).astype(jnp.float32)

    def strided(ref, f, a):
        return ref.at[f].reshape(retained * rows, retained), pl.ds(a, retained, stride=rows)

    total = halves * groups
    barrier = pltpu.get_barrier_semaphore()

    def hello(other):
        pl.semaphore_signal(
            barrier, inc=1, device_id=other, device_id_type=pl.DeviceIdType.MESH
        )

    def greet(step, carry):
        other = lax.rem(spot + step, near_group)
        for half in range(halves):
            hello(device(half, other // near, side * near + lax.rem(other, near)))
        return carry

    hello(across)
    hello(beside)
    lax.fori_loop(1, near_group, greet, 0)

    @pl.when(position == 0)
    def _():
        pltpu.make_async_copy(stored, raw, load_sem).start()

    loads = [
        pltpu.make_async_copy(source, target, table_sem.at[i])
        for i, (source, target) in enumerate(zip(kept_tables, loaded))
    ]
    needed = (0, 7)
    for i in needed:
        loads[i].start()
    for i in needed:
        loads[i].wait()
    lanes = plane_refs[0]
    turn, wave_z = lanes[0:1, :], lanes[1:2, :]

    def project(values, wave_y):
        wave_x = wave_x_ref[...]
        squared = wave_x * wave_x + (wave_y * wave_y + wave_z * wave_z)
        divergence = (wave_x * values[0] + wave_y * values[1] + wave_z * values[2]) / jnp.maximum(
            squared, 1.0
        )
        projected = [
            values[0] - wave_x * divergence,
            values[1] - wave_y * divergence,
            values[2] - wave_z * divergence,
        ]
        return projected

    def flat_squares(wave_y):
        squares = wave_y * wave_y + wave_z * wave_z
        return squares < 0.5, 1.0 / jnp.maximum(squares, 1.0)

    @pl.when(position == 0)
    def _():
        pltpu.make_async_copy(stored, raw, load_sem).wait()

    for i, load in enumerate(loads):
        if i not in needed:
            load.start()

    def enter(start, stop):
        def first(a, carry):
            wave_y = wave_y_of(a, member)
            values = []
            for f in range(3):
                view, rows_of = strided(raw, f, a)
                values.append(view[rows_of, :])
            values = project(values, wave_y)
            for f in range(3):
                view, rows_of = strided(out, f, a)
                view[rows_of, :] = values[f]
            still, inverse = flat_squares(wave_y)
            turning = (wave_y * values[2] - wave_z * values[1]) * inverse
            modes[0, a, 0:retained, :] = jnp.where(still, values[1], values[0])
            modes[0, a, retained : 2 * retained, :] = jnp.where(still, values[2], turning)
            modes[0, a, 2 * retained : 2 * retained + 8, :] = values[0][0:8]
            return carry

        lax.fori_loop(start, stop, first, 0)

    @pl.when(position == 0)
    def _():
        enter(band, rows)

    pl.semaphore_wait(barrier, 2 * near_group)

    def rebuild(slot, a, owner):
        wave_y = wave_y_of(a, owner)
        wave_x = wave_x_ref[...]
        still, inverse = flat_squares(wave_y)
        first = modes[slot, a, 0:retained, :]
        second = modes[slot, a, retained : 2 * retained, :]
        mean = modes[slot, a, 2 * retained : 2 * retained + 1, :]
        pushed = wave_x * first
        v0 = jnp.where(still, jnp.where(wave_x == 0.0, mean, 0.0), first)
        v1 = jnp.where(still, first, -(wave_y * inverse) * pushed - wave_z * second)
        v2 = jnp.where(still, second, -(wave_z * inverse) * pushed + wave_y * second)
        return v0, v1, v2

    def own_copy(a):
        return remote(modes.at[0, a], modes.at[0, a], mode_send, own_recv.at[a], across)

    def pair_copy(a):
        return remote(modes.at[0, a], modes.at[1, a], mode_send, pair_recv.at[a], beside)

    def relay_copy(a):
        return remote(modes.at[1, a], modes.at[1, a], mode_send, pair_recv.at[a], across)

    def each(start, stop, do):
        def body(a, carry):
            do(a)
            return carry

        lax.fori_loop(start, stop, body, 0)

    few = band // 2
    final = 5
    crossing = 6
    late = 8

    def transform(step, slot, high, half, kept=(1, 2, 0)):
        owner = pair_member if slot else member
        top_row = high * band + half * few
        fields = [rebuild(slot, top_row + a, owner) for a in range(few)]
        points = planes * near_group
        chunk = (1 - side if slot else side) * 2 + high
        slots = (half * 4 + chunk) * near_group
        mean_slots = chunk * near_group
        complete = step % 2 == 1
        operands = []
        for f in kept:
            parts = [fields[a][f] for a in range(few)]
            stacked = jnp.concatenate(
                [
                    jnp.concatenate(parts, axis=1),
                    jnp.concatenate([turned(p) for p in parts], axis=1),
                ],
                axis=0,
            )
            operands.append((f, split(stacked)))

        def deliver(target, place_in, away, only=kept):
            tables = (xi0[target * 2 + side], xi1[target * 2 + side])
            for f, stacked in operands:
                if f not in only:
                    continue
                count = 2 if f else 1
                moved = dot3([t[: count * points] for t in tables], stacked)
                for p in range(planes):
                    for c in range(count):
                        if f:
                            view, offset = spread.at[place_in, p], 2 * (f - 1) + c
                        else:
                            view, offset = spread_mean.at[place_in // 2, p // 2], 2 * half + p % 2
                        view = view.reshape(near_group * rows, retained)
                        top = c * points + p * near_group
                        for a in range(few):
                            view[pl.ds(4 * a + offset, near_group, stride=rows), :] = moved[
                                top : top + near_group, a * retained : (a + 1) * retained
                            ]
            if not away:
                recv[:, slots + spot] = spread[place_in, :, spot]
                if complete:
                    recv_mean[:, mean_slots + spot] = spread_mean[place_in // 2, :, spot]

            def send(other, k):
                to = device(target, other // near, side * near + lax.rem(other, near))
                if only != (0,):
                    remote(
                        spread.at[place_in, pl.ds(2 * k, 2), other],
                        recv.at[pl.ds(2 * k, 2), slots + spot],
                        field_send,
                        field_recv.at[field_class(place_in) * pairs + k],
                        to,
                    ).start()
                if complete:
                    remote(
                        spread_mean.at[place_in // 2, k, other],
                        recv_mean.at[k, mean_slots + spot],
                        field_send,
                        mean_recv.at[mean_class(place_in) * pairs + k],
                        to,
                    ).start()

            def emit(*parts):
                for k in parts:

                    def push(turn_index, carry, k=k):
                        send(lax.rem(spot + near_group - turn_index, near_group), k)
                        return carry

                    lax.fori_loop(0 if away else 1, near_group, push, 0)

            return emit

        if step in (final - 1, final):

            @pl.when(position == 0)
            def _():
                emit = deliver(1, step + 2, True, kept if step == final else (0,))
                if complete:
                    emit(*range(pairs))

        return deliver(position, step, False)

    def field_class(place_in):
        return place_in if place_in <= final else place_in - 2 if place_in >= late else place_in

    def mean_class(place_in):
        return min(place_in // 2, final // 2 + 1)

    def await_fields(k, kind, senders):
        some = recv.at[pl.ds(2 * k, 2), pl.ds(0, senders)]
        remote(some, some, field_send, field_recv.at[kind * pairs + k], beside).wait_recv()

    def await_means(k, kind, senders):
        some = recv_mean.at[k, pl.ds(0, senders)]
        remote(some, some, field_send, mean_recv.at[kind * pairs + k], beside).wait_recv()

    low, high = list(range(band)), list(range(band, rows))
    own_order = high + low[::-1]

    def send_pair(rows_of):
        for a in rows_of:
            pair_copy(a).start()

    def take_own(rows_of):
        for a in rows_of:
            own_copy(a).wait_recv()
            if a in high:
                pair_copy(a).start()

    def take_pair(rows_of):
        for a in rows_of:
            pair_copy(a).wait_recv()
            if a in high or a < few:

                @pl.when(position == (1 if a in high else 0))
                def _():
                    relay_copy(a).start()

    def on(which, do):
        @pl.when(position == which)
        def _():
            do()

    def start_first():
        for a in high:
            own_copy(a).start()
        enter(0, band)
        send_pair(low[:2])
        for a in low[::-1]:
            own_copy(a).start()

    on(0, start_first)
    for i, load in enumerate(loads):
        if i not in needed:
            load.wait()
    on(1, lambda: take_own(high[:few]))
    rest, every = range(1, pairs), range(pairs)

    def emit_all(*emits):
        for k in every:
            for emit in emits:
                emit(k)

    emit_0 = transform(0, 0, 1, 0)
    on(0, lambda: emit_0(0))
    on(1, lambda: emit_0(*every))
    on(0, lambda: send_pair(low[2:3]))
    on(1, lambda: take_own(high[few:]))
    emit_1 = transform(1, 0, 1, 1)
    on(0, lambda: emit_1(0))
    on(1, lambda: emit_1(*every))
    on(0, lambda: send_pair(low[3:]))
    on(1, lambda: take_own(low[few:][::-1]))
    on(1, lambda: take_pair(high[:1]))
    emit_2 = transform(2, 0, 0, 1)
    on(0, lambda: emit_2(0))
    on(1, lambda: emit_2(*every))
    on(1, lambda: take_own(low[:few][::-1]))
    emit_3 = transform(3, 0, 0, 0)
    emit_3(0)

    def emit_own():
        for k in rest:
            for emit in (emit_0, emit_1, emit_2, emit_3):
                emit(k)

    on(0, emit_own)
    on(0, lambda: take_pair(low[:few]))
    on(1, lambda: take_pair(high[1:few]))
    emit_4 = transform(4, 1, position, 0)
    emit_4(0)
    on(1, lambda: emit_3(*rest))
    emit_4(*rest)
    on(0, lambda: take_pair(low[few:]))
    on(1, lambda: take_pair(high[few:]))
    emit_5 = transform(5, 1, position, 1)

    def finish_late():
        emit_5(0)
        take_pair(high[:few])
        emit_6 = transform(late, 1, 1, 0)
        emit_6(0)
        emit_5(*rest)
        emit_6(*rest)
        take_pair(high[few:])
        transform(late + 1, 1, 1, 1)(*every)

    def join_late():
        take_pair(low[:few])
        emit_all(emit_5, transform(late, 1, 0, 0, (1, 2)))

    on(0, finish_late)
    on(1, join_late)

    tables = [ref[...] for ref in plane_refs]

    def plane_pair(k, carry):
        for kind in range(7):
            await_fields(k, kind, near_group - 1)
        for kind in range(3):
            await_means(k, kind, near_group - 1)

        def await_last(senders):
            await_fields(k, 7, senders)
            await_means(k, 3, senders)

        on(0, lambda: await_last(near_group - 1))
        on(1, lambda: await_last(near_group))

        def plane(odd, carry):
            p = 2 * k + odd

            view = recv.at[p].reshape(8 * near_group * rows, retained)
            v1, d1, v2, d2 = [view[pl.ds(i, retained, stride=4), :] for i in range(4)]
            view = recv_mean.at[k].reshape(4 * near_group * rows, retained)
            v0 = jnp.concatenate(
                [
                    view[pl.ds(2 * half + odd, retained // 2, stride=4), :]
                    for half in range(2)
                ],
                axis=0,
            )
            for f, values in enumerate(plane_math([v0, v1, v2, d1, d2], tables)):
                result[p, :, f] = values.reshape(groups, rows, retained)

            def push(turn_index, carry):
                to_place = lax.rem(place + near + turn_index // count_py, count_pz)
                to_row = lax.rem(row + turn_index, count_py)
                to_member = to_row * count_pz + to_place

                @pl.when(jnp.logical_or(position == 0, to_member != member))
                def _():
                    remote(
                        result.at[p, to_member],
                        arrived.at[p, position * groups + member],
                        back_send,
                        back_recv.at[p],
                        device(1, to_row, to_place),
                    ).start()

                return carry

            lax.fori_loop(0, groups, push, 0)

            @pl.when(position == 1)
            def _():
                arrived[p, groups + member] = result[p, member]

            return carry

        return lax.fori_loop(0, 2, plane, carry)

    lax.fori_loop(0, pairs, plane_pair, 0)

    def gather(start, count, a):
        view = arrived.reshape(planes * total * 3 * rows, retained)
        wide = jnp.concatenate(
            [
                view[pl.ds((start * total * 3 + f) * rows + a, count * total, stride=3 * rows), :]
                for f in range(3)
            ],
            axis=1,
        )
        back = jnp.concatenate(
            [
                turned(wide[:, f * retained : (f + 1) * retained])
                for f in range(3)
            ],
            axis=1,
        )
        return split(jnp.concatenate([wide, back], axis=0))

    @pl.when(position == 1)
    def _():
        def await_plane(p):
            some = arrived.at[p, pl.ds(0, total - 1)]
            remote(some, some, back_send, back_recv.at[p], beside).wait_recv()

        each(0, early, await_plane)

        def begin(a):
            before = jnp.concatenate(rebuild(0, a, member), axis=1)
            change = dot3((fa0[...], fa1[...]), gather(0, early, a))
            partial_sum[a] = before + time_step * change
            wave_x, wave_y = wave_x_ref[...], wave_y_of(a, member)
            squared = wave_x * wave_x + (wave_y * wave_y + wave_z * wave_z)
            damping = jnp.exp((-viscosity * time_step) * squared)
            scales[0, a] = damping
            scales[1, a] = damping / jnp.maximum(squared, 1.0)

        each(0, rows, begin)
        each(early, planes, await_plane)

        def finish(pair):
            sides = [gather(early, planes - early, 2 * pair + i) for i in range(2)]
            both = [jnp.concatenate(parts, axis=1) for parts in zip(*sides)]
            change = dot3((fb0[...], fb1[...]), both)
            for i in range(2):
                a = 2 * pair + i
                after = partial_sum[a] + time_step * change[:, 3 * i * retained : 3 * (i + 1) * retained]
                values = [after[:, f * retained : (f + 1) * retained] for f in range(3)]
                waves = (wave_x_ref[...], wave_y_of(a, member), wave_z)
                inner = sum(wave * value for wave, value in zip(waves, values)) * scales[1, a]
                for f in range(3):
                    view, rows_of = strided(out, f, a)
                    view[rows_of, :] = scales[0, a] * values[f] - waves[f] * inner

        each(0, rows // 2, finish)

    def await_sends(*sent):
        for some in sent:
            remote(some, some, field_send, field_recv.at[0], beside).wait_send()

    others = pl.ds(0, near_group - 1)
    await_sends(
        spread.at[pl.ds(0, crossing), :, others],
        spread_mean.at[pl.ds(0, crossing // 2), :, others],
    )

    @pl.when(position == 0)
    def _():
        await_sends(
            spread.at[crossing + 1],
            spread_mean.at[crossing // 2],
            spread.at[pl.ds(late, 2), :, others],
            spread_mean.at[late // 2, :, others],
        )

    @pl.when(position == 1)
    def _():
        await_sends(spread.at[late, :, others])

    some = modes.at[1, pl.ds(0, band)]
    remote(modes.at[0], modes.at[0], mode_send, own_recv.at[0], beside).wait_send()

    @pl.when(position == 0)
    def _():
        remote(some, some, mode_send, own_recv.at[0], beside).wait_send()
        relayed = modes.at[1, pl.ds(0, few)]
        remote(relayed, relayed, mode_send, own_recv.at[0], beside).wait_send()
        remote(result, result, back_send, back_recv.at[0], beside).wait_send()

    @pl.when(position == 1)
    def _():
        some = result.at[:, pl.ds(0, groups - 1)]
        remote(some, some, back_send, back_recv.at[0], beside).wait_send()


def helped_advance(stored, count_py, count_pz, halves):
    _, retained, rows, _ = stored.shape
    groups = count_py * count_pz
    extent = 3 * retained // 2
    near_group = groups // 2
    planes = extent // (groups * halves)
    pairs = planes // 2
    tables = x_tables(extent, retained, count_py, count_pz, halves)
    tables += plane_tables(extent, retained, count_py, count_pz)
    tables = [jnp.asarray(table) for table in tables]
    vmem = pl.BlockSpec(memory_space=pltpu.VMEM)
    return pl.pallas_call(
        step_kernel,
        in_specs=[pl.BlockSpec(memory_space=pl.ANY)] * (1 + len(tables)),
        out_specs=vmem,
        out_shape=pltpu.VMEM(stored.shape, jnp.float32),
        scratch_shapes=[pltpu.VMEM(table.shape, table.dtype) for table in tables]
        + [
            pltpu.VMEM(stored.shape, jnp.float32),
            pltpu.VMEM((2, rows, 2 * retained + 8, retained), jnp.float32),
            pltpu.VMEM((10, planes, near_group, rows, retained), jnp.float32),
            pltpu.VMEM((5, pairs, near_group, rows, retained), jnp.float32),
            pltpu.VMEM((planes, 8 * near_group, rows, retained), jnp.float32),
            pltpu.VMEM((pairs, 4 * near_group, rows, retained), jnp.float32),
            pltpu.VMEM((planes, groups, 3, rows, retained), jnp.float32),
            pltpu.VMEM((planes, halves * groups, 3, rows, retained), jnp.float32),
            pltpu.VMEM((rows, retained, 3 * retained), jnp.float32),
            pltpu.VMEM((2, rows, retained, retained), jnp.float32),
            pltpu.SemaphoreType.DMA,
            pltpu.SemaphoreType.DMA((len(tables),)),
            pltpu.SemaphoreType.DMA,
            pltpu.SemaphoreType.DMA((rows,)),
            pltpu.SemaphoreType.DMA((rows,)),
            pltpu.SemaphoreType.DMA,
            pltpu.SemaphoreType.DMA((8 * pairs,)),
            pltpu.SemaphoreType.DMA((4 * pairs,)),
            pltpu.SemaphoreType.DMA,
            pltpu.SemaphoreType.DMA((planes,)),
        ],
        compiler_params=pltpu.CompilerParams(
            has_side_effects=True, collective_id=0, vmem_limit_bytes=56 * 1024 * 1024
        ),
        name="step",
    )(stored, *tables)


def shards(start_states):
    count_py = lax.axis_size("py")
    count_pz = lax.axis_size("pz")
    groups = count_py * count_pz
    member = lax.axis_index("py") * count_pz + lax.axis_index("pz")
    layout = (count_py, count_pz, groups, member)
    position = lax.axis_index("tm")
    slices = lax.axis_size("tm")
    retained = start_states.shape[-1]
    stored = start_states.reshape(3, retained, start_states.shape[3], retained)
    if slices == 2:
        result = helped_advance(stored, count_py, count_pz, slices)
        return result.reshape(1, 3, retained, stored.shape[2], 1, retained)
    spectral_state = project(stored, wave_grid(retained, layout))
    fine_end = advance(spectral_state, "fine", layout)
    coarse_start = restrict(spectral_state, M, groups)
    coarse_next = advance(coarse_start, "coarse", layout)
    fine_low = restrict(fine_end, M, groups)
    correction = fine_low - coarse_next

    def relay(chained):
        return shifted(chained, "tm", 1)

    current = jnp.where(position == 1, relay(fine_low), coarse_start)

    def sweep_turn(turn_index, current):
        candidate = advance(current, "coarse", layout) + correction
        arrived = relay(candidate)
        return jnp.where(position == turn_index + 1, arrived, current)

    current = lax.fori_loop(1, slices - 1, sweep_turn, current)
    upper_band = fine_end - prolong(fine_low, retained, groups)
    previous = shifted(upper_band, "tm", 1)
    updated = prolong(current, retained, groups) + previous
    result = jnp.where(position == 0, spectral_state, updated)
    return result.reshape(1, result.shape[0], retained, result.shape[2], 1, retained)


def solution(mesh):
    in_specs = (P("tm", None, None, None, ("py", "pz"), None),)
    out_specs = P("tm", None, None, None, ("py", "pz"), None)
    return jax.shard_map(shards, mesh=mesh, in_specs=in_specs, out_specs=out_specs, check_vma=False)
```

```python
from functools import partial
import math

import jax
import jax.numpy as jnp
from jax import lax
import numpy as np
from jax.experimental import pallas as pl
from jax.experimental.pallas import tpu as pltpu
from jax.sharding import PartitionSpec as P

M = 64


viscosity = 0.03
time_step = 0.004
highest = lax.Precision.HIGHEST


def shifted(block, axis, distance):
    devices = range(lax.axis_size(axis))
    route = [(i - distance, i) for i in devices if i - distance in devices]
    return lax.ppermute(block, axis, route)


def signed_wave(places, length):
    return jnp.where(places < length // 2, places, places - length)


def rotate(values):
    halfway = values.shape[-1] // 2
    return jnp.concatenate([-values[..., halfway:], values[..., :halfway]], axis=-1)


def trig_pair(outer, inner, extent, factor):
    residue = jnp.mod(outer[:, None] * inner[None, :], extent)
    radians = residue.astype(jnp.float32) * (2.0 * math.pi / extent)
    return (jnp.cos(radians) * factor, jnp.sin(radians) * factor)


def complex_apply(cosine_part, sine_part, values, contracted, direction_sign):
    kernel = jnp.stack(
        [
            jnp.stack([cosine_part, -direction_sign * sine_part]),
            jnp.stack([direction_sign * sine_part, cosine_part]),
        ]
    )
    halfway = values.shape[-1] // 2
    split = values.reshape(values.shape[:-1] + (2, halfway))
    if contracted == 1:
        pattern = "pqok,fkaqh->foaph"
    else:
        pattern = "pqok,flkqh->floph"
    result = jnp.einsum(pattern, kernel, split, precision=highest)
    return result.reshape(result.shape[:-2] + (2 * halfway,))


def inverse_z(extent, retained):
    halfway = retained // 2
    columns = jnp.arange(retained, dtype=jnp.int32)
    harmonic = columns % halfway
    weight = jnp.where(harmonic == 0, 1.0, 2.0) * retained ** (-0.5)
    residue = jnp.mod(harmonic[:, None] * jnp.arange(extent, dtype=jnp.int32)[None, :], extent)
    radians = residue.astype(jnp.float32) * (2.0 * math.pi / extent)
    return (
        jnp.where((columns < halfway)[:, None], jnp.cos(radians), -jnp.sin(radians))
        * weight[:, None]
    )


def forward_z(extent, retained):
    halfway = retained // 2
    columns = jnp.arange(retained, dtype=jnp.int32)
    harmonic = columns % halfway
    residue = jnp.mod(jnp.arange(extent, dtype=jnp.int32)[:, None] * harmonic[None, :], extent)
    radians = residue.astype(jnp.float32) * (2.0 * math.pi / extent)
    return jnp.where((columns < halfway)[None, :], jnp.cos(radians), -jnp.sin(radians)) * (
        math.sqrt(retained) / extent
    )


def inverse_tail(portion, extent, sectioned, layout):
    count_py, count_pz, groups, member = layout
    retained = portion.shape[2]
    local_rows = retained // groups
    places = jnp.arange(retained, dtype=jnp.int32)
    owners = places // local_rows
    wave_y = signed_wave(places % local_rows * groups + owners, retained)
    points = jnp.arange(extent, dtype=jnp.int32)
    cosine_part, sine_part = trig_pair(points, wave_y, extent, retained ** (-0.5))
    along_y = complex_apply(cosine_part, sine_part, portion, 2, 1.0)
    return jnp.einsum("flyr,rz->flyz", along_y, inverse_z(extent, retained), precision=highest)


def forward_tail(portion, retained, sectioned, layout):
    count_py, count_pz, groups, member = layout
    extent = portion.shape[1]
    local_rows = extent // groups
    places = jnp.arange(extent, dtype=jnp.int32)
    points = places // local_rows * local_rows + places % local_rows
    wave_x = signed_wave(jnp.arange(retained, dtype=jnp.int32), retained)
    cosine_part, sine_part = trig_pair(wave_x, points, extent, math.sqrt(retained) / extent)
    return complex_apply(cosine_part, sine_part, portion, 1, -1.0)


def to_physical(coeffs, wavegrid, extent, resolution, layout):
    wave_x, wave_y, wave_z = wavegrid
    retained = coeffs.shape[1]
    seeds = jnp.concatenate([coeffs, wave_x * coeffs[1:3]], axis=0)
    points = jnp.arange(extent, dtype=jnp.int32)
    wave_rows = signed_wave(jnp.arange(retained, dtype=jnp.int32), retained)
    cosine_part, sine_part = trig_pair(points, wave_rows, extent, retained ** (-0.5))
    moved_x = complex_apply(cosine_part, sine_part, seeds, 1, 1.0)
    curl_x = rotate(wave_y * moved_x[2] - wave_z * moved_x[1])
    curl_y = rotate(wave_z * moved_x[0] - moved_x[4])
    curl_z = rotate(moved_x[3] - wave_y * moved_x[0])
    spread = jnp.concatenate([moved_x[:3], jnp.stack([curl_x, curl_y, curl_z])], axis=0)
    if resolution == "coarse":
        finish = partial(inverse_tail, extent=extent, sectioned=False, layout=layout)
        return finish(lax.all_to_all(spread, ("py", "pz"), split_axis=1, concat_axis=2, tiled=True))
    else:
        finish = partial(inverse_tail, extent=extent, sectioned=False, layout=layout)
        return finish(lax.all_to_all(spread, ("py", "pz"), split_axis=1, concat_axis=2, tiled=True))


def to_spectral(fields, retained, resolution, layout):
    count_py, count_pz, groups, member = layout
    extent = fields.shape[-1]
    along_z = jnp.einsum("flyz,zr->flyr", fields, forward_z(extent, retained), precision=highest)
    local_rows = retained // groups
    places = jnp.arange(retained, dtype=jnp.int32)
    wave_y = signed_wave(places % local_rows * groups + places // local_rows, retained)
    cosine_part, sine_part = trig_pair(
        wave_y, jnp.arange(extent, dtype=jnp.int32), extent, math.sqrt(retained) / extent
    )
    along_y = complex_apply(cosine_part, sine_part, along_z, 2, -1.0)
    if resolution == "coarse":
        finish = partial(forward_tail, retained=retained, sectioned=False, layout=layout)
        return finish(
            lax.all_to_all(along_y, ("py", "pz"), split_axis=2, concat_axis=1, tiled=True)
        )
    else:
        finish = partial(forward_tail, retained=retained, sectioned=False, layout=layout)
        return finish(
            lax.all_to_all(along_y, ("py", "pz"), split_axis=2, concat_axis=1, tiled=True)
        )


def wave_grid(retained, layout):
    count_py, count_pz, groups, member = layout
    places = jnp.arange(retained, dtype=jnp.int32)
    wave_x = signed_wave(places, retained).astype(jnp.float32)[:, None, None]
    local_places = jnp.arange(retained // groups, dtype=jnp.int32)
    wave_y = signed_wave(local_places * groups + member, retained).astype(jnp.float32)[
        None, :, None
    ]
    wave_z = (places % (retained // 2)).astype(jnp.float32)[None, None, :]
    return (wave_x, wave_y, wave_z)


def project(coeffs, wavegrid):
    wave_x, wave_y, wave_z = wavegrid
    squared = wave_x * wave_x + wave_y * wave_y + wave_z * wave_z
    divergence = (wave_x * coeffs[0] + wave_y * coeffs[1] + wave_z * coeffs[2]) / jnp.maximum(
        squared, 1.0
    )
    return jnp.stack(
        [
            coeffs[0] - wave_x * divergence,
            coeffs[1] - wave_y * divergence,
            coeffs[2] - wave_z * divergence,
        ]
    )


def cross_product(first_field, second_field):
    return jnp.stack(
        [
            first_field[1] * second_field[2] - first_field[2] * second_field[1],
            first_field[2] * second_field[0] - first_field[0] * second_field[2],
            first_field[0] * second_field[1] - first_field[1] * second_field[0],
        ]
    )


def advance(coeffs, resolution, layout):
    retained = coeffs.shape[1]
    extent = 3 * retained // 2
    wavegrid = wave_grid(retained, layout)
    fields = to_physical(coeffs, wavegrid, extent, resolution, layout)
    product = cross_product(fields[:3], fields[3:])
    nonlinear = to_spectral(product, retained, resolution, layout)
    wave_x, wave_y, wave_z = wavegrid
    squared = wave_x * wave_x + wave_y * wave_y + wave_z * wave_z
    damping = jnp.exp(-viscosity * time_step * squared)
    return damping * (coeffs + time_step * project(nonlinear, wavegrid))


def restrict(coeffs, kept, groups):
    halfway = kept // 2
    retained = coeffs.shape[1]
    rows_kept = jnp.concatenate([coeffs[:, :halfway], coeffs[:, retained - halfway :]], axis=1)
    local_rows = coeffs.shape[2]
    local_kept = kept // groups // 2
    rows_kept = jnp.concatenate(
        [rows_kept[:, :, :local_kept], rows_kept[:, :, local_rows - local_kept :]], axis=2
    )
    columns_half = coeffs.shape[3] // 2
    return jnp.concatenate(
        [rows_kept[..., :halfway], rows_kept[..., columns_half : columns_half + halfway]], axis=3
    )


def prolong(coeffs, retained, groups):
    components, kept, local_kept, width = coeffs.shape
    halfway = kept // 2
    zeros_x = jnp.zeros((components, retained - kept, local_kept, width), jnp.float32)
    wider = jnp.concatenate([coeffs[:, :halfway], zeros_x, coeffs[:, halfway:]], axis=1)
    local_rows = retained // groups
    split_rows = local_kept // 2
    zeros_y = jnp.zeros((components, retained, local_rows - local_kept, width), jnp.float32)
    wider = jnp.concatenate([wider[:, :, :split_rows], zeros_y, wider[:, :, split_rows:]], axis=2)
    zeros_z = jnp.zeros((components, retained, local_rows, retained // 2 - halfway), jnp.float32)
    return jnp.concatenate([wider[..., :halfway], zeros_z, wider[..., halfway:], zeros_z], axis=3)


def wave_table(length):
    places = np.arange(length)
    return np.where(places < length // 2, places, places - length)


def trig_table(outer, inner, extent):
    radians = 2.0 * np.pi / extent * np.mod(np.outer(outer, inner), extent)
    return np.cos(radians), np.sin(radians)


def split_table(table):
    table = np.asarray(table, np.float32)
    high = table.astype(jnp.bfloat16)
    low = (table - high.astype(np.float32)).astype(jnp.bfloat16)
    return high, low


def split(values):
    high = values.astype(jnp.bfloat16)
    low = (values - high.astype(jnp.float32)).astype(jnp.bfloat16)
    return high, low


def dot3(left, right):
    def dot(a, b):
        return jnp.dot(a, b, preferred_element_type=jnp.float32)

    return dot(left[0], right[0]) + dot(left[0], right[1]) + dot(left[1], right[0])


def z_tables(extent, retained):
    halfway = retained // 2
    columns = np.arange(retained)
    harmonic = columns % halfway
    cosine, sine = trig_table(harmonic, np.arange(extent), extent)
    table = np.where((columns < halfway)[:, None], cosine, -sine)
    weight = np.where(harmonic == 0, 1.0, 2.0)[:, None] * retained ** (-0.5)
    return table * weight, table.T * (math.sqrt(retained) / extent)


def wave_order(retained, count_py, count_pz):
    groups = count_py * count_pz
    rows, near = retained // groups, count_pz // 2
    half, side, high, line, z_low, inner = np.meshgrid(
        np.arange(2),
        np.arange(2),
        np.arange(2),
        np.arange(count_py),
        np.arange(near),
        np.arange(rows // 4),
        indexing="ij",
    )
    owner = line * count_pz + side * near + z_low
    return (((high * 2 + half) * (rows // 4) + inner) * groups + owner).reshape(-1)


def plane_tables(extent, retained, count_py, count_pz):
    groups = count_py * count_pz
    rows = retained // groups
    places = np.arange(retained)
    wave_in = wave_table(retained)[wave_order(retained, count_py, count_pz)]
    wave_out = wave_table(retained)[places % rows * groups + places // rows]
    cosine, sine = trig_table(np.arange(extent), wave_in, extent)
    inverse_y = np.concatenate([cosine, sine], axis=1) * retained ** (-0.5)
    cosine, sine = trig_table(wave_out, np.arange(extent), extent)
    forward_y = np.concatenate([cosine, -sine], axis=1) * (math.sqrt(retained) / extent)
    inverse_last, forward_last = z_tables(extent, retained)
    halfway = retained // 2
    lanes = np.zeros((8, retained), np.float32)
    lanes[0] = np.where(places < halfway, -1.0, 1.0)
    lanes[1] = places % halfway
    column = np.broadcast_to(wave_in[:, None], (retained, retained)).astype(np.float32)
    tables = [lanes, column]
    for table in (inverse_y, inverse_last, forward_last, forward_y):
        tables += split_table(table)
    return tables


def plane_math(fields, tables):
    lanes, wave_y, iy0, iy1, iz0, iz1, fz0, fz1, fy0, fy1 = tables
    turn, wave_z = lanes[0:1, :], lanes[1:2, :]
    retained = wave_y.shape[0]
    extent = iy0.shape[0]

    def turned(values):
        return pltpu.roll(values, retained // 2, 1) * turn

    v0, v1, v2, d1, d2 = fields
    i0 = turned(v0)
    w0 = turned(wave_y * v2 - wave_z * v1)
    w1 = wave_z * i0 - d2
    w2 = d1 - wave_y * i0
    six = (v0, v1, v2, w0, w1, w2)
    stacked = jnp.concatenate(
        [jnp.concatenate(six, axis=1), jnp.concatenate([i0] + [turned(f) for f in six[1:]], axis=1)],
        axis=0,
    )
    along_y = dot3((iy0, iy1), split(stacked))
    rows = jnp.concatenate(
        [along_y[:, f * retained : (f + 1) * retained] for f in range(6)], axis=0
    )
    physical = dot3(split(rows), (iz0, iz1))
    u0, u1, u2, w0, w1, w2 = [physical[f * extent : (f + 1) * extent] for f in range(6)]
    product = jnp.concatenate([u1 * w2 - u2 * w1, u2 * w0 - u0 * w2, u0 * w1 - u1 * w0], axis=0)
    along_z = dot3(split(product), (fz0, fz1))
    parts = [along_z[f * extent : (f + 1) * extent] for f in range(3)]
    stacked = jnp.concatenate(
        [jnp.concatenate(parts, axis=1), jnp.concatenate([turned(p) for p in parts], axis=1)],
        axis=0,
    )
    result = dot3((fy0, fy1), split(stacked))
    return [result[:, f * retained : (f + 1) * retained] for f in range(3)]


def point_place(position, side, spot, plane, near_group, planes):
    return ((position * 2 + side) * near_group + spot) * planes + plane


def x_tables(extent, retained, count_py, count_pz, halves):
    near = count_pz // 2
    near_group = count_py * near
    planes = extent // (2 * near_group * halves)
    wave_x = wave_table(retained)
    plane, spot = np.meshgrid(np.arange(planes), np.arange(near_group), indexing="ij")
    inverse = []
    for position in range(halves):
        for side in range(2):
            points = point_place(position, side, spot, plane, near_group, planes).reshape(-1)
            cosine, sine = trig_table(points, wave_x, extent)
            values = np.concatenate([cosine, sine], axis=1)
            slopes = np.concatenate([-sine * wave_x, cosine * wave_x], axis=1)
            inverse.append(np.concatenate([values, slopes], axis=0))
    inverse = np.stack(inverse) * retained ** (-0.5)
    plane, position, line, side, z_low = np.meshgrid(
        np.arange(planes),
        np.arange(halves),
        np.arange(count_py),
        np.arange(2),
        np.arange(near),
        indexing="ij",
    )
    points = point_place(position, side, line * near + z_low, plane, near_group, planes)
    points = points.reshape(planes, -1)
    early = planes - 2
    forward = []
    for some in (points[:early].reshape(-1), points[early:].reshape(-1)):
        cosine, sine = trig_table(wave_x, some, extent)
        forward.append(np.concatenate([cosine, -sine], axis=1) * (math.sqrt(retained) / extent))
    column = np.broadcast_to(wave_x[:, None], (retained, retained)).astype(np.float32)
    tables = [column]
    for table in [inverse] + forward:
        tables += split_table(table)
    return tables


def step_kernel(*refs):
    stored = refs[0]
    kept_tables = refs[1:18]
    out = refs[18]
    loaded = refs[19:36]
    wave_x_ref, xi0, xi1, fa0, fa1, fb0, fb1 = loaded[:7]
    plane_refs = loaded[7:]
    raw, modes, spread, spread_mean, recv, recv_mean = refs[36:42]
    result, arrived, partial_sum, scales = refs[42:46]
    load_sem, table_sem, mode_send, own_recv, pair_recv = refs[46:51]
    field_send, field_recv, mean_recv, back_send, back_recv = refs[51:]

    _, retained, rows, _ = stored.shape
    planes, groups = result.shape[:2]
    halves = arrived.shape[1] // groups
    count_py, count_pz = lax.axis_size("py"), lax.axis_size("pz")
    near = count_pz // 2
    near_group = count_py * near
    band = rows // 2
    pairs = planes // 2
    early = planes - 2
    position = lax.axis_index("tm")
    row, place = lax.axis_index("py"), lax.axis_index("pz")
    side, z_low = place // near, lax.rem(place, near)
    spot = row * near + z_low
    member = row * count_pz + place
    pair_place = lax.rem(place + near, count_pz)
    pair_member = row * count_pz + pair_place

    def remote(source, target, send_sem, recv_sem, device):
        return pltpu.make_async_remote_copy(
            src_ref=source,
            dst_ref=target,
            send_sem=send_sem,
            recv_sem=recv_sem,
            device_id=device,
            device_id_type=pl.DeviceIdType.MESH,
        )

    def device(half, line, z_place):
        return {"tm": half, "py": line, "pz": z_place}

    across = device(1 - position, row, place)
    beside = device(position, row, pair_place)

    def turned(values):
        return pltpu.roll(values, retained // 2, 1) * turn

    def wave_y_of(a, owner):
        place_y = a * groups + owner
        return jnp.where(place_y < retained // 2, place_y, place_y - retained).astype(jnp.float32)

    def strided(ref, f, a):
        return ref.at[f].reshape(retained * rows, retained), pl.ds(a, retained, stride=rows)

    total = halves * groups
    barrier = pltpu.get_barrier_semaphore()

    def hello(other):
        pl.semaphore_signal(
            barrier, inc=1, device_id=other, device_id_type=pl.DeviceIdType.MESH
        )

    def greet(step, carry):
        other = lax.rem(spot + step, near_group)
        for half in range(halves):
            hello(device(half, other // near, side * near + lax.rem(other, near)))
        return carry

    hello(across)
    hello(beside)
    lax.fori_loop(1, near_group, greet, 0)

    @pl.when(position == 0)
    def _():
        pltpu.make_async_copy(stored, raw, load_sem).start()

    loads = [
        pltpu.make_async_copy(source, target, table_sem.at[i])
        for i, (source, target) in enumerate(zip(kept_tables, loaded))
    ]
    modes[:, 1:, 2 * retained : 2 * retained + 8, :] = jnp.zeros(
        (2, rows - 1, 8, retained), jnp.float32
    )
    needed = (0, 7)
    for i in needed:
        loads[i].start()
    for i in needed:
        loads[i].wait()
    lanes = plane_refs[0]
    turn, wave_z = lanes[0:1, :], lanes[1:2, :]

    def project(values, wave_y):
        wave_x = wave_x_ref[...]
        squared = wave_x * wave_x + (wave_y * wave_y + wave_z * wave_z)
        divergence = (wave_x * values[0] + wave_y * values[1] + wave_z * values[2]) / jnp.maximum(
            squared, 1.0
        )
        projected = [
            values[0] - wave_x * divergence,
            values[1] - wave_y * divergence,
            values[2] - wave_z * divergence,
        ]
        return projected

    def flat_squares(wave_y):
        squares = wave_y * wave_y + wave_z * wave_z
        return squares < 0.5, 1.0 / jnp.maximum(squares, 1.0)

    @pl.when(position == 0)
    def _():
        pltpu.make_async_copy(stored, raw, load_sem).wait()

    for i, load in enumerate(loads):
        if i not in needed:
            load.start()

    def enter(start, stop):
        def first(a, carry):
            wave_y = wave_y_of(a, member)
            values = []
            for f in range(3):
                view, rows_of = strided(raw, f, a)
                values.append(view[rows_of, :])
            values = project(values, wave_y)
            for f in range(3):
                view, rows_of = strided(out, f, a)
                view[rows_of, :] = values[f]
            still, inverse = flat_squares(wave_y)
            turning = (wave_y * values[2] - wave_z * values[1]) * inverse
            modes[0, a, 0:retained, :] = jnp.where(still, values[1], values[0])
            modes[0, a, retained : 2 * retained, :] = jnp.where(still, values[2], turning)

            @pl.when(a == 0)
            def _():
                modes[0, 0, 2 * retained : 2 * retained + 8, :] = values[0][0:8]

            return carry

        lax.fori_loop(start, stop, first, 0)

    @pl.when(position == 0)
    def _():
        enter(band, rows)

    pl.semaphore_wait(barrier, 2 * near_group)

    def rebuild(slot, a, owner):
        wave_y = wave_y_of(a, owner)
        wave_x = wave_x_ref[...]
        still, inverse = flat_squares(wave_y)
        first = modes[slot, a, 0:retained, :]
        second = modes[slot, a, retained : 2 * retained, :]
        mean = modes[slot, a, 2 * retained : 2 * retained + 1, :]
        pushed = wave_x * first
        v0 = jnp.where(still, jnp.where(wave_x == 0.0, mean, 0.0), first)
        v1 = jnp.where(still, first, -(wave_y * inverse) * pushed - wave_z * second)
        v2 = jnp.where(still, second, -(wave_z * inverse) * pushed + wave_y * second)
        return v0, v1, v2

    def sent_rows(slot, a):
        return modes.at[slot, a, pl.ds(0, 2 * retained + (0 if a else 8))]

    def own_copy(a):
        return remote(sent_rows(0, a), sent_rows(0, a), mode_send, own_recv.at[a], across)

    def pair_copy(a):
        return remote(sent_rows(0, a), sent_rows(1, a), mode_send, pair_recv.at[a], beside)

    def relay_copy(a):
        return remote(sent_rows(1, a), sent_rows(1, a), mode_send, pair_recv.at[a], across)

    def each(start, stop, do):
        def body(a, carry):
            do(a)
            return carry

        lax.fori_loop(start, stop, body, 0)

    few = band // 2
    final = 5
    crossing = 6
    late = 8

    def transform(step, slot, high, half, kept=(1, 2, 0)):
        owner = pair_member if slot else member
        top_row = high * band + half * few
        fields = [rebuild(slot, top_row + a, owner) for a in range(few)]
        points = planes * near_group
        chunk = (1 - side if slot else side) * 2 + high
        slots = (half * 4 + chunk) * near_group
        mean_slots = chunk * near_group
        complete = step % 2 == 1
        operands = []
        for f in kept:
            parts = [fields[a][f] for a in range(few)]
            stacked = jnp.concatenate(
                [
                    jnp.concatenate(parts, axis=1),
                    jnp.concatenate([turned(p) for p in parts], axis=1),
                ],
                axis=0,
            )
            operands.append((f, split(stacked)))

        def deliver(target, place_in, away, only=kept):
            tables = (xi0[target * 2 + side], xi1[target * 2 + side])
            for f, stacked in operands:
                if f not in only:
                    continue
                count = 2 if f else 1
                moved = dot3([t[: count * points] for t in tables], stacked)
                for p in range(planes):
                    for c in range(count):
                        if f:
                            view, offset = spread.at[place_in, p], 2 * (f - 1) + c
                        else:
                            view, offset = spread_mean.at[place_in // 2, p // 2], 2 * half + p % 2
                        view = view.reshape(near_group * rows, retained)
                        top = c * points + p * near_group
                        for a in range(few):
                            view[pl.ds(4 * a + offset, near_group, stride=rows), :] = moved[
                                top : top + near_group, a * retained : (a + 1) * retained
                            ]
            if not away:
                recv[:, slots + spot] = spread[place_in, :, spot]
                if complete:
                    recv_mean[:, mean_slots + spot] = spread_mean[place_in // 2, :, spot]

            def send(other, k):
                to = device(target, other // near, side * near + lax.rem(other, near))
                if only != (0,):
                    remote(
                        spread.at[place_in, pl.ds(2 * k, 2), other],
                        recv.at[pl.ds(2 * k, 2), slots + spot],
                        field_send,
                        field_recv.at[field_class(place_in) * pairs + k],
                        to,
                    ).start()
                if complete:
                    remote(
                        spread_mean.at[place_in // 2, k, other],
                        recv_mean.at[k, mean_slots + spot],
                        field_send,
                        mean_recv.at[mean_class(place_in) * pairs + k],
                        to,
                    ).start()

            def emit(*parts):
                for k in parts:

                    def push(turn_index, carry, k=k):
                        send(lax.rem(spot + near_group - turn_index, near_group), k)
                        return carry

                    lax.fori_loop(0 if away else 1, near_group, push, 0)

            return emit

        if step in (final - 1, final):

            @pl.when(position == 0)
            def _():
                emit = deliver(1, step + 2, True, kept if step == final else (0,))
                if complete:
                    emit(*range(pairs))

        return deliver(position, step, False)

    def field_class(place_in):
        return place_in if place_in <= final else place_in - 2 if place_in >= late else place_in

    def mean_class(place_in):
        return min(place_in // 2, final // 2 + 1)

    def await_fields(k, kind, senders):
        some = recv.at[pl.ds(2 * k, 2), pl.ds(0, senders)]
        remote(some, some, field_send, field_recv.at[kind * pairs + k], beside).wait_recv()

    def await_means(k, kind, senders):
        some = recv_mean.at[k, pl.ds(0, senders)]
        remote(some, some, field_send, mean_recv.at[kind * pairs + k], beside).wait_recv()

    low, high = list(range(band)), list(range(band, rows))
    own_order = high + low[::-1]

    def send_pair(rows_of):
        for a in rows_of:
            pair_copy(a).start()

    def take_own(rows_of):
        for a in rows_of:
            own_copy(a).wait_recv()
            if a in high:
                pair_copy(a).start()

    def take_pair(rows_of):
        for a in rows_of:
            pair_copy(a).wait_recv()
            if a in high or a < few:

                @pl.when(position == (1 if a in high else 0))
                def _():
                    relay_copy(a).start()

    def on(which, do):
        @pl.when(position == which)
        def _():
            do()

    def start_first():
        for a in high:
            own_copy(a).start()
        enter(0, band)
        send_pair(low[:2])
        for a in low[::-1]:
            own_copy(a).start()

    on(0, start_first)
    for i, load in enumerate(loads):
        if i not in needed:
            load.wait()
    on(1, lambda: take_own(high[:few]))
    rest, every = range(1, pairs), range(pairs)

    def emit_all(*emits):
        for k in every:
            for emit in emits:
                emit(k)

    emit_0 = transform(0, 0, 1, 0)
    on(0, lambda: emit_0(0))
    on(1, lambda: emit_0(*every))
    on(0, lambda: send_pair(low[2:3]))
    on(1, lambda: take_own(high[few:]))
    emit_1 = transform(1, 0, 1, 1)
    on(0, lambda: emit_1(0))
    on(1, lambda: emit_1(*every))
    on(0, lambda: send_pair(low[3:]))
    on(1, lambda: take_own(low[few:][::-1]))
    on(1, lambda: take_pair(high[:1]))
    emit_2 = transform(2, 0, 0, 1)
    on(0, lambda: emit_2(0))
    on(1, lambda: emit_2(*every))
    on(1, lambda: take_own(low[:few][::-1]))
    emit_3 = transform(3, 0, 0, 0)
    emit_3(0)

    def emit_own():
        for k in rest:
            for emit in (emit_0, emit_1, emit_2, emit_3):
                emit(k)

    on(0, emit_own)
    on(0, lambda: take_pair(low[:few]))
    on(1, lambda: take_pair(high[1:few]))
    emit_4 = transform(4, 1, position, 0)
    emit_4(0)
    on(1, lambda: emit_3(*rest))
    emit_4(*rest)
    on(0, lambda: take_pair(low[few:]))
    on(1, lambda: take_pair(high[few:]))
    emit_5 = transform(5, 1, position, 1)

    def finish_late():
        emit_5(0)
        take_pair(high[:few])
        emit_6 = transform(late, 1, 1, 0)
        emit_6(0)
        emit_5(*rest)
        emit_6(*rest)
        take_pair(high[few:])
        transform(late + 1, 1, 1, 1)(*every)

    def join_late():
        take_pair(low[:few])
        emit_all(emit_5, transform(late, 1, 0, 0, (1, 2)))

    on(0, finish_late)
    on(1, join_late)

    tables = [ref[...] for ref in plane_refs]

    def plane_pair(k, carry):
        for kind in range(7):
            await_fields(k, kind, near_group - 1)
        for kind in range(3):
            await_means(k, kind, near_group - 1)

        def await_last(senders):
            await_fields(k, 7, senders)
            await_means(k, 3, senders)

        on(0, lambda: await_last(near_group - 1))
        on(1, lambda: await_last(near_group))

        def plane(odd, carry):
            p = 2 * k + odd

            view = recv.at[p].reshape(8 * near_group * rows, retained)
            v1, d1, v2, d2 = [view[pl.ds(i, retained, stride=4), :] for i in range(4)]
            view = recv_mean.at[k].reshape(4 * near_group * rows, retained)
            v0 = jnp.concatenate(
                [
                    view[pl.ds(2 * half + odd, retained // 2, stride=4), :]
                    for half in range(2)
                ],
                axis=0,
            )
            for f, values in enumerate(plane_math([v0, v1, v2, d1, d2], tables)):
                result[p, :, f] = values.reshape(groups, rows, retained)

            def push(turn_index, carry):
                to_place = lax.rem(place + near + turn_index // count_py, count_pz)
                to_row = lax.rem(row + turn_index, count_py)
                to_member = to_row * count_pz + to_place

                @pl.when(jnp.logical_or(position == 0, to_member != member))
                def _():
                    remote(
                        result.at[p, to_member],
                        arrived.at[p, position * groups + member],
                        back_send,
                        back_recv.at[p],
                        device(1, to_row, to_place),
                    ).start()

                return carry

            lax.fori_loop(0, groups, push, 0)

            @pl.when(position == 1)
            def _():
                arrived[p, groups + member] = result[p, member]

            return carry

        return lax.fori_loop(0, 2, plane, carry)

    lax.fori_loop(0, pairs, plane_pair, 0)

    def gather(start, count, a):
        view = arrived.reshape(planes * total * 3 * rows, retained)
        wide = jnp.concatenate(
            [
                view[pl.ds((start * total * 3 + f) * rows + a, count * total, stride=3 * rows), :]
                for f in range(3)
            ],
            axis=1,
        )
        back = jnp.concatenate(
            [
                turned(wide[:, f * retained : (f + 1) * retained])
                for f in range(3)
            ],
            axis=1,
        )
        return split(jnp.concatenate([wide, back], axis=0))

    @pl.when(position == 1)
    def _():
        def await_plane(p):
            some = arrived.at[p, pl.ds(0, total - 1)]
            remote(some, some, back_send, back_recv.at[p], beside).wait_recv()

        each(0, early, await_plane)

        def begin(a):
            before = jnp.concatenate(rebuild(0, a, member), axis=1)
            change = dot3((fa0[...], fa1[...]), gather(0, early, a))
            partial_sum[a] = before + time_step * change
            wave_x, wave_y = wave_x_ref[...], wave_y_of(a, member)
            squared = wave_x * wave_x + (wave_y * wave_y + wave_z * wave_z)
            damping = jnp.exp((-viscosity * time_step) * squared)
            scales[0, a] = damping
            scales[1, a] = damping / jnp.maximum(squared, 1.0)

        each(0, rows, begin)
        each(early, planes, await_plane)

        def finish(pair):
            sides = [gather(early, planes - early, 2 * pair + i) for i in range(2)]
            both = [jnp.concatenate(parts, axis=1) for parts in zip(*sides)]
            change = dot3((fb0[...], fb1[...]), both)
            for i in range(2):
                a = 2 * pair + i
                after = partial_sum[a] + time_step * change[:, 3 * i * retained : 3 * (i + 1) * retained]
                values = [after[:, f * retained : (f + 1) * retained] for f in range(3)]
                waves = (wave_x_ref[...], wave_y_of(a, member), wave_z)
                inner = sum(wave * value for wave, value in zip(waves, values)) * scales[1, a]
                for f in range(3):
                    view, rows_of = strided(out, f, a)
                    view[rows_of, :] = scales[0, a] * values[f] - waves[f] * inner

        each(0, rows // 2, finish)

    def await_sends(*sent):
        for some in sent:
            remote(some, some, field_send, field_recv.at[0], beside).wait_send()

    others = pl.ds(0, near_group - 1)
    await_sends(
        spread.at[pl.ds(0, crossing), :, others],
        spread_mean.at[pl.ds(0, crossing // 2), :, others],
    )

    @pl.when(position == 0)
    def _():
        await_sends(
            spread.at[crossing + 1],
            spread_mean.at[crossing // 2],
            spread.at[pl.ds(late, 2), :, others],
            spread_mean.at[late // 2, :, others],
        )

    @pl.when(position == 1)
    def _():
        await_sends(spread.at[late, :, others])

    @pl.when(position == 0)
    def _():
        for a in low + high:
            own_copy(a).wait_send()
        for a in low:
            pair_copy(a).wait_send()
        for a in low[:few]:
            relay_copy(a).wait_send()
        remote(result, result, back_send, back_recv.at[0], beside).wait_send()

    @pl.when(position == 1)
    def _():
        for a in high:
            pair_copy(a).wait_send()
            relay_copy(a).wait_send()
        some = result.at[:, pl.ds(0, groups - 1)]
        remote(some, some, back_send, back_recv.at[0], beside).wait_send()


def helped_advance(stored, count_py, count_pz, halves):
    _, retained, rows, _ = stored.shape
    groups = count_py * count_pz
    extent = 3 * retained // 2
    near_group = groups // 2
    planes = extent // (groups * halves)
    pairs = planes // 2
    tables = x_tables(extent, retained, count_py, count_pz, halves)
    tables += plane_tables(extent, retained, count_py, count_pz)
    tables = [jnp.asarray(table) for table in tables]
    vmem = pl.BlockSpec(memory_space=pltpu.VMEM)
    return pl.pallas_call(
        step_kernel,
        in_specs=[pl.BlockSpec(memory_space=pl.ANY)] * (1 + len(tables)),
        out_specs=vmem,
        out_shape=pltpu.VMEM(stored.shape, jnp.float32),
        scratch_shapes=[pltpu.VMEM(table.shape, table.dtype) for table in tables]
        + [
            pltpu.VMEM(stored.shape, jnp.float32),
            pltpu.VMEM((2, rows, 2 * retained + 8, retained), jnp.float32),
            pltpu.VMEM((10, planes, near_group, rows, retained), jnp.float32),
            pltpu.VMEM((5, pairs, near_group, rows, retained), jnp.float32),
            pltpu.VMEM((planes, 8 * near_group, rows, retained), jnp.float32),
            pltpu.VMEM((pairs, 4 * near_group, rows, retained), jnp.float32),
            pltpu.VMEM((planes, groups, 3, rows, retained), jnp.float32),
            pltpu.VMEM((planes, halves * groups, 3, rows, retained), jnp.float32),
            pltpu.VMEM((rows, retained, 3 * retained), jnp.float32),
            pltpu.VMEM((2, rows, retained, retained), jnp.float32),
            pltpu.SemaphoreType.DMA,
            pltpu.SemaphoreType.DMA((len(tables),)),
            pltpu.SemaphoreType.DMA,
            pltpu.SemaphoreType.DMA((rows,)),
            pltpu.SemaphoreType.DMA((rows,)),
            pltpu.SemaphoreType.DMA,
            pltpu.SemaphoreType.DMA((8 * pairs,)),
            pltpu.SemaphoreType.DMA((4 * pairs,)),
            pltpu.SemaphoreType.DMA,
            pltpu.SemaphoreType.DMA((planes,)),
        ],
        compiler_params=pltpu.CompilerParams(
            has_side_effects=True, collective_id=0, vmem_limit_bytes=56 * 1024 * 1024
        ),
        name="step",
    )(stored, *tables)


def shards(start_states):
    count_py = lax.axis_size("py")
    count_pz = lax.axis_size("pz")
    groups = count_py * count_pz
    member = lax.axis_index("py") * count_pz + lax.axis_index("pz")
    layout = (count_py, count_pz, groups, member)
    position = lax.axis_index("tm")
    slices = lax.axis_size("tm")
    retained = start_states.shape[-1]
    stored = start_states.reshape(3, retained, start_states.shape[3], retained)
    if slices == 2:
        result = helped_advance(stored, count_py, count_pz, slices)
        return result.reshape(1, 3, retained, stored.shape[2], 1, retained)
    spectral_state = project(stored, wave_grid(retained, layout))
    fine_end = advance(spectral_state, "fine", layout)
    coarse_start = restrict(spectral_state, M, groups)
    coarse_next = advance(coarse_start, "coarse", layout)
    fine_low = restrict(fine_end, M, groups)
    correction = fine_low - coarse_next

    def relay(chained):
        return shifted(chained, "tm", 1)

    current = jnp.where(position == 1, relay(fine_low), coarse_start)

    def sweep_turn(turn_index, current):
        candidate = advance(current, "coarse", layout) + correction
        arrived = relay(candidate)
        return jnp.where(position == turn_index + 1, arrived, current)

    current = lax.fori_loop(1, slices - 1, sweep_turn, current)
    upper_band = fine_end - prolong(fine_low, retained, groups)
    previous = shifted(upper_band, "tm", 1)
    updated = prolong(current, retained, groups) + previous
    result = jnp.where(position == 0, spectral_state, updated)
    return result.reshape(1, result.shape[0], retained, result.shape[2], 1, retained)


def solution(mesh):
    in_specs = (P("tm", None, None, None, ("py", "pz"), None),)
    out_specs = P("tm", None, None, None, ("py", "pz"), None)
    return jax.shard_map(shards, mesh=mesh, in_specs=in_specs, out_specs=out_specs, check_vma=False)
```

```python
from functools import partial
import math

import jax
import jax.numpy as jnp
from jax import lax
import numpy as np
from jax.experimental import pallas as pl
from jax.experimental.pallas import tpu as pltpu
from jax.sharding import PartitionSpec as P

M = 64


viscosity = 0.03
time_step = 0.004
highest = lax.Precision.HIGHEST


def shifted(block, axis, distance):
    devices = range(lax.axis_size(axis))
    route = [(i - distance, i) for i in devices if i - distance in devices]
    return lax.ppermute(block, axis, route)


def signed_wave(places, length):
    return jnp.where(places < length // 2, places, places - length)


def rotate(values):
    halfway = values.shape[-1] // 2
    return jnp.concatenate([-values[..., halfway:], values[..., :halfway]], axis=-1)


def trig_pair(outer, inner, extent, factor):
    residue = jnp.mod(outer[:, None] * inner[None, :], extent)
    radians = residue.astype(jnp.float32) * (2.0 * math.pi / extent)
    return (jnp.cos(radians) * factor, jnp.sin(radians) * factor)


def complex_apply(cosine_part, sine_part, values, contracted, direction_sign):
    kernel = jnp.stack(
        [
            jnp.stack([cosine_part, -direction_sign * sine_part]),
            jnp.stack([direction_sign * sine_part, cosine_part]),
        ]
    )
    halfway = values.shape[-1] // 2
    split = values.reshape(values.shape[:-1] + (2, halfway))
    if contracted == 1:
        pattern = "pqok,fkaqh->foaph"
    else:
        pattern = "pqok,flkqh->floph"
    result = jnp.einsum(pattern, kernel, split, precision=highest)
    return result.reshape(result.shape[:-2] + (2 * halfway,))


def inverse_z(extent, retained):
    halfway = retained // 2
    columns = jnp.arange(retained, dtype=jnp.int32)
    harmonic = columns % halfway
    weight = jnp.where(harmonic == 0, 1.0, 2.0) * retained ** (-0.5)
    residue = jnp.mod(harmonic[:, None] * jnp.arange(extent, dtype=jnp.int32)[None, :], extent)
    radians = residue.astype(jnp.float32) * (2.0 * math.pi / extent)
    return (
        jnp.where((columns < halfway)[:, None], jnp.cos(radians), -jnp.sin(radians))
        * weight[:, None]
    )


def forward_z(extent, retained):
    halfway = retained // 2
    columns = jnp.arange(retained, dtype=jnp.int32)
    harmonic = columns % halfway
    residue = jnp.mod(jnp.arange(extent, dtype=jnp.int32)[:, None] * harmonic[None, :], extent)
    radians = residue.astype(jnp.float32) * (2.0 * math.pi / extent)
    return jnp.where((columns < halfway)[None, :], jnp.cos(radians), -jnp.sin(radians)) * (
        math.sqrt(retained) / extent
    )


def inverse_tail(portion, extent, sectioned, layout):
    count_py, count_pz, groups, member = layout
    retained = portion.shape[2]
    local_rows = retained // groups
    places = jnp.arange(retained, dtype=jnp.int32)
    owners = places // local_rows
    wave_y = signed_wave(places % local_rows * groups + owners, retained)
    points = jnp.arange(extent, dtype=jnp.int32)
    cosine_part, sine_part = trig_pair(points, wave_y, extent, retained ** (-0.5))
    along_y = complex_apply(cosine_part, sine_part, portion, 2, 1.0)
    return jnp.einsum("flyr,rz->flyz", along_y, inverse_z(extent, retained), precision=highest)


def forward_tail(portion, retained, sectioned, layout):
    count_py, count_pz, groups, member = layout
    extent = portion.shape[1]
    local_rows = extent // groups
    places = jnp.arange(extent, dtype=jnp.int32)
    points = places // local_rows * local_rows + places % local_rows
    wave_x = signed_wave(jnp.arange(retained, dtype=jnp.int32), retained)
    cosine_part, sine_part = trig_pair(wave_x, points, extent, math.sqrt(retained) / extent)
    return complex_apply(cosine_part, sine_part, portion, 1, -1.0)


def to_physical(coeffs, wavegrid, extent, resolution, layout):
    wave_x, wave_y, wave_z = wavegrid
    retained = coeffs.shape[1]
    seeds = jnp.concatenate([coeffs, wave_x * coeffs[1:3]], axis=0)
    points = jnp.arange(extent, dtype=jnp.int32)
    wave_rows = signed_wave(jnp.arange(retained, dtype=jnp.int32), retained)
    cosine_part, sine_part = trig_pair(points, wave_rows, extent, retained ** (-0.5))
    moved_x = complex_apply(cosine_part, sine_part, seeds, 1, 1.0)
    curl_x = rotate(wave_y * moved_x[2] - wave_z * moved_x[1])
    curl_y = rotate(wave_z * moved_x[0] - moved_x[4])
    curl_z = rotate(moved_x[3] - wave_y * moved_x[0])
    spread = jnp.concatenate([moved_x[:3], jnp.stack([curl_x, curl_y, curl_z])], axis=0)
    if resolution == "coarse":
        finish = partial(inverse_tail, extent=extent, sectioned=False, layout=layout)
        return finish(lax.all_to_all(spread, ("py", "pz"), split_axis=1, concat_axis=2, tiled=True))
    else:
        finish = partial(inverse_tail, extent=extent, sectioned=False, layout=layout)
        return finish(lax.all_to_all(spread, ("py", "pz"), split_axis=1, concat_axis=2, tiled=True))


def to_spectral(fields, retained, resolution, layout):
    count_py, count_pz, groups, member = layout
    extent = fields.shape[-1]
    along_z = jnp.einsum("flyz,zr->flyr", fields, forward_z(extent, retained), precision=highest)
    local_rows = retained // groups
    places = jnp.arange(retained, dtype=jnp.int32)
    wave_y = signed_wave(places % local_rows * groups + places // local_rows, retained)
    cosine_part, sine_part = trig_pair(
        wave_y, jnp.arange(extent, dtype=jnp.int32), extent, math.sqrt(retained) / extent
    )
    along_y = complex_apply(cosine_part, sine_part, along_z, 2, -1.0)
    if resolution == "coarse":
        finish = partial(forward_tail, retained=retained, sectioned=False, layout=layout)
        return finish(
            lax.all_to_all(along_y, ("py", "pz"), split_axis=2, concat_axis=1, tiled=True)
        )
    else:
        finish = partial(forward_tail, retained=retained, sectioned=False, layout=layout)
        return finish(
            lax.all_to_all(along_y, ("py", "pz"), split_axis=2, concat_axis=1, tiled=True)
        )


def wave_grid(retained, layout):
    count_py, count_pz, groups, member = layout
    places = jnp.arange(retained, dtype=jnp.int32)
    wave_x = signed_wave(places, retained).astype(jnp.float32)[:, None, None]
    local_places = jnp.arange(retained // groups, dtype=jnp.int32)
    wave_y = signed_wave(local_places * groups + member, retained).astype(jnp.float32)[
        None, :, None
    ]
    wave_z = (places % (retained // 2)).astype(jnp.float32)[None, None, :]
    return (wave_x, wave_y, wave_z)


def project(coeffs, wavegrid):
    wave_x, wave_y, wave_z = wavegrid
    squared = wave_x * wave_x + wave_y * wave_y + wave_z * wave_z
    divergence = (wave_x * coeffs[0] + wave_y * coeffs[1] + wave_z * coeffs[2]) / jnp.maximum(
        squared, 1.0
    )
    return jnp.stack(
        [
            coeffs[0] - wave_x * divergence,
            coeffs[1] - wave_y * divergence,
            coeffs[2] - wave_z * divergence,
        ]
    )


def cross_product(first_field, second_field):
    return jnp.stack(
        [
            first_field[1] * second_field[2] - first_field[2] * second_field[1],
            first_field[2] * second_field[0] - first_field[0] * second_field[2],
            first_field[0] * second_field[1] - first_field[1] * second_field[0],
        ]
    )


def advance(coeffs, resolution, layout):
    retained = coeffs.shape[1]
    extent = 3 * retained // 2
    wavegrid = wave_grid(retained, layout)
    fields = to_physical(coeffs, wavegrid, extent, resolution, layout)
    product = cross_product(fields[:3], fields[3:])
    nonlinear = to_spectral(product, retained, resolution, layout)
    wave_x, wave_y, wave_z = wavegrid
    squared = wave_x * wave_x + wave_y * wave_y + wave_z * wave_z
    damping = jnp.exp(-viscosity * time_step * squared)
    return damping * (coeffs + time_step * project(nonlinear, wavegrid))


def restrict(coeffs, kept, groups):
    halfway = kept // 2
    retained = coeffs.shape[1]
    rows_kept = jnp.concatenate([coeffs[:, :halfway], coeffs[:, retained - halfway :]], axis=1)
    local_rows = coeffs.shape[2]
    local_kept = kept // groups // 2
    rows_kept = jnp.concatenate(
        [rows_kept[:, :, :local_kept], rows_kept[:, :, local_rows - local_kept :]], axis=2
    )
    columns_half = coeffs.shape[3] // 2
    return jnp.concatenate(
        [rows_kept[..., :halfway], rows_kept[..., columns_half : columns_half + halfway]], axis=3
    )


def prolong(coeffs, retained, groups):
    components, kept, local_kept, width = coeffs.shape
    halfway = kept // 2
    zeros_x = jnp.zeros((components, retained - kept, local_kept, width), jnp.float32)
    wider = jnp.concatenate([coeffs[:, :halfway], zeros_x, coeffs[:, halfway:]], axis=1)
    local_rows = retained // groups
    split_rows = local_kept // 2
    zeros_y = jnp.zeros((components, retained, local_rows - local_kept, width), jnp.float32)
    wider = jnp.concatenate([wider[:, :, :split_rows], zeros_y, wider[:, :, split_rows:]], axis=2)
    zeros_z = jnp.zeros((components, retained, local_rows, retained // 2 - halfway), jnp.float32)
    return jnp.concatenate([wider[..., :halfway], zeros_z, wider[..., halfway:], zeros_z], axis=3)


def wave_table(length):
    places = np.arange(length)
    return np.where(places < length // 2, places, places - length)


def trig_table(outer, inner, extent):
    radians = 2.0 * np.pi / extent * np.mod(np.outer(outer, inner), extent)
    return np.cos(radians), np.sin(radians)


def split_table(table):
    table = np.asarray(table, np.float32)
    high = table.astype(jnp.bfloat16)
    low = (table - high.astype(np.float32)).astype(jnp.bfloat16)
    return high, low


def split(values):
    high = values.astype(jnp.bfloat16)
    low = (values - high.astype(jnp.float32)).astype(jnp.bfloat16)
    return high, low


def dot3(left, right):
    def dot(a, b):
        return jnp.dot(a, b, preferred_element_type=jnp.float32)

    return dot(left[0], right[0]) + dot(left[0], right[1]) + dot(left[1], right[0])


def z_tables(extent, retained):
    halfway = retained // 2
    columns = np.arange(retained)
    harmonic = columns % halfway
    cosine, sine = trig_table(harmonic, np.arange(extent), extent)
    table = np.where((columns < halfway)[:, None], cosine, -sine)
    weight = np.where(harmonic == 0, 1.0, 2.0)[:, None] * retained ** (-0.5)
    return table * weight, table.T * (math.sqrt(retained) / extent)


def wave_order(retained, count_py, count_pz):
    groups = count_py * count_pz
    rows, near = retained // groups, count_pz // 2
    half, side, high, line, z_low, inner = np.meshgrid(
        np.arange(2),
        np.arange(2),
        np.arange(2),
        np.arange(count_py),
        np.arange(near),
        np.arange(rows // 4),
        indexing="ij",
    )
    owner = line * count_pz + side * near + z_low
    return (((high * 2 + half) * (rows // 4) + inner) * groups + owner).reshape(-1)


def plane_tables(extent, retained, count_py, count_pz):
    groups = count_py * count_pz
    rows = retained // groups
    places = np.arange(retained)
    wave_in = wave_table(retained)[wave_order(retained, count_py, count_pz)]
    wave_out = wave_table(retained)[places % rows * groups + places // rows]
    cosine, sine = trig_table(np.arange(extent), wave_in, extent)
    inverse_y = np.concatenate([cosine, sine], axis=1) * retained ** (-0.5)
    cosine, sine = trig_table(wave_out, np.arange(extent), extent)
    forward_y = np.concatenate([cosine, -sine], axis=1) * (math.sqrt(retained) / extent)
    inverse_last, forward_last = z_tables(extent, retained)
    halfway = retained // 2
    lanes = np.zeros((8, retained), np.float32)
    lanes[0] = np.where(places < halfway, -1.0, 1.0)
    lanes[1] = places % halfway
    column = np.broadcast_to(wave_in[:, None], (retained, retained)).astype(np.float32)
    tables = [lanes, column]
    for table in (inverse_y, inverse_last, forward_last, forward_y):
        tables += split_table(table)
    return tables


def plane_math(fields, tables):
    lanes, wave_y, iy0, iy1, iz0, iz1, fz0, fz1, fy0, fy1 = tables
    turn, wave_z = lanes[0:1, :], lanes[1:2, :]
    retained = wave_y.shape[0]
    extent = iy0.shape[0]

    def turned(values):
        return pltpu.roll(values, retained // 2, 1) * turn

    v0, v1, v2, d1, d2 = fields
    i0 = turned(v0)
    w0 = turned(wave_y * v2 - wave_z * v1)
    w1 = wave_z * i0 - d2
    w2 = d1 - wave_y * i0
    six = (v0, v1, v2, w0, w1, w2)
    stacked = jnp.concatenate(
        [jnp.concatenate(six, axis=1), jnp.concatenate([i0] + [turned(f) for f in six[1:]], axis=1)],
        axis=0,
    )
    along_y = dot3((iy0, iy1), split(stacked))
    rows = jnp.concatenate(
        [along_y[:, f * retained : (f + 1) * retained] for f in range(6)], axis=0
    )
    physical = dot3(split(rows), (iz0, iz1))
    u0, u1, u2, w0, w1, w2 = [physical[f * extent : (f + 1) * extent] for f in range(6)]
    product = jnp.concatenate([u1 * w2 - u2 * w1, u2 * w0 - u0 * w2, u0 * w1 - u1 * w0], axis=0)
    along_z = dot3(split(product), (fz0, fz1))
    parts = [along_z[f * extent : (f + 1) * extent] for f in range(3)]
    stacked = jnp.concatenate(
        [jnp.concatenate(parts, axis=1), jnp.concatenate([turned(p) for p in parts], axis=1)],
        axis=0,
    )
    result = dot3((fy0, fy1), split(stacked))
    return [result[:, f * retained : (f + 1) * retained] for f in range(3)]


def point_place(position, side, spot, plane, near_group, planes):
    return ((position * 2 + side) * near_group + spot) * planes + plane


def x_tables(extent, retained, count_py, count_pz, halves):
    near = count_pz // 2
    near_group = count_py * near
    planes = extent // (2 * near_group * halves)
    wave_x = wave_table(retained)
    plane, spot = np.meshgrid(np.arange(planes), np.arange(near_group), indexing="ij")
    inverse = []
    for position in range(halves):
        for side in range(2):
            points = point_place(position, side, spot, plane, near_group, planes).reshape(-1)
            cosine, sine = trig_table(points, wave_x, extent)
            values = np.concatenate([cosine, sine], axis=1)
            slopes = np.concatenate([-sine * wave_x, cosine * wave_x], axis=1)
            inverse.append(np.concatenate([values, slopes], axis=0))
    inverse = np.stack(inverse) * retained ** (-0.5)
    plane, position, line, side, z_low = np.meshgrid(
        np.arange(planes),
        np.arange(halves),
        np.arange(count_py),
        np.arange(2),
        np.arange(near),
        indexing="ij",
    )
    points = point_place(position, side, line * near + z_low, plane, near_group, planes)
    points = points.reshape(planes, -1)
    early = planes - 2
    forward = []
    for some in (points[:early].reshape(-1), points[early:].reshape(-1)):
        cosine, sine = trig_table(wave_x, some, extent)
        forward.append(np.concatenate([cosine, -sine], axis=1) * (math.sqrt(retained) / extent))
    column = np.broadcast_to(wave_x[:, None], (retained, retained)).astype(np.float32)
    tables = [column]
    for table in [inverse] + forward:
        tables += split_table(table)
    return tables


def step_kernel(*refs):
    stored = refs[0]
    kept_tables = refs[1:18]
    out = refs[18]
    loaded = refs[19:36]
    wave_x_ref, xi0, xi1, fa0, fa1, fb0, fb1 = loaded[:7]
    plane_refs = loaded[7:]
    raw, modes, spread, spread_mean, recv, recv_mean = refs[36:42]
    result, arrived, partial_sum, scales = refs[42:46]
    load_sem, table_sem, mode_send, own_recv, pair_recv = refs[46:51]
    field_send, field_recv, mean_recv, back_send, back_recv = refs[51:]

    _, retained, rows, _ = stored.shape
    planes, groups = result.shape[:2]
    halves = arrived.shape[1] // groups
    count_py, count_pz = lax.axis_size("py"), lax.axis_size("pz")
    near = count_pz // 2
    near_group = count_py * near
    band = rows // 2
    pairs = planes // 2
    early = planes - 2
    position = lax.axis_index("tm")
    row, place = lax.axis_index("py"), lax.axis_index("pz")
    side, z_low = place // near, lax.rem(place, near)
    spot = row * near + z_low
    member = row * count_pz + place
    pair_place = lax.rem(place + near, count_pz)
    pair_member = row * count_pz + pair_place

    def remote(source, target, send_sem, recv_sem, device):
        return pltpu.make_async_remote_copy(
            src_ref=source,
            dst_ref=target,
            send_sem=send_sem,
            recv_sem=recv_sem,
            device_id=device,
            device_id_type=pl.DeviceIdType.MESH,
        )

    def device(half, line, z_place):
        return {"tm": half, "py": line, "pz": z_place}

    across = device(1 - position, row, place)
    beside = device(position, row, pair_place)

    def turned(values):
        return pltpu.roll(values, retained // 2, 1) * turn

    def wave_y_of(a, owner):
        place_y = a * groups + owner
        return jnp.where(place_y < retained // 2, place_y, place_y - retained).astype(jnp.float32)

    def strided(ref, f, a):
        return ref.at[f].reshape(retained * rows, retained), pl.ds(a, retained, stride=rows)

    total = halves * groups
    barrier = pltpu.get_barrier_semaphore()

    def hello(other):
        pl.semaphore_signal(
            barrier, inc=1, device_id=other, device_id_type=pl.DeviceIdType.MESH
        )

    def greet(step, carry):
        other = lax.rem(spot + step, near_group)
        for half in range(halves):
            hello(device(half, other // near, side * near + lax.rem(other, near)))
        return carry

    hello(across)
    hello(beside)
    lax.fori_loop(1, near_group, greet, 0)

    @pl.when(position == 0)
    def _():
        pltpu.make_async_copy(stored, raw, load_sem).start()

    loads = [
        pltpu.make_async_copy(source, target, table_sem.at[i])
        for i, (source, target) in enumerate(zip(kept_tables, loaded))
    ]
    modes[:, 1:, 2 * retained : 2 * retained + 8, :] = jnp.zeros(
        (2, rows - 1, 8, retained), jnp.float32
    )
    needed = (0, 7)
    for i in needed:
        loads[i].start()
    for i in needed:
        loads[i].wait()
    lanes = plane_refs[0]
    turn, wave_z = lanes[0:1, :], lanes[1:2, :]

    def project(values, wave_y):
        wave_x = wave_x_ref[...]
        squared = wave_x * wave_x + (wave_y * wave_y + wave_z * wave_z)
        divergence = (wave_x * values[0] + wave_y * values[1] + wave_z * values[2]) / jnp.maximum(
            squared, 1.0
        )
        projected = [
            values[0] - wave_x * divergence,
            values[1] - wave_y * divergence,
            values[2] - wave_z * divergence,
        ]
        return projected

    def flat_squares(wave_y):
        squares = wave_y * wave_y + wave_z * wave_z
        return squares < 0.5, 1.0 / jnp.maximum(squares, 1.0)

    @pl.when(position == 0)
    def _():
        pltpu.make_async_copy(stored, raw, load_sem).wait()

    for i, load in enumerate(loads):
        if i not in needed:
            load.start()

    def enter(start, stop):
        def first(a, carry):
            wave_y = wave_y_of(a, member)
            values = []
            for f in range(3):
                view, rows_of = strided(raw, f, a)
                values.append(view[rows_of, :])
            values = project(values, wave_y)
            for f in range(3):
                view, rows_of = strided(out, f, a)
                view[rows_of, :] = values[f]
            still, inverse = flat_squares(wave_y)
            turning = (wave_y * values[2] - wave_z * values[1]) * inverse
            modes[0, a, 0:retained, :] = jnp.where(still, values[1], values[0])
            modes[0, a, retained : 2 * retained, :] = jnp.where(still, values[2], turning)

            @pl.when(a == 0)
            def _():
                modes[0, 0, 2 * retained : 2 * retained + 8, :] = values[0][0:8]

            return carry

        lax.fori_loop(start, stop, first, 0)

    @pl.when(position == 0)
    def _():
        enter(band, rows)

    pl.semaphore_wait(barrier, 2 * near_group)

    def rebuild(slot, a, owner):
        wave_y = wave_y_of(a, owner)
        wave_x = wave_x_ref[...]
        still, inverse = flat_squares(wave_y)
        first = modes[slot, a, 0:retained, :]
        second = modes[slot, a, retained : 2 * retained, :]
        mean = modes[slot, a, 2 * retained : 2 * retained + 1, :]
        pushed = wave_x * first
        v0 = jnp.where(still, jnp.where(wave_x == 0.0, mean, 0.0), first)
        v1 = jnp.where(still, first, -(wave_y * inverse) * pushed - wave_z * second)
        v2 = jnp.where(still, second, -(wave_z * inverse) * pushed + wave_y * second)
        return v0, v1, v2

    def sent_rows(slot, a):
        return modes.at[slot, a, pl.ds(0, 2 * retained + (0 if a else 8))]

    def own_copy(a):
        return remote(sent_rows(0, a), sent_rows(0, a), mode_send, own_recv.at[a], across)

    def pair_copy(a):
        return remote(sent_rows(0, a), sent_rows(1, a), mode_send, pair_recv.at[a], beside)

    def relay_copy(a):
        return remote(sent_rows(1, a), sent_rows(1, a), mode_send, pair_recv.at[a], across)

    def each(start, stop, do):
        def body(a, carry):
            do(a)
            return carry

        lax.fori_loop(start, stop, body, 0)

    few = band // 2
    final = 5
    crossing = 6
    late = 8

    def transform(step, slot, high, half, kept=(1, 2, 0)):
        owner = pair_member if slot else member
        top_row = high * band + half * few
        fields = [rebuild(slot, top_row + a, owner) for a in range(few)]
        points = planes * near_group
        chunk = (1 - side if slot else side) * 2 + high
        slots = (half * 4 + chunk) * near_group
        mean_slots = chunk * near_group
        complete = step % 2 == 1
        operands = []
        for f in kept:
            parts = [fields[a][f] for a in range(few)]
            stacked = jnp.concatenate(
                [
                    jnp.concatenate(parts, axis=1),
                    jnp.concatenate([turned(p) for p in parts], axis=1),
                ],
                axis=0,
            )
            operands.append((f, split(stacked)))

        def deliver(target, place_in, away, only=kept):
            tables = (xi0[target * 2 + side], xi1[target * 2 + side])
            for f, stacked in operands:
                if f not in only:
                    continue
                count = 2 if f else 1
                moved = dot3([t[: count * points] for t in tables], stacked)
                for p in range(planes):
                    for c in range(count):
                        if f:
                            view, offset = spread.at[place_in, p], 2 * (f - 1) + c
                        else:
                            view, offset = spread_mean.at[place_in // 2, p // 2], 2 * half + p % 2
                        view = view.reshape(near_group * rows, retained)
                        top = c * points + p * near_group
                        for a in range(few):
                            view[pl.ds(4 * a + offset, near_group, stride=rows), :] = moved[
                                top : top + near_group, a * retained : (a + 1) * retained
                            ]
            if not away:
                recv[:, slots + spot] = spread[place_in, :, spot]
                if complete:
                    recv_mean[:, mean_slots + spot] = spread_mean[place_in // 2, :, spot]

            def send(other, k):
                to = device(target, other // near, side * near + lax.rem(other, near))
                if only != (0,):
                    remote(
                        spread.at[place_in, pl.ds(2 * k, 2), other],
                        recv.at[pl.ds(2 * k, 2), slots + spot],
                        field_send,
                        field_recv.at[field_class(place_in) * pairs + k],
                        to,
                    ).start()
                if complete:
                    remote(
                        spread_mean.at[place_in // 2, k, other],
                        recv_mean.at[k, mean_slots + spot],
                        field_send,
                        mean_recv.at[mean_class(place_in) * pairs + k],
                        to,
                    ).start()

            def emit(*parts):
                for k in parts:

                    def push(turn_index, carry, k=k):
                        send(lax.rem(spot + near_group - turn_index, near_group), k)
                        return carry

                    lax.fori_loop(0 if away else 1, near_group, push, 0)

            return emit

        if step in (final - 1, final):

            @pl.when(position == 0)
            def _():
                emit = deliver(1, step + 2, True, kept if step == final else (0,))
                if complete:
                    emit(*range(pairs))

        return deliver(position, step, False)

    def field_class(place_in):
        return place_in if place_in <= final else place_in - 2 if place_in >= late else place_in

    def mean_class(place_in):
        return min(place_in // 2, final // 2 + 1)

    def await_fields(k, kind, senders):
        some = recv.at[pl.ds(2 * k, 2), pl.ds(0, senders)]
        remote(some, some, field_send, field_recv.at[kind * pairs + k], beside).wait_recv()

    def await_means(k, kind, senders):
        some = recv_mean.at[k, pl.ds(0, senders)]
        remote(some, some, field_send, mean_recv.at[kind * pairs + k], beside).wait_recv()

    low, high = list(range(band)), list(range(band, rows))
    own_order = high + low[::-1]

    def send_pair(rows_of):
        for a in rows_of:
            pair_copy(a).start()

    def take_own(rows_of):
        for a in rows_of:
            own_copy(a).wait_recv()
            if a in high:
                pair_copy(a).start()

    def take_pair(rows_of):
        for a in rows_of:
            pair_copy(a).wait_recv()
            if a in high or a < few:

                @pl.when(position == (1 if a in high else 0))
                def _():
                    relay_copy(a).start()

    def on(which, do):
        @pl.when(position == which)
        def _():
            do()

    def start_first():
        for a in high:
            own_copy(a).start()
        enter(0, band)
        send_pair(low[:2])
        for a in low[::-1]:
            own_copy(a).start()

    on(0, start_first)
    for i, load in enumerate(loads):
        if i not in needed:
            load.wait()
    on(1, lambda: take_own(high[:few]))
    rest, every = range(1, pairs), range(pairs)

    def emit_all(*emits):
        for k in every:
            for emit in emits:
                emit(k)

    emit_0 = transform(0, 0, 1, 0)
    emit_0(*every)
    on(0, lambda: send_pair(low[2:3]))
    on(1, lambda: take_own(high[few:]))
    emit_1 = transform(1, 0, 1, 1)
    emit_1(*every)
    on(0, lambda: send_pair(low[3:]))
    on(1, lambda: take_own(low[few:][::-1]))
    on(1, lambda: take_pair(high[:1]))
    emit_2 = transform(2, 0, 0, 1)
    emit_2(*every)
    on(1, lambda: take_own(low[:few][::-1]))
    emit_3 = transform(3, 0, 0, 0)
    emit_3(*every)
    on(0, lambda: take_pair(low[:few]))
    on(1, lambda: take_pair(high[1:few]))
    emit_4 = transform(4, 1, position, 0)
    emit_4(*every)
    on(0, lambda: take_pair(low[few:]))
    on(1, lambda: take_pair(high[few:]))
    emit_5 = transform(5, 1, position, 1)

    def finish_late():
        emit_5(0)
        take_pair(high[:few])
        emit_6 = transform(late, 1, 1, 0)
        emit_6(0)
        emit_5(*rest)
        emit_6(*rest)
        take_pair(high[few:])
        transform(late + 1, 1, 1, 1)(*every)

    def join_late():
        take_pair(low[:few])
        emit_all(emit_5, transform(late, 1, 0, 0, (1, 2)))

    on(0, finish_late)
    on(1, join_late)

    tables = [ref[...] for ref in plane_refs]

    def plane_pair(k, carry):
        for kind in range(7):
            await_fields(k, kind, near_group - 1)
        for kind in range(3):
            await_means(k, kind, near_group - 1)

        def await_last(senders):
            await_fields(k, 7, senders)
            await_means(k, 3, senders)

        on(0, lambda: await_last(near_group - 1))
        on(1, lambda: await_last(near_group))

        def plane(odd, carry):
            p = 2 * k + odd

            view = recv.at[p].reshape(8 * near_group * rows, retained)
            v1, d1, v2, d2 = [view[pl.ds(i, retained, stride=4), :] for i in range(4)]
            view = recv_mean.at[k].reshape(4 * near_group * rows, retained)
            v0 = jnp.concatenate(
                [
                    view[pl.ds(2 * half + odd, retained // 2, stride=4), :]
                    for half in range(2)
                ],
                axis=0,
            )
            for f, values in enumerate(plane_math([v0, v1, v2, d1, d2], tables)):
                result[p, :, f] = values.reshape(groups, rows, retained)

            def push(turn_index, carry):
                to_place = lax.rem(place + near + turn_index // count_py, count_pz)
                to_row = lax.rem(row + turn_index + p, count_py)
                to_member = to_row * count_pz + to_place

                @pl.when(jnp.logical_or(position == 0, to_member != member))
                def _():
                    remote(
                        result.at[p, to_member],
                        arrived.at[p, position * groups + member],
                        back_send,
                        back_recv.at[p],
                        device(1, to_row, to_place),
                    ).start()

                return carry

            lax.fori_loop(0, groups, push, 0)

            @pl.when(position == 1)
            def _():
                arrived[p, groups + member] = result[p, member]

            return carry

        return lax.fori_loop(0, 2, plane, carry)

    lax.fori_loop(0, pairs, plane_pair, 0)

    def gather(start, count, a):
        view = arrived.reshape(planes * total * 3 * rows, retained)
        wide = jnp.concatenate(
            [
                view[pl.ds((start * total * 3 + f) * rows + a, count * total, stride=3 * rows), :]
                for f in range(3)
            ],
            axis=1,
        )
        back = jnp.concatenate(
            [
                turned(wide[:, f * retained : (f + 1) * retained])
                for f in range(3)
            ],
            axis=1,
        )
        return split(jnp.concatenate([wide, back], axis=0))

    @pl.when(position == 1)
    def _():
        def await_plane(p):
            some = arrived.at[p, pl.ds(0, total - 1)]
            remote(some, some, back_send, back_recv.at[p], beside).wait_recv()

        each(0, early, await_plane)

        def begin(a):
            before = jnp.concatenate(rebuild(0, a, member), axis=1)
            change = dot3((fa0[...], fa1[...]), gather(0, early, a))
            partial_sum[a] = before + time_step * change
            wave_x, wave_y = wave_x_ref[...], wave_y_of(a, member)
            squared = wave_x * wave_x + (wave_y * wave_y + wave_z * wave_z)
            damping = jnp.exp((-viscosity * time_step) * squared)
            scales[0, a] = damping
            scales[1, a] = damping / jnp.maximum(squared, 1.0)

        each(0, rows, begin)
        each(early, planes, await_plane)

        def finish(pair):
            sides = [gather(early, planes - early, 2 * pair + i) for i in range(2)]
            both = [jnp.concatenate(parts, axis=1) for parts in zip(*sides)]
            change = dot3((fb0[...], fb1[...]), both)
            for i in range(2):
                a = 2 * pair + i
                after = partial_sum[a] + time_step * change[:, 3 * i * retained : 3 * (i + 1) * retained]
                values = [after[:, f * retained : (f + 1) * retained] for f in range(3)]
                waves = (wave_x_ref[...], wave_y_of(a, member), wave_z)
                inner = sum(wave * value for wave, value in zip(waves, values)) * scales[1, a]
                for f in range(3):
                    view, rows_of = strided(out, f, a)
                    view[rows_of, :] = scales[0, a] * values[f] - waves[f] * inner

        each(0, rows // 2, finish)

    def await_sends(*sent):
        for some in sent:
            remote(some, some, field_send, field_recv.at[0], beside).wait_send()

    others = pl.ds(0, near_group - 1)
    await_sends(
        spread.at[pl.ds(0, crossing), :, others],
        spread_mean.at[pl.ds(0, crossing // 2), :, others],
    )

    @pl.when(position == 0)
    def _():
        await_sends(
            spread.at[crossing + 1],
            spread_mean.at[crossing // 2],
            spread.at[pl.ds(late, 2), :, others],
            spread_mean.at[late // 2, :, others],
        )

    @pl.when(position == 1)
    def _():
        await_sends(spread.at[late, :, others])

    @pl.when(position == 0)
    def _():
        for a in low + high:
            own_copy(a).wait_send()
        for a in low:
            pair_copy(a).wait_send()
        for a in low[:few]:
            relay_copy(a).wait_send()
        remote(result, result, back_send, back_recv.at[0], beside).wait_send()

    @pl.when(position == 1)
    def _():
        for a in high:
            pair_copy(a).wait_send()
            relay_copy(a).wait_send()
        some = result.at[:, pl.ds(0, groups - 1)]
        remote(some, some, back_send, back_recv.at[0], beside).wait_send()


def helped_advance(stored, count_py, count_pz, halves):
    _, retained, rows, _ = stored.shape
    groups = count_py * count_pz
    extent = 3 * retained // 2
    near_group = groups // 2
    planes = extent // (groups * halves)
    pairs = planes // 2
    tables = x_tables(extent, retained, count_py, count_pz, halves)
    tables += plane_tables(extent, retained, count_py, count_pz)
    tables = [jnp.asarray(table) for table in tables]
    vmem = pl.BlockSpec(memory_space=pltpu.VMEM)
    return pl.pallas_call(
        step_kernel,
        in_specs=[pl.BlockSpec(memory_space=pl.ANY)] * (1 + len(tables)),
        out_specs=vmem,
        out_shape=pltpu.VMEM(stored.shape, jnp.float32),
        scratch_shapes=[pltpu.VMEM(table.shape, table.dtype) for table in tables]
        + [
            pltpu.VMEM(stored.shape, jnp.float32),
            pltpu.VMEM((2, rows, 2 * retained + 8, retained), jnp.float32),
            pltpu.VMEM((10, planes, near_group, rows, retained), jnp.float32),
            pltpu.VMEM((5, pairs, near_group, rows, retained), jnp.float32),
            pltpu.VMEM((planes, 8 * near_group, rows, retained), jnp.float32),
            pltpu.VMEM((pairs, 4 * near_group, rows, retained), jnp.float32),
            pltpu.VMEM((planes, groups, 3, rows, retained), jnp.float32),
            pltpu.VMEM((planes, halves * groups, 3, rows, retained), jnp.float32),
            pltpu.VMEM((rows, retained, 3 * retained), jnp.float32),
            pltpu.VMEM((2, rows, retained, retained), jnp.float32),
            pltpu.SemaphoreType.DMA,
            pltpu.SemaphoreType.DMA((len(tables),)),
            pltpu.SemaphoreType.DMA,
            pltpu.SemaphoreType.DMA((rows,)),
            pltpu.SemaphoreType.DMA((rows,)),
            pltpu.SemaphoreType.DMA,
            pltpu.SemaphoreType.DMA((8 * pairs,)),
            pltpu.SemaphoreType.DMA((4 * pairs,)),
            pltpu.SemaphoreType.DMA,
            pltpu.SemaphoreType.DMA((planes,)),
        ],
        compiler_params=pltpu.CompilerParams(
            has_side_effects=True, collective_id=0, vmem_limit_bytes=56 * 1024 * 1024
        ),
        name="step",
    )(stored, *tables)


def shards(start_states):
    count_py = lax.axis_size("py")
    count_pz = lax.axis_size("pz")
    groups = count_py * count_pz
    member = lax.axis_index("py") * count_pz + lax.axis_index("pz")
    layout = (count_py, count_pz, groups, member)
    position = lax.axis_index("tm")
    slices = lax.axis_size("tm")
    retained = start_states.shape[-1]
    stored = start_states.reshape(3, retained, start_states.shape[3], retained)
    if slices == 2:
        result = helped_advance(stored, count_py, count_pz, slices)
        return result.reshape(1, 3, retained, stored.shape[2], 1, retained)
    spectral_state = project(stored, wave_grid(retained, layout))
    fine_end = advance(spectral_state, "fine", layout)
    coarse_start = restrict(spectral_state, M, groups)
    coarse_next = advance(coarse_start, "coarse", layout)
    fine_low = restrict(fine_end, M, groups)
    correction = fine_low - coarse_next

    def relay(chained):
        return shifted(chained, "tm", 1)

    current = jnp.where(position == 1, relay(fine_low), coarse_start)

    def sweep_turn(turn_index, current):
        candidate = advance(current, "coarse", layout) + correction
        arrived = relay(candidate)
        return jnp.where(position == turn_index + 1, arrived, current)

    current = lax.fori_loop(1, slices - 1, sweep_turn, current)
    upper_band = fine_end - prolong(fine_low, retained, groups)
    previous = shifted(upper_band, "tm", 1)
    updated = prolong(current, retained, groups) + previous
    result = jnp.where(position == 0, spectral_state, updated)
    return result.reshape(1, result.shape[0], retained, result.shape[2], 1, retained)


def solution(mesh):
    in_specs = (P("tm", None, None, None, ("py", "pz"), None),)
    out_specs = P("tm", None, None, None, ("py", "pz"), None)
    return jax.shard_map(shards, mesh=mesh, in_specs=in_specs, out_specs=out_specs, check_vma=False)
```
